32 devices in a mesh: dp: 8 (over z, y), query: 4 (over x, core).
Axes of the slice: x: 2, y: 2, z: 4, core: 2. Of those that a mesh axis runs over, the one named last changes fastest.
Arguments:
- sensors: bfloat16 [3072, 4096], P('dp'), may hold values from -8 to 8
- query_index: int32 [2, 8192], P(None, 'query'), may hold values from 0 to 127
- targets: bfloat16 [3072, 8192], P('dp', 'query'), may hold values from -6 to 6
- w_one: bfloat16 [4096, 1024], P(None, 'query'), may hold values from -0.09375 to 0.09375
- b_one: float32 [1024], P('query'), may hold values from -3 to 3
- w_two: bfloat16 [1024, 512], P('query'), may hold values from -0.1875 to 0.1875
- b_two: float32 [512], replicated, may hold values from -3 to 3
- v_one: float32 [2, 512], replicated, may hold values from -4 to 4
- c_one: float32 [512], replicated, may hold values from -3 to 3
- v_two: bfloat16 [512, 512], replicated, may hold values from -0.25 to 0.25
- c_two: float32 [512], replicated, may hold values from -3 to 3
- v_three: bfloat16 [512, 512], replicated, may hold values from -0.25 to 0.25
- c_three: float32 [512], replicated, may hold values from -3 to 3
Outputs:
- loss: float32 [], replicated
- grad_w_one: float32 [4096, 1024], P('dp', 'query')
- grad_b_one: float32 [1024], P('query')
- grad_w_two: float32 [1024, 512], P('query', 'dp')
- grad_b_two: float32 [512], replicated
- grad_v_one: float32 [2, 512], replicated
- grad_c_one: float32 [512], replicated
- grad_v_two: float32 [512, 512], replicated
- grad_c_two: float32 [512], replicated
- grad_v_three: float32 [512, 512], replicated
- grad_c_three: float32 [512], replicated
The draws below stay inside these ranges and needn't reach their ends.
All inputs are finite; a program needn't handle non-finite values.
Results may differ from the reference program's by a relative error of at most 0.00075.
Values may be sent and summed in bfloat16 or wider, within the bound.
A program may use at most 128 MiB of HBM per device.

```python
import math
import jax
import jax.numpy as jnp
from jax import lax

SENSORS = 4096
HIDDEN_SIZE = 1024
BASIS = 512
TRUNK = 512
GRID = 128
FUNC_DEV = 384
FUNCS = 3072
QUERIES = 8192
N_DP = 8


latent_count = 8


def joint_fields(key):
    key_latent = jax.random.fold_in(key, 7101)
    key_sdirs = jax.random.fold_in(key, 7102)
    key_qdirs = jax.random.fold_in(key, 7103)
    key_snoise = jax.random.fold_in(key, 7104)
    key_tnoise = jax.random.fold_in(key, 7105)
    key_pairs = jax.random.fold_in(key, 7107)
    latent = jax.random.normal(key_latent, (FUNCS, latent_count), jnp.float32)
    sensor_dirs = jax.random.normal(key_sdirs, (latent_count, SENSORS), jnp.float32)
    query_dirs = jax.random.normal(key_qdirs, (latent_count, QUERIES), jnp.float32)
    sensor_noise = jax.random.normal(key_snoise, (FUNCS, SENSORS), jnp.float32)
    target_noise = jax.random.normal(key_tnoise, (FUNCS, QUERIES), jnp.float32)
    noise_share = 0.5
    pairing = jax.random.permutation(key_pairs, N_DP)
    func_block = jnp.arange(FUNCS, dtype=jnp.int32) // FUNC_DEV
    sensor_block = jnp.arange(SENSORS, dtype=jnp.int32) // (SENSORS // N_DP)
    spiked = pairing[func_block][:, None] == sensor_block[None, :]
    boost = jnp.where(spiked, 3.0, 1.0).astype(jnp.float32)
    mixed = jnp.dot(latent, sensor_dirs) * (0.9 / math.sqrt(latent_count))
    sensors = jnp.clip(0.5 * boost * sensor_noise + mixed, -8.0, 8.0)
    solution = jnp.dot(latent, query_dirs) * (1.0 / math.sqrt(latent_count))
    targets = jnp.clip(solution + noise_share * target_noise, -6.0, 6.0)
    return (sensors, targets)


def draw_sensors(key, part):
    return joint_fields(key)[0].astype(jnp.bfloat16)


def draw_targets(key, part):
    return joint_fields(key)[1].astype(jnp.bfloat16)


def with_ends(drawn, rng, smallest, largest):
    spot = [jax.random.randint(jax.random.fold_in(rng, axis), (), 0, length) for axis, length in enumerate(drawn.shape)]
    widest = drawn.shape.index(max(drawn.shape))
    neighbour = spot[:widest] + [(spot[widest] + 1) % drawn.shape[widest]] + spot[widest + 1:]
    return drawn.at[tuple(spot)].set(smallest).at[tuple(neighbour)].set(largest)


def shard_levels(own_key, extent, split, smallest, high):
    def one(dim, parts):
        steps = jax.random.uniform(jax.random.fold_in(jax.random.fold_in(own_key, 6), dim), (parts,), jnp.float32, smallest / len(split), high / len(split))
        return jnp.repeat(jnp.exp(steps), extent[dim] // parts).reshape((-1,) + (1,) * (len(extent) - dim - 1))

    gain = one(*split[0])
    for cut in split[1:]:
        gain = gain * one(*cut)
    return gain


def normal_values(stream_key, extent, spread, reach, cuts=(), held_as=jnp.bfloat16):
    entries = spread * jax.random.normal(stream_key, extent, jnp.float32)
    if cuts:
        entries = entries * shard_levels(stream_key, extent, cuts, -0.22, 0.18)
    return jnp.clip(entries, -reach, reach).astype(held_as)


def setup_inputs(seed: int = 0) -> dict:
    streams_of = jax.random.split(jax.random.key(seed), 14)
    sensors = draw_sensors(jax.random.fold_in(streams_of[13], 71), 0)
    query_index = with_ends(jax.random.randint(streams_of[1], (2, QUERIES), 0, GRID), jax.random.fold_in(streams_of[1], 1), 0, GRID - 1).astype(jnp.int32)
    targets = draw_targets(jax.random.fold_in(streams_of[13], 71), 0)
    w_one = normal_values(streams_of[3], (SENSORS, HIDDEN_SIZE), SENSORS ** -0.5, 0.09375, ((1, 4),))
    b_one = normal_values(streams_of[4], (HIDDEN_SIZE,), 0.5, 3.0, ((0, 4),), jnp.float32)
    w_two = normal_values(streams_of[5], (HIDDEN_SIZE, BASIS), HIDDEN_SIZE ** -0.5, 0.1875, ((0, 4),))
    b_two = normal_values(streams_of[6], (BASIS,), 0.5, 3.0, (), jnp.float32)
    v_one = normal_values(streams_of[7], (2, TRUNK), 2 ** -0.5, 4.0, (), jnp.float32)
    c_one = normal_values(streams_of[8], (TRUNK,), 0.5, 3.0, (), jnp.float32)
    v_two = normal_values(streams_of[9], (TRUNK, TRUNK), TRUNK ** -0.5, 0.25)
    c_two = normal_values(streams_of[10], (TRUNK,), 0.5, 3.0, (), jnp.float32)
    v_three = normal_values(streams_of[11], (TRUNK, BASIS), TRUNK ** -0.5, 0.25)
    c_three = normal_values(streams_of[12], (BASIS,), 0.5, 3.0, (), jnp.float32)
    return {"sensors": sensors, "query_index": query_index, "targets": targets, "w_one": w_one, "b_one": b_one, "w_two": w_two, "b_two": b_two, "v_one": v_one, "c_one": c_one, "v_two": v_two, "c_two": c_two, "v_three": v_three, "c_three": c_three}


def contract_rows(left, right, precision=None):
    return lax.dot_general(left, right, (((0,), (0,)), ((), ())), precision=precision, preferred_element_type=jnp.float32)

def contract_cols(left, right, precision=None):
    return lax.dot_general(left, right, (((1,), (1,)), ((), ())), precision=precision, preferred_element_type=jnp.float32)

def trunk_forward(coords, v_one, c_one, v_two, c_two, v_three, c_three):
    first_act = jnp.tanh(coords[0][:, None] * v_one[0][None, :] + coords[1][:, None] * v_one[1][None, :] + c_one)
    first_b = first_act.astype(jnp.bfloat16)
    second_act = jnp.tanh(jnp.dot(first_b, v_two, preferred_element_type=jnp.float32) + c_two)
    second_b = second_act.astype(jnp.bfloat16)
    basis_full = jnp.dot(second_b, v_three, preferred_element_type=jnp.float32) + c_three
    return (first_act, first_b, second_act, second_b, basis_full.astype(jnp.bfloat16))

def trunk_backward(coords, first_act, first_b, second_act, second_b, grad_basis, v_two, v_three):
    grad_basis_b = grad_basis.astype(jnp.bfloat16)
    grad_v_three = contract_rows(second_b, grad_basis_b)
    grad_c_three = lax.optimization_barrier(jnp.sum(grad_basis, axis=0))
    grad_second = contract_cols(grad_basis_b, v_three) * (1.0 - second_act * second_act)
    grad_second_b = grad_second.astype(jnp.bfloat16)
    grad_v_two = contract_rows(first_b, grad_second_b)
    grad_c_two = lax.optimization_barrier(jnp.sum(grad_second, axis=0))
    grad_first = contract_cols(grad_second_b, v_two) * (1.0 - first_act * first_act)
    grad_v_one = jnp.dot(coords, grad_first, precision=lax.Precision.HIGHEST, preferred_element_type=jnp.float32)
    grad_c_one = lax.optimization_barrier(jnp.sum(grad_first, axis=0))
    return (grad_v_one, grad_c_one, grad_v_two, grad_c_two, grad_v_three, grad_c_three)

def reference(sensors, query_index, targets, w_one, b_one, w_two, b_two, v_one, c_one, v_two, c_two, v_three, c_three):
    coords = query_index.astype(jnp.float32) / (GRID - 1)
    first_act, first_b, second_act, second_b, basis_b = trunk_forward(coords, v_one, c_one, v_two, c_two, v_three, c_three)
    inv_scale = 1.0 / math.sqrt(BASIS)
    grad_scale = 64.0 / math.sqrt(FUNCS * QUERIES)
    sens_blocks = sensors.reshape(N_DP, FUNC_DEV, SENSORS)
    target_blocks = targets.reshape(N_DP, FUNC_DEV, QUERIES)

    def accumulate(running, block):
        loss_sum, grad_basis, grad_w_one, grad_b_one, grad_w_two, grad_b_two = running
        sens_block, target_block = block
        hidden = jnp.tanh(jnp.dot(sens_block, w_one, preferred_element_type=jnp.float32) + b_one)
        hidden_b = hidden.astype(jnp.bfloat16)
        coeffs = jnp.dot(hidden_b, w_two, preferred_element_type=jnp.float32) + b_two
        coeffs_b = coeffs.astype(jnp.bfloat16)
        prediction = contract_cols(coeffs_b, basis_b) * inv_scale
        misfit = prediction - target_block.astype(jnp.float32)
        loss_sum = loss_sum + jnp.sum(misfit * misfit)
        misfit_b = (misfit * grad_scale).astype(jnp.bfloat16)
        grad_coeffs = jnp.dot(misfit_b, basis_b, preferred_element_type=jnp.float32) * inv_scale
        grad_coeffs_b = grad_coeffs.astype(jnp.bfloat16)
        grad_basis = grad_basis + contract_rows(misfit_b, coeffs_b) * inv_scale
        grad_b_two = grad_b_two + lax.optimization_barrier(jnp.sum(grad_coeffs, axis=0))
        grad_w_two = grad_w_two + contract_rows(hidden_b, grad_coeffs_b)
        grad_pre = contract_cols(grad_coeffs_b, w_two) * (1.0 - hidden * hidden)
        grad_b_one = grad_b_one + lax.optimization_barrier(jnp.sum(grad_pre, axis=0))
        grad_w_one = grad_w_one + contract_rows(sens_block, grad_pre.astype(jnp.bfloat16))
        return ((loss_sum, grad_basis, grad_w_one, grad_b_one, grad_w_two, grad_b_two), None)
    initial = (jnp.zeros((), jnp.float32), jnp.zeros((QUERIES, BASIS), jnp.float32), jnp.zeros((SENSORS, HIDDEN_SIZE), jnp.float32), jnp.zeros((HIDDEN_SIZE,), jnp.float32), jnp.zeros((HIDDEN_SIZE, BASIS), jnp.float32), jnp.zeros((BASIS,), jnp.float32))
    final, _ = lax.scan(accumulate, initial, (sens_blocks, target_blocks))
    loss_sum, grad_basis, grad_w_one, grad_b_one, grad_w_two, grad_b_two = final
    grad_v_one, grad_c_one, grad_v_two, grad_c_two, grad_v_three, grad_c_three = trunk_backward(coords, first_act, first_b, second_act, second_b, grad_basis, v_two, v_three)
    return (loss_sum / (FUNCS * QUERIES), grad_w_one, grad_b_one, grad_w_two, grad_b_two, grad_v_one, grad_c_one, grad_v_two, grad_c_two, grad_v_three, grad_c_three)
```

```python
import functools
import math

import jax
import jax.numpy as jnp
from jax import lax
from jax.experimental import pallas as pl
from jax.experimental.pallas import tpu as pltpu
from jax.sharding import PartitionSpec as P

GRID = 128


def contract_rows(left, right, precision=None):
    return lax.dot_general(
        left,
        right,
        (((0,), (0,)), ((), ())),
        precision=precision,
        preferred_element_type=jnp.float32,
    )


def contract_cols(left, right, precision=None):
    return lax.dot_general(
        left,
        right,
        (((1,), (1,)), ((), ())),
        precision=precision,
        preferred_element_type=jnp.float32,
    )


def trunk_forward(coords, v_one, c_one, v_two, c_two, v_three, c_three):
    first_act = jnp.tanh(
        coords[0][:, None] * v_one[0][None, :] + coords[1][:, None] * v_one[1][None, :] + c_one
    )
    first_b = first_act.astype(jnp.bfloat16)
    second_act = jnp.tanh(jnp.dot(first_b, v_two, preferred_element_type=jnp.float32) + c_two)
    second_b = second_act.astype(jnp.bfloat16)
    basis_full = jnp.dot(second_b, v_three, preferred_element_type=jnp.float32) + c_three
    return (first_act, first_b, second_act, second_b, basis_full.astype(jnp.bfloat16))


def swap(value, axis, mask):
    count = lax.axis_size(axis)
    return lax.ppermute(value, axis, [(i, i ^ mask) for i in range(count)])


def bits_of(count):
    return [1 << b for b in range(count.bit_length() - 1)]


def gather_xor(value, axis, masks):
    blocks, offsets = value, [0]
    for mask in masks:
        blocks = jnp.concatenate([blocks, swap(blocks, axis, mask)], axis=0)
        offsets = offsets + [o ^ mask for o in offsets]
    return blocks, offsets


def split_pair(value):
    high = lax.reduce_precision(value, 8, 7)
    return high.astype(jnp.bfloat16), (value - high).astype(jnp.bfloat16)


def trunk_backward(coords, first_act, first_b, second_act, second_b, grad_basis, v_two, v_three):
    basis_hi, basis_lo = split_pair(grad_basis)
    grad_v_three = contract_rows(second_b, basis_hi) + contract_rows(second_b, basis_lo)
    grad_c_three = jnp.sum(grad_basis, axis=0)
    grad_second = (contract_cols(basis_hi, v_three) + contract_cols(basis_lo, v_three)) * (
        1.0 - second_act * second_act
    )
    second_hi, second_lo = split_pair(grad_second)
    grad_v_two = contract_rows(first_b, second_hi) + contract_rows(first_b, second_lo)
    grad_c_two = jnp.sum(grad_second, axis=0)
    grad_first = (contract_cols(second_hi, v_two) + contract_cols(second_lo, v_two)) * (
        1.0 - first_act * first_act
    )
    grad_v_one = jnp.stack(
        [jnp.sum(coords[0][:, None] * grad_first, axis=0), jnp.sum(coords[1][:, None] * grad_first, axis=0)]
    )
    grad_c_one = jnp.sum(grad_first, axis=0)
    return (grad_v_one, grad_c_one, grad_v_two, grad_c_two, grad_v_three, grad_c_three)


def local_wide(
    sensors,
    query_index,
    targets,
    w_one,
    b_one,
    w_two,
    b_two,
    v_one,
    c_one,
    v_two,
    c_two,
    v_three,
    c_three,
):
    dp_count, q_count = lax.axis_size("dp"), lax.axis_size("query")
    func_rows = sensors.shape[0]
    query_rows = query_index.shape[1]
    count_all = func_rows * dp_count * query_rows * q_count
    grad_scale = 64.0 / math.sqrt(count_all)
    inv_scale = 1.0 / math.sqrt(w_two.shape[1])
    dp_me, q_me = lax.axis_index("dp"), lax.axis_index("query")
    dp_bits, q_bits = bits_of(dp_count), bits_of(q_count)
    half = func_rows // 2
    parity = lax.rem(q_me, 2)
    mine = parity * half
    other = half - mine

    w_two_all, _ = gather_xor(w_two, "query", q_bits[::-1])
    sensor_cols = sensors.shape[1] // dp_count
    sensors_half = lax.dynamic_slice_in_dim(sensors, mine, half, 0)
    held = []
    for offset in range(dp_count):
        start = jnp.bitwise_xor(dp_me, offset) * sensor_cols
        block = lax.dynamic_slice_in_dim(sensors_half, start, sensor_cols, 1)
        held.append(block if offset == 0 else swap(block, "dp", offset))
    sensors_mine = jnp.concatenate(held, axis=0)
    sensors_other = swap(sensors_mine, "query", 1)

    hidden = jnp.tanh(jnp.dot(sensors, w_one, preferred_element_type=jnp.float32) + b_one)
    hidden_b = hidden.astype(jnp.bfloat16)
    hidden_all, _ = gather_xor(hidden_b, "query", q_bits[::-1])
    hidden_wide = jnp.concatenate(
        [hidden_all[i * func_rows : (i + 1) * func_rows] for i in range(q_count)], axis=1
    )

    coords = query_index.astype(jnp.float32) / (GRID - 1)
    first_act, first_b, second_act, second_b, basis_b = trunk_forward(
        coords, v_one, c_one, v_two, c_two, v_three, c_three
    )

    coeffs = jnp.dot(hidden_wide, w_two_all, preferred_element_type=jnp.float32) + b_two
    coeffs_b = coeffs.astype(jnp.bfloat16)
    prediction = contract_cols(coeffs_b, basis_b) * inv_scale
    misfit = prediction - targets.astype(jnp.float32)
    loss_part = jnp.sum(misfit * misfit)
    misfit_b = (misfit * grad_scale).astype(jnp.bfloat16)

    partial = jnp.dot(misfit_b, basis_b, preferred_element_type=jnp.float32) * inv_scale
    running = lax.dynamic_slice_in_dim(partial, mine, half, 0) + swap(
        lax.dynamic_slice_in_dim(partial, other, half, 0), "query", 1
    )
    for mask in q_bits[1:]:
        running = running + swap(running, "query", mask)
    running_b = running.astype(jnp.bfloat16)
    grad_coeffs_b = jnp.concatenate([running_b, swap(running_b, "query", 1)], axis=0)

    def in_order(value):
        return jnp.concatenate(
            [
                lax.dynamic_slice_in_dim(value, mine, half, 0),
                lax.dynamic_slice_in_dim(value, other, half, 0),
            ],
            axis=0,
        )

    hidden_o = in_order(hidden)
    hidden_bo = in_order(hidden_b)
    grad_pre = contract_cols(grad_coeffs_b, w_two) * (1.0 - hidden_o * hidden_o)
    grad_pre_b = grad_pre.astype(jnp.bfloat16)
    wide_first = dp_bits[1:][::-1] + dp_bits[:1]
    wide_last = dp_bits[:1] + dp_bits[1:][::-1]
    sides = []
    for rows, masks in ((grad_pre_b[:half], wide_first), (grad_pre_b[half:], wide_last)):
        blocks, offsets = gather_xor(rows, "dp", masks)
        sides.append(
            jnp.concatenate(
                [blocks[offsets.index(o) * half : (offsets.index(o) + 1) * half] for o in range(dp_count)],
                axis=0,
            )
        )
    grad_w_one = contract_rows(
        jnp.concatenate([sensors_mine, sensors_other], axis=0), jnp.concatenate(sides, axis=0)
    )

    rest = contract_rows(grad_coeffs_b, hidden_bo)
    bias_sum = jnp.broadcast_to(jnp.sum(grad_pre, axis=0)[None, :], (8, grad_pre.shape[1]))
    for mask in dp_bits[::-1]:
        rows = rest.shape[0] // 2
        upper = jnp.bitwise_and(dp_me, mask) // mask
        keep = lax.dynamic_slice_in_dim(rest, upper * rows, rows, 0)
        give = lax.dynamic_slice_in_dim(rest, (1 - upper) * rows, rows, 0)
        both = jnp.concatenate([keep, bias_sum], axis=0) + swap(
            jnp.concatenate([give, bias_sum], axis=0), "dp", mask
        )
        rest, bias_sum = both[:rows], both[rows:]
    grad_w_two = rest.T
    grad_b_one = bias_sum[0]

    trunk_parts = trunk_backward(
        coords, first_act, first_b, second_act, second_b, inv_scale * contract_rows(misfit_b, coeffs_b), v_two, v_three
    )
    loss_sum, grad_b_two, *sums = lax.psum(
        (loss_part, jnp.sum(partial, axis=0)) + trunk_parts, ("dp", "query")
    )
    return (loss_sum / count_all, grad_w_one, grad_b_one, grad_w_two, grad_b_two, *sums)


MESH = pl.DeviceIdType.MESH
F32, BF16 = jnp.float32, jnp.bfloat16
PARTS = 4
LEAD = (0, 0, 1, 2)


def natural(left, right):
    return jnp.dot(left, right, preferred_element_type=F32)


def lanes_summed(value):
    total = value[:, :128]
    for start in range(128, value.shape[1], 128):
        total = total + value[:, start : start + 128]
    return total


def halves(value):
    high = value.astype(BF16)
    return high, (value - high.astype(F32)).astype(BF16)


def step_kernel(
    n_dp,
    n_q,
    count_all,
    sensors_h,
    qidx,
    targets_h,
    w_one_h,
    b_one,
    w_two_h,
    b_two,
    v_one,
    c_one,
    v_two_h,
    c_two,
    v_three_h,
    c_three,
    loss_o,
    gw_one_o,
    gb_one_o,
    gw_two_o,
    gb_two_o,
    gv_one_o,
    gc_one_o,
    gv_two_o,
    gc_two_o,
    gv_three_o,
    gc_three_o,
    sens,
    tgt,
    w_one,
    w_two,
    v_two,
    v_three,
    v_two_t,
    v_three_t,
    hid,
    hid_b,
    first,
    second,
    first_b,
    second_b,
    basis,
    coef_b,
    coef_bt,
    mis_b,
    gco,
    gco_in,
    gco_run,
    gco_b,
    pre_all,
    sens_all,
    rest,
    rest_in,
    bias,
    bias_in,
    trunk,
    trunk_in,
    trunk_out,
    small,
    small_in,
    sums,
    loss_row,
    acc,
    load_sem,
    send_sem,
    recv_sem,
):
    func_rows, sensor_all = sens.shape
    hidden = w_one.shape[1]
    units, queries = first.shape
    basis_n = coef_b.shape[1]
    cols_dp = sensor_all // n_dp
    block = min(512, queries)
    blocks = queries // block
    inv_scale = 1.0 / math.sqrt(basis_n)
    grad_scale = 64.0 / math.sqrt(count_all)
    dp, q = lax.axis_index("dp"), lax.axis_index("query")
    me = {"dp": dp, "query": q}
    dp_bits, q_bits = bits_of(n_dp), bits_of(n_q)
    half = func_rows // 2
    part = lax.rem(q, 2)
    mine = pl.multiple_of(part * half, 8)
    other = pl.multiple_of((1 - part) * half, 8)

    def bit(index, mask):
        return lax.rem(index // mask, 2)

    def flip(index, offset):
        result = index
        for mask in bits_of(n_dp * n_q):
            if offset & mask:
                result = result + mask * (1 - 2 * bit(index, mask))
        return result

    used = [0]

    def remote(src, dst, axis, peer):
        k = used[0]
        used[0] = k + 1
        return pltpu.make_async_remote_copy(
            src_ref=src,
            dst_ref=dst,
            send_sem=send_sem.at[k],
            recv_sem=recv_sem.at[k],
            device_id={axis: peer},
            device_id_type=MESH,
        )

    sent = []

    def launch(copy):
        copy.start()
        sent.append(copy)
        return copy

    barrier = pltpu.get_barrier_semaphore()
    for offset in range(1, n_dp):
        pl.semaphore_signal(barrier, inc=1, device_id={"dp": flip(dp, offset)}, device_id_type=MESH)
    for mask in q_bits:
        pl.semaphore_signal(barrier, inc=1, device_id={"query": flip(q, mask)}, device_id_type=MESH)
    loads = {}
    own_cols = pl.ds(pl.multiple_of(dp * cols_dp, 128), cols_dp)
    for k, (name, src, dst) in enumerate(
        (
            ("w_one", w_one_h, w_one),
            ("sens", sensors_h, sens),
            ("v_two", v_two_h, v_two),
            ("v_three", v_three_h, v_three),
            ("w_two", w_two_h, w_two.at[q]),
            ("targets", targets_h, tgt),
            ("own", sensors_h.at[:, own_cols], sens_all.at[dp]),
        )
    ):
        loads[name] = pltpu.make_async_copy(src, dst, load_sem.at[k])
        loads[name].start()
    pl.semaphore_wait(barrier, n_dp - 1 + len(q_bits))

    q_order = q_bits[::-1]
    w_first = launch(remote(w_two_h, w_two.at[q], "query", flip(q, q_order[0])))
    bulk = []
    for offset in range(n_dp - 1, 0, -1):
        peer = flip(dp, offset)
        bulk.append(
            (
                peer,
                launch(
                    remote(
                        sensors_h.at[pl.ds(mine, half), pl.ds(pl.multiple_of(peer * cols_dp, 128), cols_dp)],
                        sens_all.at[dp, pl.ds(mine, half), :],
                        "dp",
                        peer,
                    )
                ),
            )
        )

    loads["w_one"].wait()
    loads["sens"].wait()
    pre = natural(sens[...], w_one[...]) + b_one[...]
    act = jnp.tanh(pre)
    hid[...] = act
    hid_b[q] = act.astype(BF16)
    h_first = launch(remote(hid_b.at[q], hid_b.at[q], "query", flip(q, q_order[0])))

    loads["v_two"].wait()
    loads["v_three"].wait()
    v_two_t[...] = v_two[...].astype(F32).T.astype(BF16)
    v_three_t[...] = v_three[...].astype(F32).T.astype(BF16)
    columns = jnp.concatenate(
        [v_one[...], c_one[...], c_two[...], c_three[...], jnp.zeros((3, units), F32)], axis=0
    ).T

    def coords_of(span):
        x = qidx[0:1, span].astype(F32) / (GRID - 1)
        y = qidx[1:2, span].astype(F32) / (GRID - 1)
        return x, y

    def forward(i, carry):
        span = pl.ds(pl.multiple_of(i * block, 128), block)
        x, y = coords_of(span)
        one = jnp.tanh(columns[:, 0:1] * x + columns[:, 1:2] * y + columns[:, 2:3])
        first[:, span] = one
        one_b = one.astype(BF16)
        first_b[:, span] = one_b
        two = jnp.tanh(natural(v_two_t[...], one_b) + columns[:, 3:4])
        second[:, span] = two
        two_b = two.astype(BF16)
        second_b[:, span] = two_b
        basis[:, span] = (natural(v_three_t[...], two_b) + columns[:, 4:5]).astype(BF16)
        return carry

    def spread(buffer, first_copy, held, masks, out):
        first_copy.wait_recv()
        for mask in masks:
            group = [
                launch(remote(buffer.at[flip(q, o)], buffer.at[flip(q, o)], "query", flip(q, mask))) for o in held
            ]
            held = held + [o ^ mask for o in held]
            out.extend(group)
            if mask != masks[-1]:
                for copy in group:
                    copy.wait_recv()
        return group

    lax.fori_loop(0, blocks // 2, forward, 0)
    loads["w_two"].wait()
    extra = []
    w_last = spread(w_two, w_first, [0, q_order[0]], q_order[1:], extra)
    lax.fori_loop(blocks // 2, blocks, forward, 0)
    h_last = spread(hid_b, h_first, [0, q_order[0]], q_order[1:], extra)
    for copy in w_last + h_last:
        copy.wait_recv()

    coef = natural(hid_b[0], w_two[0])
    for i in range(1, n_q):
        coef = coef + natural(hid_b[i], w_two[i])
    coef = coef + b_two[...]
    coef_b[...] = coef.astype(BF16)
    coef_bt[...] = coef.T.astype(BF16)

    loads["targets"].wait()
    gco[...] = jnp.zeros_like(gco)
    loss_row[...] = jnp.zeros_like(loss_row)

    def fit(i, carry):
        span = pl.ds(pl.multiple_of(i * block, 128), block)
        base = basis[:, span]
        miss = natural(coef_b[...], base) * inv_scale - tgt[:, span].astype(F32)
        loss_row[0:1, :] += jnp.sum(miss * miss, axis=0, keepdims=True)
        miss_b = (miss * grad_scale).astype(BF16)
        mis_b[:, span] = miss_b
        gco[...] += contract_cols(miss_b, base)
        return carry

    lax.fori_loop(0, blocks, fit, 0)
    gco[...] = gco[...] * inv_scale
    core_step = launch(remote(gco.at[pl.ds(other, half), :], gco_in.at[0], "query", flip(q, 1)))
    gb_two_row = jnp.sum(gco[...], axis=0, keepdims=True)
    core_step.wait_recv()
    gco_run[0] = gco[pl.ds(mine, half), :] + gco_in[0]
    reduce_steps = [launch(remote(gco_run.at[0], gco_in.at[1], "query", flip(q, q_bits[1])))]

    trunk[...] = jnp.zeros_like(trunk)
    sums[...] = jnp.zeros_like(sums)

    def backward(i, carry):
        span = pl.ds(pl.multiple_of(i * block, 128), block)
        x, y = coords_of(span)
        g_base = natural(coef_bt[...], mis_b[:, span]) * inv_scale
        sums[0] += lanes_summed(g_base)
        hi, lo = halves(g_base)
        two_b = second_b[:, span]
        trunk[:units, :] += contract_cols(two_b, hi) + contract_cols(two_b, lo)
        two = second[:, span]
        g_two = (natural(v_three[...], hi) + natural(v_three[...], lo)) * (1.0 - two * two)
        sums[1] += lanes_summed(g_two)
        hi, lo = halves(g_two)
        one_b = first_b[:, span]
        trunk[units:, :] += contract_cols(one_b, hi) + contract_cols(one_b, lo)
        one = first[:, span]
        g_one = (natural(v_two[...], hi) + natural(v_two[...], lo)) * (1.0 - one * one)
        sums[2] += lanes_summed(g_one)
        sums[3] += lanes_summed(g_one * x)
        sums[4] += lanes_summed(g_one * y)
        return carry

    lax.fori_loop(0, blocks, backward, 0)

    lane = lax.broadcasted_iota(jnp.int32, (units, 128), 1)
    table = jnp.zeros((units, 128), F32)
    for row, which in enumerate((3, 4, 2, 1, 0)):
        table = jnp.where(lane == row, jnp.sum(sums[which], axis=1, keepdims=True), table)
    rows = table.T[0:8]
    line = lax.broadcasted_iota(jnp.int32, rows.shape, 0)
    rows = jnp.where(line == 5, gb_two_row, rows)
    rows = jnp.where(line == 6, loss_row[0:1, :], rows)
    small[0] = rows

    bits = [("query", m) for m in q_bits] + [("dp", m) for m in dp_bits]
    size_all = trunk.shape[0] // PARTS
    orders, offs = [], []
    for p in range(PARTS):
        later = bits[1:]
        head = later[LEAD[p] % len(later)]
        orders.append([bits[0], head] + [b for b in later if b != head])
        offs.append(p * size_all)
    ins = [p * size_all for p in range(PARTS)]
    state = {"size": size_all}
    rounds = len(bits)
    flight = []

    def halve_start(k):
        size = state["size"] // 2
        for p in range(PARTS):
            axis, mask = orders[p][k]
            up = bit(me[axis], mask)
            give = pl.multiple_of(offs[p] + (1 - up) * size, 8)
            flight.append(
                launch(
                    remote(
                        trunk.at[pl.ds(give, size), :],
                        trunk_in.at[pl.ds(ins[p], size), :],
                        axis,
                        flip(me[axis], mask),
                    )
                )
            )
            offs[p] = offs[p] + up * size
        axis, mask = bits[k]
        flight.append(launch(remote(small.at[k], small_in.at[k], axis, flip(me[axis], mask))))

    def halve_end(k):
        size = state["size"] // 2
        for p in range(PARTS):
            flight[p].wait_recv()
            keep = pl.ds(pl.multiple_of(offs[p], 8), size)
            total = trunk[keep, :] + trunk_in[ins[p] : ins[p] + size, :]
            if k == rounds - 1:
                trunk_out[keep, :] = total
            else:
                trunk[keep, :] = total
            ins[p] += size
        flight[PARTS].wait_recv()
        small[k + 1] = small[k] + small_in[k]
        flight.clear()
        state["size"] = size

    def double_start(k):
        size = state["size"]
        for p in range(PARTS):
            axis, mask = orders[p][k]
            keep = pl.ds(pl.multiple_of(offs[p], 8), size)
            flight.append(launch(remote(trunk_out.at[keep, :], trunk_out.at[keep, :], axis, flip(me[axis], mask))))
            offs[p] = offs[p] - bit(me[axis], mask) * size

    def double_end(k):
        for copy in flight:
            copy.wait_recv()
        flight.clear()
        state["size"] *= 2

    halve_start(0)

    for k, mask in enumerate(q_bits[1:]):
        reduce_steps[k].wait_recv()
        total = gco_run[k] + gco_in[k + 1]
        if k + 2 < len(q_bits):
            gco_run[k + 1] = total
            reduce_steps.append(launch(remote(gco_run.at[k + 1], gco_in.at[k + 2], "query", flip(q, q_bits[k + 2]))))
    gco_b[pl.ds(mine, half), :] = total.astype(BF16)
    share = launch(remote(gco_b.at[pl.ds(mine, half), :], gco_b.at[pl.ds(mine, half), :], "query", flip(q, 1)))
    halve_end(0)
    halve_start(1)
    share.wait_recv()

    act = hid[...]
    g_pre = contract_cols(gco_b[...], w_two[q]) * (1.0 - act * act)
    pre_all[dp] = g_pre.astype(BF16)

    line_at, line_n = dp // 2, n_dp // 2
    side = lax.rem(dp, 2)
    pair = flip(dp, 1)
    chunks = 2
    rows_c = func_rows // chunks

    def slot(at, c):
        return pre_all.at[at * 2 + side, c * rows_c : (c + 1) * rows_c, :]

    def hop(at, c, peer):
        at = jnp.clip(at, 0, line_n - 1)
        return remote(slot(at, c), slot(at, c), "dp", peer)

    to_right = jnp.minimum(dp + 2, n_dp - 2 + side)
    to_left = jnp.maximum(dp - 2, side)
    steps = line_n - 1
    rights = [[hop(line_at - s, c, to_right) for c in range(chunks)] for s in range(steps)]
    lefts = [[hop(line_at + s, c, to_left) for c in range(chunks)] for s in range(steps)]
    own_pair = [hop(line_at, c, pair) for c in range(chunks)]
    left_pair = [[hop(line_at - 1 - s, c, pair) for c in range(chunks)] for s in range(steps)]
    right_pair = [[hop(line_at + 1 + s, c, pair) for c in range(chunks)] for s in range(steps)]

    def sends_right(s):
        return jnp.logical_and(line_at - s >= 0, line_at < line_n - 1)

    def sends_left(s):
        return jnp.logical_and(line_at + s < line_n, line_at > 0)

    for c in range(chunks):
        pl.when(sends_right(0))(rights[0][c].start)
        pl.when(sends_left(0))(lefts[0][c].start)
        own_pair[c].start()

    bias[0] = jnp.broadcast_to(jnp.sum(g_pre, axis=0, keepdims=True), bias.shape[1:])

    gco_bt = gco_b[...].astype(F32).T.astype(BF16)
    rest_all = natural(gco_bt, hid_b[q])
    rows_dp = basis_n // n_dp
    for j in range(n_dp):
        rest[j] = rest_all[j * rows_dp : (j + 1) * rows_dp, :]
    rest_held = [list(range(n_dp))]
    rest_at = [0]

    def gather_step(s):
        for c in range(chunks):

            @pl.when(line_at - 1 - s >= 0)
            def _():
                rights[s][c].wait_recv()
                left_pair[s][c].start()
                if s + 1 < steps:
                    pl.when(sends_right(s + 1))(rights[s + 1][c].start)

            @pl.when(line_at + 1 + s < line_n)
            def _():
                lefts[s][c].wait_recv()
                right_pair[s][c].start()
                if s + 1 < steps:
                    pl.when(sends_left(s + 1))(lefts[s + 1][c].start)

    b_flight = []

    def rest_start(k):
        mask = dp_bits[k]
        low = lax.rem(dp, mask) if mask > 1 else 0
        keep_n = n_dp // (2 * mask)
        want = low + (1 - bit(dp, mask)) * mask
        group = []
        for j in range(keep_n):
            group.append(
                launch(
                    remote(rest.at[want + j * 2 * mask], rest_in.at[rest_at[0] + j], "dp", flip(dp, mask))
                )
            )
        group.append(launch(remote(bias.at[k], bias_in.at[k], "dp", flip(dp, mask))))
        b_flight.append(group)

    def rest_end(k):
        mask = dp_bits[k]
        low = lax.rem(dp, mask) if mask > 1 else 0
        keep_n = n_dp // (2 * mask)
        have = low + bit(dp, mask) * mask
        for copy in b_flight[k]:
            copy.wait_recv()
        for j in range(keep_n):
            rest[have + j * 2 * mask] += rest_in[rest_at[0] + j]
        rest_at[0] += keep_n
        bias[k + 1] = bias[k] + bias_in[k]

    rest_start(0)
    halve_end(1)
    halve_start(2)
    gather_step(0)
    rest_end(0)
    rest_start(1)
    halve_end(2)
    halve_start(3)
    gather_step(1)
    rest_end(1)
    rest_start(2)
    halve_end(3)
    halve_start(4)
    for s in range(2, steps):
        gather_step(s)
    rest_end(2)
    halve_end(4)
    double_start(4)

    loads["own"].wait()
    passed = []
    for peer, copy in bulk:
        copy.wait_recv()
        block_ref = sens_all.at[peer, pl.ds(mine, half), :]
        passed.append(launch(remote(block_ref, block_ref, "query", flip(q, 1))))

    double_end(4)
    double_start(3)
    for copy in passed:
        copy.wait_recv()

    acc[...] = jnp.zeros_like(acc)

    def add_block(at):
        acc[...] += contract_rows(sens_all[at], pre_all[at])

    def line_block(i, carry):
        add_block(i * 2 + side)
        return carry

    def pair_block(i, carry):
        add_block(i * 2 + (1 - side))
        return carry

    lax.fori_loop(0, line_n, line_block, 0)
    double_end(3)
    double_start(2)
    double_end(2)
    double_start(1)

    for c in range(chunks):
        own_pair[c].wait_recv()
    for s in range(steps):
        for c in range(chunks):
            pl.when(line_at - 1 - s >= 0)(left_pair[s][c].wait_recv)
            pl.when(line_at + 1 + s < line_n)(right_pair[s][c].wait_recv)
    lax.fori_loop(0, line_n, pair_block, 0)
    out_one = pltpu.make_async_copy(acc, gw_one_o, load_sem.at[0])
    out_one.start()
    double_end(1)
    double_start(0)

    low_rows = jnp.concatenate([rest[dp], jnp.zeros((128 - rows_dp, hidden), F32)], axis=0)
    gw_two_o[...] = low_rows.T[:, :rows_dp]
    gb_one_o[...] = bias[len(dp_bits)][0:1, :]
    final = small[rounds]
    gv_one_o[...] = final[0:2]
    gc_one_o[...] = final[2:3]
    gc_two_o[...] = final[3:4]
    gc_three_o[...] = final[4:5]
    gb_two_o[...] = final[5:6]
    loss_o[...] = jnp.broadcast_to(jnp.sum(final[6:7], axis=1, keepdims=True) * (1.0 / count_all), loss_o.shape)
    double_end(0)
    outs = [out_one]
    for k, (src, dst) in enumerate(
        ((trunk_out.at[:units, :], gv_three_o), (trunk_out.at[units:, :], gv_two_o))
    ):
        copy = pltpu.make_async_copy(src, dst, load_sem.at[1 + k])
        copy.start()
        outs.append(copy)
    for copy in sent:
        copy.wait_send()
    for c in range(chunks):
        own_pair[c].wait_send()
    for s in range(steps):
        for c in range(chunks):
            pl.when(sends_right(s))(rights[s][c].wait_send)
            pl.when(sends_left(s))(lefts[s][c].wait_send)
            pl.when(line_at - 1 - s >= 0)(left_pair[s][c].wait_send)
            pl.when(line_at + 1 + s < line_n)(right_pair[s][c].wait_send)
    for copy in outs:
        copy.wait()


def local_dense(
    sensors, query_index, targets, w_one, b_one, w_two, b_two, v_one, c_one, v_two, c_two, v_three, c_three
):
    n_dp, n_q = lax.axis_size("dp"), lax.axis_size("query")
    func_rows, sensor_all = sensors.shape
    queries = query_index.shape[1]
    hidden, basis_n = w_two.shape
    units = v_two.shape[0]
    cols_dp = sensor_all // n_dp
    count_all = func_rows * n_dp * queries * n_q
    n_bits, dp_n, q_n = len(bits_of(n_dp * n_q)), len(bits_of(n_dp)), len(bits_of(n_q))
    half = func_rows // 2
    rows_dp = basis_n // n_dp
    hbm, vmem = pl.BlockSpec(memory_space=pl.ANY), pl.BlockSpec(memory_space=pltpu.VMEM)
    sem_n = 160

    def row(value):
        return value.reshape(1, -1)

    def result(*shape):
        return jax.ShapeDtypeStruct(shape, F32)

    outs = pl.pallas_call(
        functools.partial(step_kernel, n_dp, n_q, count_all),
        out_shape=(
            result(1, 128),
            result(cols_dp, hidden),
            result(1, hidden),
            result(hidden, rows_dp),
            result(1, basis_n),
            result(2, units),
            result(1, units),
            result(units, units),
            result(1, units),
            result(units, basis_n),
            result(1, basis_n),
        ),
        in_specs=[hbm, vmem, hbm, hbm, vmem, hbm, vmem, vmem, vmem, hbm, vmem, hbm, vmem],
        out_specs=(vmem, hbm, vmem, vmem, vmem, vmem, vmem, hbm, vmem, hbm, vmem),
        scratch_shapes=[
            pltpu.VMEM((func_rows, sensor_all), BF16),
            pltpu.VMEM((func_rows, queries), BF16),
            pltpu.VMEM((sensor_all, hidden), BF16),
            pltpu.VMEM((n_q, hidden, basis_n), BF16),
            pltpu.VMEM((units, units), BF16),
            pltpu.VMEM((units, basis_n), BF16),
            pltpu.VMEM((units, units), BF16),
            pltpu.VMEM((basis_n, units), BF16),
            pltpu.VMEM((func_rows, hidden), F32),
            pltpu.VMEM((n_q, func_rows, hidden), BF16),
            pltpu.VMEM((units, queries), F32),
            pltpu.VMEM((units, queries), F32),
            pltpu.VMEM((units, queries), BF16),
            pltpu.VMEM((units, queries), BF16),
            pltpu.VMEM((basis_n, queries), BF16),
            pltpu.VMEM((func_rows, basis_n), BF16),
            pltpu.VMEM((basis_n, func_rows), BF16),
            pltpu.VMEM((func_rows, queries), BF16),
            pltpu.VMEM((func_rows, basis_n), F32),
            pltpu.VMEM((q_n, half, basis_n), F32),
            pltpu.VMEM((q_n, half, basis_n), F32),
            pltpu.VMEM((func_rows, basis_n), BF16),
            pltpu.VMEM((n_dp, func_rows, hidden), BF16),
            pltpu.VMEM((n_dp, func_rows, cols_dp), BF16),
            pltpu.VMEM((n_dp, rows_dp, hidden), F32),
            pltpu.VMEM((n_dp, rows_dp, hidden), F32),
            pltpu.VMEM((dp_n + 1, 8, hidden), F32),
            pltpu.VMEM((dp_n, 8, hidden), F32),
            pltpu.VMEM((2 * units, basis_n), F32),
            pltpu.VMEM((2 * units, basis_n), F32),
            pltpu.VMEM((2 * units, basis_n), F32),
            pltpu.VMEM((n_bits + 1, 8, units), F32),
            pltpu.VMEM((n_bits, 8, units), F32),
            pltpu.VMEM((5, units, 128), F32),
            pltpu.VMEM((8, min(512, queries)), F32),
            pltpu.VMEM((cols_dp, hidden), F32),
            pltpu.SemaphoreType.DMA((8,)),
            pltpu.SemaphoreType.DMA((sem_n,)),
            pltpu.SemaphoreType.DMA((sem_n,)),
        ],
        compiler_params=pltpu.CompilerParams(
            collective_id=0, has_side_effects=True, vmem_limit_bytes=67043328
        ),
        name="step",
    )(
        sensors,
        query_index,
        targets,
        w_one,
        row(b_one),
        w_two,
        row(b_two),
        v_one,
        row(c_one),
        v_two,
        row(c_two),
        v_three,
        row(c_three),
    )
    loss, gw_one, gb_one, gw_two, gb_two, gv_one, gc_one, gv_two, gc_two, gv_three, gc_three = outs
    return (
        loss[0, 0],
        gw_one,
        gb_one.reshape(-1),
        gw_two,
        gb_two.reshape(-1),
        gv_one,
        gc_one.reshape(-1),
        gv_two,
        gc_two.reshape(-1),
        gv_three,
        gc_three.reshape(-1),
    )


def local(sensors, query_index, targets, w_one, b_one, w_two, b_two, v_one, c_one, v_two, *others):
    n_dp, n_q = lax.axis_size("dp"), lax.axis_size("query")
    units, basis_n = v_two.shape[0], w_two.shape[1]
    dense = (
        (sensors.shape[1] // n_dp) % 128 == 0
        and units == basis_n == min(512, query_index.shape[1])
        and (2 * units // PARTS) % (8 * n_dp * n_q) == 0
        and len(bits_of(n_q)) > 1
        and len(bits_of(n_dp)) == 3
    )
    chosen = local_dense if dense else local_wide
    return chosen(sensors, query_index, targets, w_one, b_one, w_two, b_two, v_one, c_one, v_two, *others)


def solution(mesh):
    placed = (
        P("dp", None),
        P(None, "query"),
        P("dp", "query"),
        P(None, "query"),
        P("query"),
        P("query", None),
        P(),
        P(),
        P(),
        P(),
        P(),
        P(),
        P(),
    )
    return jax.shard_map(
        local,
        mesh=mesh,
        in_specs=placed,
        out_specs=(
            P(),
            P("dp", "query"),
            P("query"),
            P("query", "dp"),
            P(),
            P(),
            P(),
            P(),
            P(),
            P(),
            P(),
        ),
        check_vma=False,
    )
```

```python
import functools
import math

import jax
import jax.numpy as jnp
from jax import lax
from jax.experimental import pallas as pl
from jax.experimental.pallas import tpu as pltpu
from jax.sharding import PartitionSpec as P

GRID = 128


def contract_rows(left, right, precision=None):
    return lax.dot_general(
        left,
        right,
        (((0,), (0,)), ((), ())),
        precision=precision,
        preferred_element_type=jnp.float32,
    )


def contract_cols(left, right, precision=None):
    return lax.dot_general(
        left,
        right,
        (((1,), (1,)), ((), ())),
        precision=precision,
        preferred_element_type=jnp.float32,
    )


def trunk_forward(coords, v_one, c_one, v_two, c_two, v_three, c_three):
    first_act = jnp.tanh(
        coords[0][:, None] * v_one[0][None, :] + coords[1][:, None] * v_one[1][None, :] + c_one
    )
    first_b = first_act.astype(jnp.bfloat16)
    second_act = jnp.tanh(jnp.dot(first_b, v_two, preferred_element_type=jnp.float32) + c_two)
    second_b = second_act.astype(jnp.bfloat16)
    basis_full = jnp.dot(second_b, v_three, preferred_element_type=jnp.float32) + c_three
    return (first_act, first_b, second_act, second_b, basis_full.astype(jnp.bfloat16))


def swap(value, axis, mask):
    count = lax.axis_size(axis)
    return lax.ppermute(value, axis, [(i, i ^ mask) for i in range(count)])


def bits_of(count):
    return [1 << b for b in range(count.bit_length() - 1)]


def gather_xor(value, axis, masks):
    blocks, offsets = value, [0]
    for mask in masks:
        blocks = jnp.concatenate([blocks, swap(blocks, axis, mask)], axis=0)
        offsets = offsets + [o ^ mask for o in offsets]
    return blocks, offsets


def split_pair(value):
    high = lax.reduce_precision(value, 8, 7)
    return high.astype(jnp.bfloat16), (value - high).astype(jnp.bfloat16)


def trunk_backward(coords, first_act, first_b, second_act, second_b, grad_basis, v_two, v_three):
    basis_hi, basis_lo = split_pair(grad_basis)
    grad_v_three = contract_rows(second_b, basis_hi) + contract_rows(second_b, basis_lo)
    grad_c_three = jnp.sum(grad_basis, axis=0)
    grad_second = (contract_cols(basis_hi, v_three) + contract_cols(basis_lo, v_three)) * (
        1.0 - second_act * second_act
    )
    second_hi, second_lo = split_pair(grad_second)
    grad_v_two = contract_rows(first_b, second_hi) + contract_rows(first_b, second_lo)
    grad_c_two = jnp.sum(grad_second, axis=0)
    grad_first = (contract_cols(second_hi, v_two) + contract_cols(second_lo, v_two)) * (
        1.0 - first_act * first_act
    )
    grad_v_one = jnp.stack(
        [jnp.sum(coords[0][:, None] * grad_first, axis=0), jnp.sum(coords[1][:, None] * grad_first, axis=0)]
    )
    grad_c_one = jnp.sum(grad_first, axis=0)
    return (grad_v_one, grad_c_one, grad_v_two, grad_c_two, grad_v_three, grad_c_three)


def local_wide(
    sensors,
    query_index,
    targets,
    w_one,
    b_one,
    w_two,
    b_two,
    v_one,
    c_one,
    v_two,
    c_two,
    v_three,
    c_three,
):
    dp_count, q_count = lax.axis_size("dp"), lax.axis_size("query")
    func_rows = sensors.shape[0]
    query_rows = query_index.shape[1]
    count_all = func_rows * dp_count * query_rows * q_count
    grad_scale = 64.0 / math.sqrt(count_all)
    inv_scale = 1.0 / math.sqrt(w_two.shape[1])
    dp_me, q_me = lax.axis_index("dp"), lax.axis_index("query")
    dp_bits, q_bits = bits_of(dp_count), bits_of(q_count)
    half = func_rows // 2
    parity = lax.rem(q_me, 2)
    mine = parity * half
    other = half - mine

    w_two_all, _ = gather_xor(w_two, "query", q_bits[::-1])
    sensor_cols = sensors.shape[1] // dp_count
    sensors_half = lax.dynamic_slice_in_dim(sensors, mine, half, 0)
    held = []
    for offset in range(dp_count):
        start = jnp.bitwise_xor(dp_me, offset) * sensor_cols
        block = lax.dynamic_slice_in_dim(sensors_half, start, sensor_cols, 1)
        held.append(block if offset == 0 else swap(block, "dp", offset))
    sensors_mine = jnp.concatenate(held, axis=0)
    sensors_other = swap(sensors_mine, "query", 1)

    hidden = jnp.tanh(jnp.dot(sensors, w_one, preferred_element_type=jnp.float32) + b_one)
    hidden_b = hidden.astype(jnp.bfloat16)
    hidden_all, _ = gather_xor(hidden_b, "query", q_bits[::-1])
    hidden_wide = jnp.concatenate(
        [hidden_all[i * func_rows : (i + 1) * func_rows] for i in range(q_count)], axis=1
    )

    coords = query_index.astype(jnp.float32) / (GRID - 1)
    first_act, first_b, second_act, second_b, basis_b = trunk_forward(
        coords, v_one, c_one, v_two, c_two, v_three, c_three
    )

    coeffs = jnp.dot(hidden_wide, w_two_all, preferred_element_type=jnp.float32) + b_two
    coeffs_b = coeffs.astype(jnp.bfloat16)
    prediction = contract_cols(coeffs_b, basis_b) * inv_scale
    misfit = prediction - targets.astype(jnp.float32)
    loss_part = jnp.sum(misfit * misfit)
    misfit_b = (misfit * grad_scale).astype(jnp.bfloat16)

    partial = jnp.dot(misfit_b, basis_b, preferred_element_type=jnp.float32) * inv_scale
    running = lax.dynamic_slice_in_dim(partial, mine, half, 0) + swap(
        lax.dynamic_slice_in_dim(partial, other, half, 0), "query", 1
    )
    for mask in q_bits[1:]:
        running = running + swap(running, "query", mask)
    running_b = running.astype(jnp.bfloat16)
    grad_coeffs_b = jnp.concatenate([running_b, swap(running_b, "query", 1)], axis=0)

    def in_order(value):
        return jnp.concatenate(
            [
                lax.dynamic_slice_in_dim(value, mine, half, 0),
                lax.dynamic_slice_in_dim(value, other, half, 0),
            ],
            axis=0,
        )

    hidden_o = in_order(hidden)
    hidden_bo = in_order(hidden_b)
    grad_pre = contract_cols(grad_coeffs_b, w_two) * (1.0 - hidden_o * hidden_o)
    grad_pre_b = grad_pre.astype(jnp.bfloat16)
    wide_first = dp_bits[1:][::-1] + dp_bits[:1]
    wide_last = dp_bits[:1] + dp_bits[1:][::-1]
    sides = []
    for rows, masks in ((grad_pre_b[:half], wide_first), (grad_pre_b[half:], wide_last)):
        blocks, offsets = gather_xor(rows, "dp", masks)
        sides.append(
            jnp.concatenate(
                [blocks[offsets.index(o) * half : (offsets.index(o) + 1) * half] for o in range(dp_count)],
                axis=0,
            )
        )
    grad_w_one = contract_rows(
        jnp.concatenate([sensors_mine, sensors_other], axis=0), jnp.concatenate(sides, axis=0)
    )

    rest = contract_rows(grad_coeffs_b, hidden_bo)
    bias_sum = jnp.broadcast_to(jnp.sum(grad_pre, axis=0)[None, :], (8, grad_pre.shape[1]))
    for mask in dp_bits[::-1]:
        rows = rest.shape[0] // 2
        upper = jnp.bitwise_and(dp_me, mask) // mask
        keep = lax.dynamic_slice_in_dim(rest, upper * rows, rows, 0)
        give = lax.dynamic_slice_in_dim(rest, (1 - upper) * rows, rows, 0)
        both = jnp.concatenate([keep, bias_sum], axis=0) + swap(
            jnp.concatenate([give, bias_sum], axis=0), "dp", mask
        )
        rest, bias_sum = both[:rows], both[rows:]
    grad_w_two = rest.T
    grad_b_one = bias_sum[0]

    trunk_parts = trunk_backward(
        coords, first_act, first_b, second_act, second_b, inv_scale * contract_rows(misfit_b, coeffs_b), v_two, v_three
    )
    loss_sum, grad_b_two, *sums = lax.psum(
        (loss_part, jnp.sum(partial, axis=0)) + trunk_parts, ("dp", "query")
    )
    return (loss_sum / count_all, grad_w_one, grad_b_one, grad_w_two, grad_b_two, *sums)


MESH = pl.DeviceIdType.MESH
F32, BF16 = jnp.float32, jnp.bfloat16
def natural(left, right):
    return jnp.dot(left, right, preferred_element_type=F32)


def lanes_summed(value):
    total = value[:, :128]
    for start in range(128, value.shape[1], 128):
        total = total + value[:, start : start + 128]
    return total


class Trunk:
    def __init__(self, partial, landing, total, base, rows, bits, me, flip, bit, line, launch, remote):
        self.partial, self.landing, self.total = partial, landing, total
        self.me, self.flip, self.bit, self.line = me, flip, bit, line
        self.launch, self.remote = launch, remote
        self.orders = [bits, [bits[0]] + bits[1:][::-1]]
        self.size = rows // len(self.orders)
        self.offs = [base + p * self.size for p in range(len(self.orders))]
        self.ins = list(self.offs)
        self.flight = []

    def span(self, start, size):
        return pl.ds(pl.multiple_of(start, 8), size)

    def wait(self):
        for copy in self.flight:
            copy.wait_recv()
        self.flight = []

    def start(self, k):
        size = self.size // 2
        for p, order in enumerate(self.orders):
            axis, mask = order[k]
            up = self.bit(self.me[axis], mask)
            give = self.span(self.offs[p] + (1 - up) * size, size)
            land = self.landing.at[self.ins[p] : self.ins[p] + size, :]
            peer = self.flip(self.me[axis], mask)
            self.flight.append(self.launch(self.remote(self.partial.at[give, :], land, axis, peer)))
            self.offs[p] = self.offs[p] + up * size

    def end(self, k):
        size = self.size = self.size // 2
        for p in range(len(self.orders)):
            self.flight[p].wait_recv()
            keep = self.span(self.offs[p], size)
            self.partial[keep, :] += self.landing[self.ins[p] : self.ins[p] + size, :]
            self.ins[p] += size
        self.flight = []

    def line_start(self):
        at, count = self.line
        size = self.size // count
        for p in range(len(self.orders)):
            for k in range(1, count):
                to = self.flip(at, k)
                give = self.span(self.offs[p] + to * size, size)
                first = self.ins[p] + (k - 1) * size
                land = self.landing.at[first : first + size, :]
                copy = self.remote(self.partial.at[give, :], land, "dp", self.flip(self.me["dp"], 2 * k))
                self.flight.append(self.launch(copy))

    def line_end(self):
        at, count = self.line
        size = self.size = self.size // count
        self.wait()
        for p in range(len(self.orders)):
            self.offs[p] = self.offs[p] + at * size
            keep = self.span(self.offs[p], size)
            value = self.partial[keep, :]
            for k in range(1, count):
                first = self.ins[p] + (k - 1) * size
                value = value + self.landing[first : first + size, :]
            self.total[keep, :] = value

    def back_line_start(self):
        at, count = self.line
        for p in range(len(self.orders)):
            mine = self.total.at[self.span(self.offs[p], self.size), :]
            for k in range(1, count):
                self.flight.append(self.launch(self.remote(mine, mine, "dp", self.flip(self.me["dp"], 2 * k))))
            self.offs[p] = self.offs[p] - at * self.size

    def back_line_end(self):
        self.wait()
        self.size *= self.line[1]

    def back_start(self, k):
        for p, order in enumerate(self.orders):
            axis, mask = order[k]
            mine = self.total.at[self.span(self.offs[p], self.size), :]
            self.flight.append(self.launch(self.remote(mine, mine, axis, self.flip(self.me[axis], mask))))
            self.offs[p] = self.offs[p] - self.bit(self.me[axis], mask) * self.size

    def back_end(self, k):
        self.wait()
        self.size *= 2


def step_kernel(
    n_dp,
    n_q,
    count_all,
    sensors_h,
    qidx,
    targets_h,
    w_one_h,
    b_one,
    w_two_h,
    b_two,
    v_one,
    c_one,
    v_two_h,
    c_two,
    v_three_h,
    c_three,
    loss_o,
    gw_one_o,
    gb_one_o,
    gw_two_o,
    gb_two_o,
    gv_one_o,
    gc_one_o,
    gv_two_o,
    gc_two_o,
    gv_three_o,
    gc_three_o,
    sens,
    tgt,
    w_one,
    w_two,
    v_two,
    v_three,
    v_two_t,
    v_three_t,
    hid,
    hid_b,
    first,
    second,
    first_b,
    second_b,
    basis,
    coef_b,
    coef_bt,
    mis_b,
    gco,
    gco_in,
    gco_run,
    gco_rx,
    gco_b,
    pre_all,
    sens_all,
    rest,
    rest_in,
    rest_line,
    bias,
    bias_in,
    trunk,
    trunk_in,
    trunk_out,
    small,
    small_in,
    sums,
    loss_row,
    g_two_b,
    acc,
    acc_in,
    load_sem,
    send_sem,
    recv_sem,
):
    func_rows, sensor_all = sens.shape
    hidden = w_one.shape[1]
    units, queries = first.shape
    basis_n = coef_b.shape[1]
    cols_dp = sensor_all // n_dp
    block = min(512, queries)
    blocks = queries // block
    inv_scale = 1.0 / math.sqrt(basis_n)
    grad_scale = 64.0 / math.sqrt(count_all)
    dp, q = lax.axis_index("dp"), lax.axis_index("query")
    me = {"dp": dp, "query": q}
    q_bits = bits_of(n_q)
    half = func_rows // 2
    part = lax.rem(q, 2)
    mine = pl.multiple_of(part * half, 8)
    other = pl.multiple_of((1 - part) * half, 8)
    side, line_at, line_n = lax.rem(dp, 2), dp // 2, n_dp // 2

    def bit(index, mask):
        return lax.rem(index // mask, 2)

    def flip(index, offset):
        result = index
        for mask in bits_of(n_dp * n_q):
            if offset & mask:
                result = result + mask * (1 - 2 * bit(index, mask))
        return result

    used = [0]

    def remote(src, dst, axis, peer):
        k = used[0]
        used[0] = k + 1
        return pltpu.make_async_remote_copy(
            src_ref=src,
            dst_ref=dst,
            send_sem=send_sem.at[k],
            recv_sem=recv_sem.at[k],
            device_id={axis: peer},
            device_id_type=MESH,
        )

    sent = []

    def launch(copy):
        copy.start()
        sent.append(copy)
        return copy

    pair = flip(dp, 1)
    barrier = pltpu.get_barrier_semaphore()
    dp_peers = [pair] + [flip(dp, 2 * k) for k in range(1, line_n)]
    for peer in dp_peers:
        pl.semaphore_signal(barrier, inc=1, device_id={"dp": peer}, device_id_type=MESH)
    for mask in q_bits:
        pl.semaphore_signal(barrier, inc=1, device_id={"query": flip(q, mask)}, device_id_type=MESH)

    def sensor_block(index, rows):
        return sensors_h.at[rows, pl.ds(pl.multiple_of(index * cols_dp, 128), cols_dp)]

    every = pl.ds(0, func_rows)
    loads = {}
    for k, (name, src, dst) in enumerate(
        (
            ("w_one", w_one_h, w_one),
            ("sens", sensors_h, sens),
            ("v_two", v_two_h, v_two),
            ("v_three", v_three_h, v_three),
            ("w_two", w_two_h, w_two.at[q]),
            ("targets", targets_h, tgt),
            ("own0", sensor_block(line_at * 2, every), sens_all.at[line_at * 2]),
            ("own1", sensor_block(line_at * 2 + 1, every), sens_all.at[line_at * 2 + 1]),
        )
    ):
        loads[name] = pltpu.make_async_copy(src, dst, load_sem.at[k])
        loads[name].start()
    pl.semaphore_wait(barrier, len(dp_peers) + len(q_bits))

    q_order = q_bits[::-1]
    w_half = hidden // 2
    w_rows = pl.ds(pl.multiple_of(side * w_half, 16), w_half)
    q_far = flip(q, q_order[0])
    w_far = launch(remote(w_two_h.at[w_rows, :], w_two.at[q, w_rows, :], "query", q_far))
    bulk = []
    rows_mine = pl.ds(mine, half)
    share_n = func_rows // n_q

    def rows_of(member):
        return pl.ds(pl.multiple_of(member * share_n, 16), share_n)

    for k in [1] + list(range(line_n - 1, 1, -1)):
        to = flip(line_at, k)
        for s in range(2):
            copy = remote(
                sensor_block(to * 2 + s, rows_of(q)), sens_all.at[line_at * 2 + s, rows_of(q), :], "dp", flip(dp, 2 * k)
            )
            bulk.append((to * 2 + s, launch(copy)))

    def pass_on(index, member, mask):
        ref = sens_all.at[index, rows_of(member), :]
        return launch(remote(ref, ref, "query", flip(q, mask)))

    far, passed = [], []

    def pass_far(k):
        for index, copy in bulk[2 * k : 2 * k + 2]:
            copy.wait_recv()
            far.append((index, pass_on(index, q, q_order[0])))
            passed.append(pass_on(index, q, 1))


    loads["w_one"].wait()
    loads["sens"].wait()
    act = jnp.tanh(natural(sens[...], w_one[...]) + b_one[...])
    hid[...] = act
    hid_b[q] = act.astype(BF16)
    h_far = launch(remote(hid_b.at[q], hid_b.at[q], "query", q_far))

    loads["v_two"].wait()
    loads["v_three"].wait()
    v_two_t[...] = v_two[...].astype(F32).T.astype(BF16)
    v_three_t[...] = v_three[...].astype(F32).T.astype(BF16)
    columns = jnp.concatenate(
        [v_one[...], c_one[...], c_two[...], c_three[...], jnp.zeros((3, units), F32)], axis=0
    ).T

    def coords_of(span):
        x = qidx[0:1, span].astype(F32) / (GRID - 1)
        y = qidx[1:2, span].astype(F32) / (GRID - 1)
        return x, y

    def forward(i, carry):
        span = pl.ds(pl.multiple_of(i * block, 128), block)
        x, y = coords_of(span)
        one = jnp.tanh(columns[:, 0:1] * x + columns[:, 1:2] * y + columns[:, 2:3])
        first[:, span] = one
        one_b = one.astype(BF16)
        first_b[:, span] = one_b
        two = jnp.tanh(natural(v_two_t[...], one_b) + columns[:, 3:4])
        second[:, span] = two
        two_b = two.astype(BF16)
        second_b[:, span] = two_b
        basis[:, span] = (natural(v_three_t[...], two_b) + columns[:, 4:5]).astype(BF16)
        return carry

    def spread(buffer, held, masks):
        group = []
        for mask in masks:
            for copy in group:
                copy.wait_recv()
            group = [
                launch(remote(buffer.at[flip(q, o)], buffer.at[flip(q, o)], "query", flip(q, mask))) for o in held
            ]
            held = held + [o ^ mask for o in held]
        return group

    lax.fori_loop(0, blocks // 2, forward, 0)
    w_far.wait_recv()
    w_pair = launch(remote(w_two.at[q_far, w_rows, :], w_two.at[q_far, w_rows, :], "dp", pair))
    lax.fori_loop(blocks // 2, blocks, forward, 0)
    loads["w_two"].wait()
    h_far.wait_recv()
    h_last = spread(hid_b, [0, q_order[0]], q_order[1:])
    w_pair.wait_recv()
    w_last = spread(w_two, [0, q_order[0]], q_order[1:])
    for copy in h_last + w_last:
        copy.wait_recv()

    pass_far(0)
    coef = natural(hid_b[0], w_two[0])
    for i in range(1, n_q):
        coef = coef + natural(hid_b[i], w_two[i])
    coef = coef + b_two[...]
    coef_b[...] = coef.astype(BF16)
    coef_bt[...] = coef.T.astype(BF16)

    loads["targets"].wait()
    gco[...] = jnp.zeros_like(gco)
    loss_row[...] = jnp.zeros_like(loss_row)

    def fit(i, carry):
        span = pl.ds(pl.multiple_of(i * block, 128), block)
        base = basis[:, span]
        miss = natural(coef_b[...], base) * inv_scale - tgt[:, span].astype(F32)
        loss_row[0:1, :] += jnp.sum(miss * miss, axis=0, keepdims=True)
        miss_b = (miss * grad_scale).astype(BF16)
        mis_b[:, span] = miss_b
        gco[...] += contract_cols(miss_b, base)
        return carry

    lax.fori_loop(0, blocks, fit, 0)
    gco[...] = gco[...] * inv_scale
    core_step = launch(remote(gco.at[pl.ds(other, half), :], gco_in, "query", flip(q, 1)))
    gb_two_row = jnp.sum(gco[...], axis=0, keepdims=True)
    trunk[...] = jnp.zeros_like(trunk)
    sums[...] = jnp.zeros_like(sums)
    core_step.wait_recv()
    gco_run[0] = gco[rows_mine, :] + gco_in[...]
    reduce_steps = [launch(remote(gco_run.at[0], gco_rx.at[0], "query", flip(q, q_bits[1])))]

    bits = [("query", m) for m in q_bits] + [("dp", 1)]
    place = (bits, me, flip, bit, (line_at, line_n), launch, remote)
    three = Trunk(trunk, trunk_in, trunk_out, 0, units, *place)
    two_ = Trunk(trunk, trunk_in, trunk_out, units, units, *place)

    def backward_top(i, carry):
        span = pl.ds(pl.multiple_of(i * block, 128), block)
        g_base = natural(coef_bt[...], mis_b[:, span]) * inv_scale
        sums[0] += lanes_summed(g_base)
        g_base = g_base.astype(BF16)
        trunk[:units, :] += contract_cols(second_b[:, span], g_base)
        two = second[:, span]
        g_two = natural(v_three[...], g_base) * (1.0 - two * two)
        sums[1] += lanes_summed(g_two)
        g_two_b[:, span] = g_two.astype(BF16)
        return carry

    def backward_low(i, carry):
        span = pl.ds(pl.multiple_of(i * block, 128), block)
        x, y = coords_of(span)
        g_two = g_two_b[:, span]
        trunk[units:, :] += contract_cols(first_b[:, span], g_two)
        one = first[:, span]
        g_one = natural(v_two[...], g_two) * (1.0 - one * one)
        sums[2] += lanes_summed(g_one)
        sums[3] += lanes_summed(g_one * x)
        sums[4] += lanes_summed(g_one * y)
        return carry

    lax.fori_loop(0, blocks, backward_top, 0)
    three.start(0)
    lax.fori_loop(0, blocks // 2, backward_low, 0)
    three.end(0)
    three.start(1)
    lax.fori_loop(blocks // 2, blocks, backward_low, 0)

    for k in range(len(q_bits) - 1):
        reduce_steps[k].wait_recv()
        total = gco_run[k] + gco_rx[k]
        if k + 2 < len(q_bits):
            gco_run[k + 1] = total
            reduce_steps.append(launch(remote(gco_run.at[k + 1], gco_rx.at[k + 1], "query", flip(q, q_bits[k + 2]))))
    gco_b[rows_mine, :] = total.astype(BF16)
    share = launch(remote(gco_b.at[rows_mine, :], gco_b.at[rows_mine, :], "query", flip(q, 1)))

    two_.start(0)
    lane = lax.broadcasted_iota(jnp.int32, (units, 128), 1)
    table = jnp.zeros((units, 128), F32)
    for row, which in enumerate((3, 4, 2, 1, 0)):
        table = jnp.where(lane == row, jnp.sum(sums[which], axis=1, keepdims=True), table)
    rows = table.T[0:8]
    line = lax.broadcasted_iota(jnp.int32, rows.shape, 0)
    rows = jnp.where(line == 5, gb_two_row, rows)
    rows = jnp.where(line == 6, loss_row[0:1, :], rows)
    small[0] = rows
    s_flight = []

    def small_start(k):
        axis, mask = bits[k]
        s_flight.append(launch(remote(small.at[k], small_in.at[k], axis, flip(me[axis], mask))))

    def small_end(k):
        s_flight.pop().wait_recv()
        small[k + 1] = small[k] + small_in[k]

    def small_line_start():
        k = len(bits)
        for o in range(1, line_n):
            s_flight.append(launch(remote(small.at[k], small_in.at[k + o - 1], "dp", flip(dp, 2 * o))))

    def small_line_end():
        k = len(bits)
        total = small[k]
        for o in range(1, line_n):
            s_flight[o - 1].wait_recv()
            total = total + small_in[k + o - 1]
        return total

    small_start(0)

    share.wait_recv()
    act = hid[...]
    g_pre = contract_cols(gco_b[...], w_two[q]) * (1.0 - act * act)
    pre_all[line_at] = g_pre.astype(BF16)

    chunks = 2
    rows_c = func_rows // chunks

    def hop(at, c, peer):
        ref = pre_all.at[jnp.clip(at, 0, line_n - 1), c * rows_c : (c + 1) * rows_c, :]
        return remote(ref, ref, "dp", peer)

    to_right = jnp.minimum(dp + 2, n_dp - 2 + side)
    to_left = jnp.maximum(dp - 2, side)
    steps = line_n - 1
    rights = [[hop(line_at - s, c, to_right) for c in range(chunks)] for s in range(steps)]
    lefts = [[hop(line_at + s, c, to_left) for c in range(chunks)] for s in range(steps)]

    def sends_right(s):
        return jnp.logical_and(line_at - s >= 0, line_at < line_n - 1)

    def sends_left(s):
        return jnp.logical_and(line_at + s < line_n, line_at > 0)

    for c in range(chunks):
        pl.when(sends_right(0))(rights[0][c].start)
        pl.when(sends_left(0))(lefts[0][c].start)

    def gather_step(s):
        for c in range(chunks):

            @pl.when(line_at - 1 - s >= 0)
            def _():
                rights[s][c].wait_recv()
                if s + 1 < steps:
                    pl.when(sends_right(s + 1))(rights[s + 1][c].start)

            @pl.when(line_at + 1 + s < line_n)
            def _():
                lefts[s][c].wait_recv()
                if s + 1 < steps:
                    pl.when(sends_left(s + 1))(lefts[s + 1][c].start)

    bias[0] = jnp.broadcast_to(jnp.sum(g_pre, axis=0, keepdims=True), bias.shape[1:])
    gco_bt = gco_b[...].astype(F32).T.astype(BF16)
    rest_all = natural(gco_bt, hid_b[q])
    rows_dp = basis_n // n_dp
    for j in range(n_dp):
        rest[j % 2, j // 2] = rest_all[j * rows_dp : (j + 1) * rows_dp, :]
    two_.end(0)
    two_.start(1)
    small_end(0)
    small_start(1)
    three.end(1)
    three.start(2)
    for k in range(1, line_n - 1):
        pass_far(k)
    gather_step(0)
    two_.end(1)
    two_.start(2)
    small_end(1)
    small_start(2)
    three.end(2)
    three.line_start()
    rest_pair = [
        launch(remote(rest.at[1 - side], rest_in, "dp", pair)),
        launch(remote(bias.at[0], bias_in.at[0], "dp", pair)),
    ]
    for s in range(1, steps - 1):
        gather_step(s)
    two_.end(2)
    two_.line_start()
    small_end(2)
    small_line_start()
    three.line_end()
    three.back_line_start()
    loads["own0"].wait()
    loads["own1"].wait()
    for index, copy in far:
        copy.wait_recv()
        passed.append(pass_on(index, q_far, 1))
    gather_step(steps - 1)
    for copy in passed:
        copy.wait_recv()

    pieces = 4
    cols_p = cols_dp // pieces
    across = []

    def sum_of(whose, first_col, width):
        cols = slice(first_col, first_col + width)

        def body(j, carry):
            index = j * 2 + (1 - side if whose else side)
            return carry + contract_rows(sens_all[index, :, cols], pre_all[j])

        acc[whose, cols, :] = lax.fori_loop(0, line_n, body, jnp.zeros((width, hidden), F32))

    def send_across(piece):
        cols = slice(piece * cols_p, (piece + 1) * cols_p)
        across.append(launch(remote(acc.at[1, cols, :], acc_in.at[cols, :], "dp", pair)))

    sum_of(1, 0, 2 * cols_p)
    send_across(0)
    send_across(1)
    sum_of(1, 2 * cols_p, 2 * cols_p)
    for copy in rest_pair:
        copy.wait_recv()
    rest[side] += rest_in[...]
    bias[1] = bias[0] + bias_in[0]
    rest_flight = []
    for k in range(1, line_n):
        peer = flip(dp, 2 * k)
        rest_flight.append(launch(remote(rest.at[side, flip(line_at, k)], rest_line.at[k - 1], "dp", peer)))
        rest_flight.append(launch(remote(bias.at[1], bias_in.at[k], "dp", peer)))
    three.back_line_end()
    three.back_start(2)
    send_across(2)
    two_.line_end()
    two_.back_line_start()
    three.back_end(2)
    three.back_start(1)
    send_across(3)
    two_.back_line_end()
    two_.back_start(2)
    sum_of(0, 0, cols_dp)
    for copy in rest_flight:
        copy.wait_recv()
    final_rest = rest[side, line_at]
    final_bias = bias[1]
    for k in range(1, line_n):
        final_rest = final_rest + rest_line[k - 1]
        final_bias = final_bias + bias_in[k]
    gw_two_o[...] = final_rest
    gb_one_o[...] = final_bias[0:1, :]
    final = small_line_end()
    gv_one_o[...] = final[0:2]
    gc_one_o[...] = final[2:3]
    gc_two_o[...] = final[3:4]
    gc_three_o[...] = final[4:5]
    gb_two_o[...] = final[5:6]
    loss_o[...] = jnp.broadcast_to(jnp.sum(final[6:7], axis=1, keepdims=True) * (1.0 / count_all), loss_o.shape)
    three.back_end(1)
    three.back_start(0)
    two_.back_end(2)
    two_.back_start(1)
    three.back_end(0)
    outs = [pltpu.make_async_copy(trunk_out.at[:units, :], gv_three_o, load_sem.at[0])]
    outs[-1].start()
    two_.back_end(1)
    two_.back_start(0)
    for copy in across:
        copy.wait_recv()
    acc[0] += acc_in[...]
    outs.append(pltpu.make_async_copy(acc.at[0], gw_one_o, load_sem.at[1]))
    outs[-1].start()
    two_.back_end(0)
    outs.append(pltpu.make_async_copy(trunk_out.at[units:, :], gv_two_o, load_sem.at[2]))
    outs[-1].start()
    for copy in sent:
        copy.wait_send()
    for s in range(steps):
        for c in range(chunks):
            pl.when(sends_right(s))(rights[s][c].wait_send)
            pl.when(sends_left(s))(lefts[s][c].wait_send)
    for copy in outs:
        copy.wait()


def hand_over(*refs):
    count = (len(refs) - 2) // 3
    near, sems_in, sems_out = refs[2 * count : 3 * count], refs[-2], refs[-1]
    ins = [pltpu.make_async_copy(refs[k], near[k], sems_in.at[k]) for k in range(count)]
    outs = [pltpu.make_async_copy(near[k], refs[count + k], sems_out.at[k]) for k in range(count)]
    for copy in ins:
        copy.start()
    for came, goes in zip(ins, outs):
        came.wait()
        goes.start()
    for copy in outs:
        copy.wait()


def local_dense(
    sensors, query_index, targets, w_one, b_one, w_two, b_two, v_one, c_one, v_two, c_two, v_three, c_three
):
    n_dp, n_q = lax.axis_size("dp"), lax.axis_size("query")
    func_rows, sensor_all = sensors.shape
    queries = query_index.shape[1]
    hidden, basis_n = w_two.shape
    units = v_two.shape[0]
    cols_dp = sensor_all // n_dp
    count_all = func_rows * n_dp * queries * n_q
    line_n, q_n = n_dp // 2, len(bits_of(n_q))
    half = func_rows // 2
    rows_dp = basis_n // n_dp
    hbm, vmem = pl.BlockSpec(memory_space=pl.ANY), pl.BlockSpec(memory_space=pltpu.VMEM)
    sem_n = 160

    def row(value):
        return value.reshape(1, -1)

    def result(*shape):
        return jax.ShapeDtypeStruct(shape, F32)

    results = (
        result(1, 128),
        result(cols_dp, hidden),
        result(1, hidden),
        result(rows_dp, hidden),
        result(1, basis_n),
        result(2, units),
        result(1, units),
        result(units, units),
        result(1, units),
        result(units, basis_n),
        result(1, basis_n),
    )
    outs = pl.pallas_call(
        functools.partial(step_kernel, n_dp, n_q, count_all),
        out_shape=results,
        in_specs=[hbm, vmem, hbm, hbm, vmem, hbm, vmem, vmem, vmem, hbm, vmem, hbm, vmem],
        out_specs=(vmem, hbm, vmem, vmem, vmem, vmem, vmem, hbm, vmem, hbm, vmem),
        scratch_shapes=[
            pltpu.VMEM((func_rows, sensor_all), BF16),
            pltpu.VMEM((func_rows, queries), BF16),
            pltpu.VMEM((sensor_all, hidden), BF16),
            pltpu.VMEM((n_q, hidden, basis_n), BF16),
            pltpu.VMEM((units, units), BF16),
            pltpu.VMEM((units, basis_n), BF16),
            pltpu.VMEM((units, units), BF16),
            pltpu.VMEM((basis_n, units), BF16),
            pltpu.VMEM((func_rows, hidden), F32),
            pltpu.VMEM((n_q, func_rows, hidden), BF16),
            pltpu.VMEM((units, queries), F32),
            pltpu.VMEM((units, queries), F32),
            pltpu.VMEM((units, queries), BF16),
            pltpu.VMEM((units, queries), BF16),
            pltpu.VMEM((basis_n, queries), BF16),
            pltpu.VMEM((func_rows, basis_n), BF16),
            pltpu.VMEM((basis_n, func_rows), BF16),
            pltpu.VMEM((func_rows, queries), BF16),
            pltpu.VMEM((func_rows, basis_n), F32),
            pltpu.VMEM((half, basis_n), F32),
            pltpu.VMEM((q_n, half, basis_n), F32),
            pltpu.VMEM((q_n, half, basis_n), F32),
            pltpu.VMEM((func_rows, basis_n), BF16),
            pltpu.VMEM((line_n, func_rows, hidden), BF16),
            pltpu.VMEM((n_dp, func_rows, cols_dp), BF16),
            pltpu.VMEM((2, line_n, rows_dp, hidden), F32),
            pltpu.VMEM((line_n, rows_dp, hidden), F32),
            pltpu.VMEM((line_n, rows_dp, hidden), F32),
            pltpu.VMEM((2, 8, hidden), F32),
            pltpu.VMEM((line_n, 8, hidden), F32),
            pltpu.VMEM((2 * units, basis_n), F32),
            pltpu.VMEM((2 * units, basis_n), F32),
            pltpu.VMEM((2 * units, basis_n), F32),
            pltpu.VMEM((q_n + 2, 8, units), F32),
            pltpu.VMEM((q_n + line_n, 8, units), F32),
            pltpu.VMEM((5, units, 128), F32),
            pltpu.VMEM((8, min(512, queries)), F32),
            pltpu.VMEM((units, queries), BF16),
            pltpu.VMEM((2, cols_dp, hidden), F32),
            pltpu.VMEM((cols_dp, hidden), F32),
            pltpu.SemaphoreType.DMA((8,)),
            pltpu.SemaphoreType.DMA((sem_n,)),
            pltpu.SemaphoreType.DMA((sem_n,)),
        ],
        compiler_params=pltpu.CompilerParams(
            collective_id=0, has_side_effects=True, vmem_limit_bytes=67043328
        ),
        name="step",
    )(
        sensors,
        query_index,
        targets,
        w_one,
        row(b_one),
        w_two,
        row(b_two),
        v_one,
        row(c_one),
        v_two,
        row(c_two),
        v_three,
        row(c_three),
    )
    outs = pl.pallas_call(
        hand_over,
        out_shape=results,
        in_specs=[hbm] * len(results),
        out_specs=(hbm,) * len(results),
        scratch_shapes=[pltpu.VMEM(value.shape, F32) for value in results]
        + [pltpu.SemaphoreType.DMA((len(results),))] * 2,
        name="hand_over",
    )(*outs)
    loss, gw_one, gb_one, gw_two, gb_two, gv_one, gc_one, gv_two, gc_two, gv_three, gc_three = outs
    return (
        loss[0, 0],
        gw_one,
        gb_one.reshape(-1),
        gw_two.T,
        gb_two.reshape(-1),
        gv_one,
        gc_one.reshape(-1),
        gv_two,
        gc_two.reshape(-1),
        gv_three,
        gc_three.reshape(-1),
    )


def local(sensors, query_index, targets, w_one, b_one, w_two, b_two, v_one, c_one, v_two, *others):
    n_dp, n_q = lax.axis_size("dp"), lax.axis_size("query")
    units, basis_n = v_two.shape[0], w_two.shape[1]
    dense = (
        (sensors.shape[1] // n_dp) % 128 == 0
        and units == basis_n == min(512, query_index.shape[1])
        and (units // 2) % (8 * n_dp * n_q) == 0
        and sensors.shape[0] % (16 * n_q) == 0
        and len(bits_of(n_q)) == 2
        and len(bits_of(n_dp)) == 3
    )
    chosen = local_dense if dense else local_wide
    return chosen(sensors, query_index, targets, w_one, b_one, w_two, b_two, v_one, c_one, v_two, *others)


def solution(mesh):
    placed = (
        P("dp", None),
        P(None, "query"),
        P("dp", "query"),
        P(None, "query"),
        P("query"),
        P("query", None),
        P(),
        P(),
        P(),
        P(),
        P(),
        P(),
        P(),
    )
    return jax.shard_map(
        local,
        mesh=mesh,
        in_specs=placed,
        out_specs=(
            P(),
            P("dp", "query"),
            P("query"),
            P("query", "dp"),
            P(),
            P(),
            P(),
            P(),
            P(),
            P(),
            P(),
        ),
        check_vma=False,
    )
```

```python
import functools
import math

import jax
import jax.numpy as jnp
from jax import lax
from jax.experimental import pallas as pl
from jax.experimental.pallas import tpu as pltpu
from jax.sharding import PartitionSpec as P

GRID = 128


def contract_rows(left, right, precision=None):
    return lax.dot_general(
        left,
        right,
        (((0,), (0,)), ((), ())),
        precision=precision,
        preferred_element_type=jnp.float32,
    )


def contract_cols(left, right, precision=None):
    return lax.dot_general(
        left,
        right,
        (((1,), (1,)), ((), ())),
        precision=precision,
        preferred_element_type=jnp.float32,
    )


def trunk_forward(coords, v_one, c_one, v_two, c_two, v_three, c_three):
    first_act = jnp.tanh(
        coords[0][:, None] * v_one[0][None, :] + coords[1][:, None] * v_one[1][None, :] + c_one
    )
    first_b = first_act.astype(jnp.bfloat16)
    second_act = jnp.tanh(jnp.dot(first_b, v_two, preferred_element_type=jnp.float32) + c_two)
    second_b = second_act.astype(jnp.bfloat16)
    basis_full = jnp.dot(second_b, v_three, preferred_element_type=jnp.float32) + c_three
    return (first_act, first_b, second_act, second_b, basis_full.astype(jnp.bfloat16))


def swap(value, axis, mask):
    count = lax.axis_size(axis)
    return lax.ppermute(value, axis, [(i, i ^ mask) for i in range(count)])


def bits_of(count):
    return [1 << b for b in range(count.bit_length() - 1)]


def gather_xor(value, axis, masks):
    blocks, offsets = value, [0]
    for mask in masks:
        blocks = jnp.concatenate([blocks, swap(blocks, axis, mask)], axis=0)
        offsets = offsets + [o ^ mask for o in offsets]
    return blocks, offsets


def split_pair(value):
    high = lax.reduce_precision(value, 8, 7)
    return high.astype(jnp.bfloat16), (value - high).astype(jnp.bfloat16)


def trunk_backward(coords, first_act, first_b, second_act, second_b, grad_basis, v_two, v_three):
    basis_hi, basis_lo = split_pair(grad_basis)
    grad_v_three = contract_rows(second_b, basis_hi) + contract_rows(second_b, basis_lo)
    grad_c_three = jnp.sum(grad_basis, axis=0)
    grad_second = (contract_cols(basis_hi, v_three) + contract_cols(basis_lo, v_three)) * (
        1.0 - second_act * second_act
    )
    second_hi, second_lo = split_pair(grad_second)
    grad_v_two = contract_rows(first_b, second_hi) + contract_rows(first_b, second_lo)
    grad_c_two = jnp.sum(grad_second, axis=0)
    grad_first = (contract_cols(second_hi, v_two) + contract_cols(second_lo, v_two)) * (
        1.0 - first_act * first_act
    )
    grad_v_one = jnp.stack(
        [jnp.sum(coords[0][:, None] * grad_first, axis=0), jnp.sum(coords[1][:, None] * grad_first, axis=0)]
    )
    grad_c_one = jnp.sum(grad_first, axis=0)
    return (grad_v_one, grad_c_one, grad_v_two, grad_c_two, grad_v_three, grad_c_three)


def local_wide(
    sensors,
    query_index,
    targets,
    w_one,
    b_one,
    w_two,
    b_two,
    v_one,
    c_one,
    v_two,
    c_two,
    v_three,
    c_three,
):
    dp_count, q_count = lax.axis_size("dp"), lax.axis_size("query")
    func_rows = sensors.shape[0]
    query_rows = query_index.shape[1]
    count_all = func_rows * dp_count * query_rows * q_count
    grad_scale = 64.0 / math.sqrt(count_all)
    inv_scale = 1.0 / math.sqrt(w_two.shape[1])
    dp_me, q_me = lax.axis_index("dp"), lax.axis_index("query")
    dp_bits, q_bits = bits_of(dp_count), bits_of(q_count)
    half = func_rows // 2
    parity = lax.rem(q_me, 2)
    mine = parity * half
    other = half - mine

    w_two_all, _ = gather_xor(w_two, "query", q_bits[::-1])
    sensor_cols = sensors.shape[1] // dp_count
    sensors_half = lax.dynamic_slice_in_dim(sensors, mine, half, 0)
    held = []
    for offset in range(dp_count):
        start = jnp.bitwise_xor(dp_me, offset) * sensor_cols
        block = lax.dynamic_slice_in_dim(sensors_half, start, sensor_cols, 1)
        held.append(block if offset == 0 else swap(block, "dp", offset))
    sensors_mine = jnp.concatenate(held, axis=0)
    sensors_other = swap(sensors_mine, "query", 1)

    hidden = jnp.tanh(jnp.dot(sensors, w_one, preferred_element_type=jnp.float32) + b_one)
    hidden_b = hidden.astype(jnp.bfloat16)
    hidden_all, _ = gather_xor(hidden_b, "query", q_bits[::-1])
    hidden_wide = jnp.concatenate(
        [hidden_all[i * func_rows : (i + 1) * func_rows] for i in range(q_count)], axis=1
    )

    coords = query_index.astype(jnp.float32) / (GRID - 1)
    first_act, first_b, second_act, second_b, basis_b = trunk_forward(
        coords, v_one, c_one, v_two, c_two, v_three, c_three
    )

    coeffs = jnp.dot(hidden_wide, w_two_all, preferred_element_type=jnp.float32) + b_two
    coeffs_b = coeffs.astype(jnp.bfloat16)
    prediction = contract_cols(coeffs_b, basis_b) * inv_scale
    misfit = prediction - targets.astype(jnp.float32)
    loss_part = jnp.sum(misfit * misfit)
    misfit_b = (misfit * grad_scale).astype(jnp.bfloat16)

    partial = jnp.dot(misfit_b, basis_b, preferred_element_type=jnp.float32) * inv_scale
    running = lax.dynamic_slice_in_dim(partial, mine, half, 0) + swap(
        lax.dynamic_slice_in_dim(partial, other, half, 0), "query", 1
    )
    for mask in q_bits[1:]:
        running = running + swap(running, "query", mask)
    running_b = running.astype(jnp.bfloat16)
    grad_coeffs_b = jnp.concatenate([running_b, swap(running_b, "query", 1)], axis=0)

    def in_order(value):
        return jnp.concatenate(
            [
                lax.dynamic_slice_in_dim(value, mine, half, 0),
                lax.dynamic_slice_in_dim(value, other, half, 0),
            ],
            axis=0,
        )

    hidden_o = in_order(hidden)
    hidden_bo = in_order(hidden_b)
    grad_pre = contract_cols(grad_coeffs_b, w_two) * (1.0 - hidden_o * hidden_o)
    grad_pre_b = grad_pre.astype(jnp.bfloat16)
    wide_first = dp_bits[1:][::-1] + dp_bits[:1]
    wide_last = dp_bits[:1] + dp_bits[1:][::-1]
    sides = []
    for rows, masks in ((grad_pre_b[:half], wide_first), (grad_pre_b[half:], wide_last)):
        blocks, offsets = gather_xor(rows, "dp", masks)
        sides.append(
            jnp.concatenate(
                [blocks[offsets.index(o) * half : (offsets.index(o) + 1) * half] for o in range(dp_count)],
                axis=0,
            )
        )
    grad_w_one = contract_rows(
        jnp.concatenate([sensors_mine, sensors_other], axis=0), jnp.concatenate(sides, axis=0)
    )

    rest = contract_rows(grad_coeffs_b, hidden_bo)
    bias_sum = jnp.broadcast_to(jnp.sum(grad_pre, axis=0)[None, :], (8, grad_pre.shape[1]))
    for mask in dp_bits[::-1]:
        rows = rest.shape[0] // 2
        upper = jnp.bitwise_and(dp_me, mask) // mask
        keep = lax.dynamic_slice_in_dim(rest, upper * rows, rows, 0)
        give = lax.dynamic_slice_in_dim(rest, (1 - upper) * rows, rows, 0)
        both = jnp.concatenate([keep, bias_sum], axis=0) + swap(
            jnp.concatenate([give, bias_sum], axis=0), "dp", mask
        )
        rest, bias_sum = both[:rows], both[rows:]
    grad_w_two = rest.T
    grad_b_one = bias_sum[0]

    trunk_parts = trunk_backward(
        coords, first_act, first_b, second_act, second_b, inv_scale * contract_rows(misfit_b, coeffs_b), v_two, v_three
    )
    loss_sum, grad_b_two, *sums = lax.psum(
        (loss_part, jnp.sum(partial, axis=0)) + trunk_parts, ("dp", "query")
    )
    return (loss_sum / count_all, grad_w_one, grad_b_one, grad_w_two, grad_b_two, *sums)


MESH = pl.DeviceIdType.MESH
F32, BF16 = jnp.float32, jnp.bfloat16
def natural(left, right):
    return jnp.dot(left, right, preferred_element_type=F32)


def lanes_summed(value):
    total = value[:, :128]
    for start in range(128, value.shape[1], 128):
        total = total + value[:, start : start + 128]
    return total


class Trunk:
    def __init__(self, partial, landing, total, base, rows, order, back, me, flip, bit, line, launch, remote):
        self.partial, self.landing, self.total = partial, landing, total
        self.me, self.flip, self.bit, self.line = me, flip, bit, line
        self.launch, self.remote = launch, remote
        self.order, self.back = order, back
        self.size, self.off, self.land = rows, base, base
        self.stride = {step: rows >> (k + 1) for k, step in enumerate(order)}
        self.flight = []

    def span(self, start, size):
        return pl.ds(pl.multiple_of(start, 8), size)

    def send(self, src, dst, axis, offset):
        self.flight.append(self.launch(self.remote(src, dst, axis, self.flip(self.me[axis], offset))))

    def wait(self):
        for copy in self.flight:
            copy.wait_recv()
        self.flight = []

    def start(self, k):
        axis, mask = self.order[k]
        size = self.size // 2
        up = self.bit(self.me[axis], mask)
        give = self.span(self.off + (1 - up) * size, size)
        self.send(self.partial.at[give, :], self.landing.at[self.land : self.land + size, :], axis, mask)
        self.off = self.off + up * size

    def end(self, k):
        self.wait()
        self.size //= 2
        self.partial[self.span(self.off, self.size), :] += self.landing[self.land : self.land + self.size, :]
        self.land += self.size

    def line_start(self):
        at, count = self.line
        size = self.size // count
        for k in range(1, count):
            give = self.span(self.off + self.flip(at, k) * size, size)
            first = self.land + (k - 1) * size
            self.send(self.partial.at[give, :], self.landing.at[first : first + size, :], "dp", 2 * k)

    def line_end(self):
        at, count = self.line
        size = self.size // count
        self.wait()
        mine = self.span(self.off + at * size, size)
        value = self.partial[mine, :]
        for k in range(1, count):
            first = self.land + (k - 1) * size
            value = value + self.landing[first : first + size, :]
        self.total[mine, :] = value

    def back_line_start(self):
        at, count = self.line
        size = self.size // count
        mine = self.total.at[self.span(self.off + at * size, size), :]
        for k in range(1, count):
            self.send(mine, mine, "dp", 2 * k)
        self.held = [(self.off, self.size)]

    def back_start(self, k):
        axis, mask = step = self.back[k]
        if k == len(self.back) - 1:
            rows = self.stride[step]
            self.held = [(self.held[0][0] // rows * rows, rows)]
        for off, size in self.held:
            block = self.total.at[self.span(off, size), :]
            self.send(block, block, axis, mask)
        turn = self.stride[step] * (1 - 2 * self.bit(self.me[axis], mask))
        self.held = self.held + [(off + turn, size) for off, size in self.held]

    def back_end(self, k):
        self.wait()

    def back_line_end(self):
        self.wait()


def step_kernel(
    n_dp,
    n_q,
    count_all,
    sensors_h,
    qidx,
    targets_h,
    w_one_h,
    b_one,
    w_two_h,
    b_two,
    v_one,
    c_one,
    v_two_h,
    c_two,
    v_three_h,
    c_three,
    loss_o,
    gw_one_o,
    gb_one_o,
    gw_two_o,
    gb_two_o,
    gv_one_o,
    gc_one_o,
    gv_two_o,
    gc_two_o,
    gv_three_o,
    gc_three_o,
    sens,
    tgt,
    w_one,
    w_two,
    v_two,
    v_three,
    v_two_t,
    v_three_t,
    hid,
    hid_b,
    first,
    second,
    first_b,
    second_b,
    basis,
    coef_b,
    coef_bt,
    mis_b,
    gco,
    gco_in,
    gco_run,
    gco_rx,
    gco_b,
    pre_all,
    sens_all,
    rest,
    rest_in,
    rest_line,
    bias,
    bias_in,
    trunk,
    trunk_in,
    trunk_out,
    small,
    small_in,
    sums,
    loss_row,
    g_two_b,
    acc,
    acc_in,
    load_sem,
    send_sem,
    recv_sem,
):
    func_rows, sensor_all = sens.shape
    hidden = w_one.shape[1]
    units, queries = first.shape
    basis_n = coef_b.shape[1]
    cols_dp = sensor_all // n_dp
    block = min(512, queries)
    blocks = queries // block
    inv_scale = 1.0 / math.sqrt(basis_n)
    grad_scale = 64.0 / math.sqrt(count_all)
    dp, q = lax.axis_index("dp"), lax.axis_index("query")
    me = {"dp": dp, "query": q}
    q_bits = bits_of(n_q)
    half = func_rows // 2
    part = lax.rem(q, 2)
    mine = pl.multiple_of(part * half, 8)
    other = pl.multiple_of((1 - part) * half, 8)
    side, line_at, line_n = lax.rem(dp, 2), dp // 2, n_dp // 2

    def bit(index, mask):
        return lax.rem(index // mask, 2)

    def flip(index, offset):
        result = index
        for mask in bits_of(n_dp * n_q):
            if offset & mask:
                result = result + mask * (1 - 2 * bit(index, mask))
        return result

    used = [0]

    def remote(src, dst, axis, peer):
        k = used[0]
        used[0] = k + 1
        return pltpu.make_async_remote_copy(
            src_ref=src,
            dst_ref=dst,
            send_sem=send_sem.at[k],
            recv_sem=recv_sem.at[k],
            device_id={axis: peer},
            device_id_type=MESH,
        )

    sent = []

    def launch(copy):
        copy.start()
        sent.append(copy)
        return copy

    pair = flip(dp, 1)
    barrier = pltpu.get_barrier_semaphore()
    dp_peers = [pair] + [flip(dp, 2 * k) for k in range(1, line_n)]
    for peer in dp_peers:
        pl.semaphore_signal(barrier, inc=1, device_id={"dp": peer}, device_id_type=MESH)
    for mask in q_bits:
        pl.semaphore_signal(barrier, inc=1, device_id={"query": flip(q, mask)}, device_id_type=MESH)

    def sensor_block(index, rows):
        return sensors_h.at[rows, pl.ds(pl.multiple_of(index * cols_dp, 128), cols_dp)]

    every = pl.ds(0, func_rows)
    loads = {}
    for k, (name, src, dst) in enumerate(
        (
            ("w_one", w_one_h, w_one),
            ("sens", sensors_h, sens),
            ("v_two", v_two_h, v_two),
            ("v_three", v_three_h, v_three),
            ("w_two", w_two_h, w_two.at[q]),
            ("targets", targets_h, tgt),
            ("own0", sensor_block(line_at * 2, every), sens_all.at[line_at * 2]),
            ("own1", sensor_block(line_at * 2 + 1, every), sens_all.at[line_at * 2 + 1]),
        )
    ):
        loads[name] = pltpu.make_async_copy(src, dst, load_sem.at[k])
        loads[name].start()
    pl.semaphore_wait(barrier, len(dp_peers) + len(q_bits))

    q_order = q_bits[::-1]
    w_half = hidden // 2
    w_rows = [pl.ds(pl.multiple_of(side * w_half + c * (w_half // 2), 16), w_half // 2) for c in range(2)]
    q_far = flip(q, q_order[0])
    w_far = [launch(remote(w_two_h.at[rows, :], w_two.at[q, rows, :], "query", q_far)) for rows in w_rows]
    bulk = []
    rows_mine = pl.ds(mine, half)
    share_n = func_rows // n_q

    def rows_of(member):
        return pl.ds(pl.multiple_of(member * share_n, 16), share_n)

    for k in [1] + list(range(line_n - 1, 1, -1)):
        to = flip(line_at, k)
        for s in range(2):
            copy = remote(
                sensor_block(to * 2 + s, rows_of(q)), sens_all.at[line_at * 2 + s, rows_of(q), :], "dp", flip(dp, 2 * k)
            )
            bulk.append((to * 2 + s, launch(copy)))

    def pass_on(index, member, mask):
        ref = sens_all.at[index, rows_of(member), :]
        return launch(remote(ref, ref, "query", flip(q, mask)))

    far, passed = [], []

    def pass_far(k):
        for index, copy in bulk[2 * k : 2 * k + 2]:
            copy.wait_recv()
            far.append((index, pass_on(index, q, q_order[0])))
            passed.append(pass_on(index, q, 1))


    loads["w_one"].wait()
    loads["sens"].wait()
    act = jnp.tanh(natural(sens[...], w_one[...]) + b_one[...])
    hid[...] = act
    hid_b[q] = act.astype(BF16)
    h_far = launch(remote(hid_b.at[q], hid_b.at[q], "query", q_far))

    loads["v_two"].wait()
    loads["v_three"].wait()
    v_two_t[...] = v_two[...].astype(F32).T.astype(BF16)
    v_three_t[...] = v_three[...].astype(F32).T.astype(BF16)
    columns = jnp.concatenate(
        [v_one[...], c_one[...], c_two[...], c_three[...], jnp.zeros((3, units), F32)], axis=0
    ).T

    def coords_of(span):
        x = qidx[0:1, span].astype(F32) / (GRID - 1)
        y = qidx[1:2, span].astype(F32) / (GRID - 1)
        return x, y

    def forward(i, carry):
        span = pl.ds(pl.multiple_of(i * block, 128), block)
        x, y = coords_of(span)
        one = jnp.tanh(columns[:, 0:1] * x + columns[:, 1:2] * y + columns[:, 2:3])
        first[:, span] = one
        one_b = one.astype(BF16)
        first_b[:, span] = one_b
        two = jnp.tanh(natural(v_two_t[...], one_b) + columns[:, 3:4])
        second[:, span] = two
        two_b = two.astype(BF16)
        second_b[:, span] = two_b
        basis[:, span] = (natural(v_three_t[...], two_b) + columns[:, 4:5]).astype(BF16)
        return carry

    def spread(buffer, held, masks):
        group = []
        for mask in masks:
            for copy in group:
                copy.wait_recv()
            group = [
                launch(remote(buffer.at[flip(q, o)], buffer.at[flip(q, o)], "query", flip(q, mask))) for o in held
            ]
            held = held + [o ^ mask for o in held]
        return group

    lax.fori_loop(0, blocks // 2, forward, 0)
    w_pair = []
    for rows, copy in zip(w_rows, w_far):
        copy.wait_recv()
        w_pair.append(launch(remote(w_two.at[q_far, rows, :], w_two.at[q_far, rows, :], "dp", pair)))
    lax.fori_loop(blocks // 2, blocks, forward, 0)
    loads["w_two"].wait()
    h_far.wait_recv()
    h_last = spread(hid_b, [0, q_order[0]], q_order[1:])
    for copy in w_pair:
        copy.wait_recv()
    w_last = spread(w_two, [0, q_order[0]], q_order[1:])
    for copy in h_last + w_last:
        copy.wait_recv()

    pass_far(0)
    coef = natural(hid_b[0], w_two[0])
    for i in range(1, n_q):
        coef = coef + natural(hid_b[i], w_two[i])
    coef = coef + b_two[...]
    coef_b[...] = coef.astype(BF16)
    coef_bt[...] = coef.T.astype(BF16)

    loads["targets"].wait()
    loss_row[...] = jnp.zeros_like(loss_row)

    def fit(i, carry):
        span = pl.ds(pl.multiple_of(i * block, 128), block)
        base = basis[:, span]
        miss = natural(coef_b[...], base) * inv_scale - tgt[:, span].astype(F32)
        loss_row[0:1, :] += jnp.sum(miss * miss, axis=0, keepdims=True)
        miss_b = (miss * grad_scale).astype(BF16)
        mis_b[:, span] = miss_b
        return carry

    lax.fori_loop(0, blocks, fit, 0, unroll=True)
    gco[pl.ds(other, half), :] = contract_cols(mis_b[pl.ds(other, half), :], basis[...]) * inv_scale
    core_step = launch(remote(gco.at[pl.ds(other, half), :], gco_in, "query", flip(q, 1)))
    gco[rows_mine, :] = contract_cols(mis_b[rows_mine, :], basis[...]) * inv_scale
    gb_two_row = jnp.sum(gco[...], axis=0, keepdims=True)
    trunk[...] = jnp.zeros_like(trunk)
    sums[...] = jnp.zeros_like(sums)
    core_step.wait_recv()
    gco_run[0] = gco[rows_mine, :] + gco_in[...]
    quarter, piece_n = half // 2, half // 4
    at_mine = bit(q, q_bits[1]) * quarter
    at_other = quarter - at_mine

    def gco_piece(start, c):
        return pl.ds(pl.multiple_of(start + c * piece_n, 16), piece_n)

    reduce_steps = [
        launch(remote(gco_run.at[0, gco_piece(at_other, c), :], gco_rx.at[0, gco_piece(0, c), :], "query", q_far))
        for c in range(2)
    ]
    shares, comes = [], []

    def reduce_piece(c):
        reduce_steps[c].wait_recv()
        total = gco_run[0, gco_piece(at_mine, c), :] + gco_rx[0, gco_piece(0, c), :]
        rows = gco_piece(mine + at_mine, c)
        gco_b[rows, :] = total.astype(BF16)
        ref = gco_b.at[rows, :]
        comes.append(launch(remote(ref, ref, "query", q_far)))
        shares.append(launch(remote(ref, ref, "query", flip(q, 1))))


    bits = [("query", m) for m in q_bits] + [("dp", 1)]
    across_q = [("query", m) for m in q_bits[1:]]
    order, back = [bits[0], ("dp", 1)] + across_q, [("dp", 1)] + across_q + [bits[0]]
    place = (me, flip, bit, (line_at, line_n), launch, remote)
    three = Trunk(trunk, trunk_in, trunk_out, 0, units, order, back, *place)
    two_ = Trunk(trunk, trunk_in, trunk_out, units, units, order, across_q + [("dp", 1), bits[0]], *place)

    def backward_top(i, carry):
        span = pl.ds(pl.multiple_of(i * block, 128), block)
        g_base = natural(coef_bt[...], mis_b[:, span]) * inv_scale
        sums[0] += lanes_summed(g_base)
        g_base = g_base.astype(BF16)
        trunk[:units, :] += contract_cols(second_b[:, span], g_base)
        two = second[:, span]
        g_two = natural(v_three[...], g_base) * (1.0 - two * two)
        sums[1] += lanes_summed(g_two)
        g_two_b[:, span] = g_two.astype(BF16)
        return carry

    def backward_low(i, carry):
        span = pl.ds(pl.multiple_of(i * block, 128), block)
        x, y = coords_of(span)
        g_two = g_two_b[:, span]
        trunk[units:, :] += contract_cols(first_b[:, span], g_two)
        one = first[:, span]
        g_one = natural(v_two[...], g_two) * (1.0 - one * one)
        sums[2] += lanes_summed(g_one)
        sums[3] += lanes_summed(g_one * x)
        sums[4] += lanes_summed(g_one * y)
        return carry

    lax.fori_loop(0, blocks, backward_top, 0, unroll=2)
    three.start(0)
    reduce_piece(0)
    lax.fori_loop(0, blocks // 2, backward_low, 0, unroll=True)
    three.end(0)
    three.start(1)
    reduce_piece(1)
    lax.fori_loop(blocks // 2, blocks, backward_low, 0, unroll=True)

    pass_far(1)
    for c in range(2):
        comes[c].wait_recv()
        ref = gco_b.at[gco_piece(mine + at_other, c), :]
        shares.append(launch(remote(ref, ref, "query", flip(q, 1))))

    two_.start(0)
    lane = lax.broadcasted_iota(jnp.int32, (units, 128), 1)
    table = jnp.zeros((units, 128), F32)
    for row, which in enumerate((3, 4, 2, 1, 0)):
        table = jnp.where(lane == row, jnp.sum(sums[which], axis=1, keepdims=True), table)
    rows = table.T[0:8]
    line = lax.broadcasted_iota(jnp.int32, rows.shape, 0)
    rows = jnp.where(line == 5, gb_two_row, rows)
    rows = jnp.where(line == 6, loss_row[0:1, :], rows)
    small[0] = rows
    s_flight = []

    def small_start(k):
        axis, mask = bits[k]
        s_flight.append(launch(remote(small.at[k], small_in.at[k], axis, flip(me[axis], mask))))

    def small_end(k):
        s_flight.pop().wait_recv()
        small[k + 1] = small[k] + small_in[k]

    def small_line_start():
        k = len(bits)
        for o in range(1, line_n):
            s_flight.append(launch(remote(small.at[k], small_in.at[k + o - 1], "dp", flip(dp, 2 * o))))

    def small_line_end():
        k = len(bits)
        total = small[k]
        for o in range(1, line_n):
            s_flight[o - 1].wait_recv()
            total = total + small_in[k + o - 1]
        return total

    small_start(0)

    for copy in shares:
        copy.wait_recv()
    act = hid[...]
    g_pre = contract_cols(gco_b[...], w_two[q]) * (1.0 - act * act)
    pre_all[line_at] = g_pre.astype(BF16)

    chunks = 4
    rows_c = func_rows // chunks

    def hop(at, c, peer):
        ref = pre_all.at[jnp.clip(at, 0, line_n - 1), c * rows_c : (c + 1) * rows_c, :]
        return remote(ref, ref, "dp", peer)

    to_right = jnp.minimum(dp + 2, n_dp - 2 + side)
    to_left = jnp.maximum(dp - 2, side)
    steps = line_n - 1
    rights = [[hop(line_at - s, c, to_right) for c in range(chunks)] for s in range(steps)]
    lefts = [[hop(line_at + s, c, to_left) for c in range(chunks)] for s in range(steps)]

    def sends_right(s):
        return jnp.logical_and(line_at - s >= 0, line_at < line_n - 1)

    def sends_left(s):
        return jnp.logical_and(line_at + s < line_n, line_at > 0)

    for c in range(chunks):
        pl.when(sends_right(0))(rights[0][c].start)
        pl.when(sends_left(0))(lefts[0][c].start)

    def gather_step(s, some=range(chunks)):
        for c in some:

            @pl.when(line_at - 1 - s >= 0)
            def _():
                rights[s][c].wait_recv()
                if s + 1 < steps:
                    pl.when(sends_right(s + 1))(rights[s + 1][c].start)

            @pl.when(line_at + 1 + s < line_n)
            def _():
                lefts[s][c].wait_recv()
                if s + 1 < steps:
                    pl.when(sends_left(s + 1))(lefts[s + 1][c].start)

    bias[0] = jnp.broadcast_to(jnp.sum(g_pre, axis=0, keepdims=True), bias.shape[1:])
    gco_bt = gco_b[...].astype(F32).T.astype(BF16)
    rest_all = natural(gco_bt, hid_b[q])
    rows_dp = basis_n // n_dp
    for j in range(n_dp):
        rest[j % 2, j // 2] = rest_all[j * rows_dp : (j + 1) * rows_dp, :]
    two_.end(0)
    two_.start(1)
    small_end(0)
    small_start(1)
    three.end(1)
    three.start(2)
    for k in range(2, line_n - 1):
        pass_far(k)
    for s in range(steps - 2):
        gather_step(s)
    gather_step(steps - 2, range(chunks // 2))
    two_.end(1)
    two_.start(2)
    gather_step(steps - 2, range(chunks // 2, chunks))
    small_end(1)
    small_start(2)
    three.end(2)
    three.line_start()
    rest_pair = [
        launch(remote(rest.at[1 - side], rest_in, "dp", pair)),
        launch(remote(bias.at[0], bias_in.at[0], "dp", pair)),
    ]
    loads["own0"].wait()
    loads["own1"].wait()
    for index, copy in far:
        copy.wait_recv()
        passed.append(pass_on(index, q_far, 1))
    two_.end(2)
    two_.line_start()
    small_end(2)
    small_line_start()
    gather_step(steps - 1)
    three.line_end()
    three.back_line_start()
    for copy in passed:
        copy.wait_recv()

    pieces = 4
    cols_p = cols_dp // pieces
    across = []

    def sum_of(whose, first_col, width):
        cols = slice(first_col, first_col + width)

        def body(j, carry):
            index = j * 2 + (1 - side if whose else side)
            return carry + contract_rows(sens_all[index, :, cols], pre_all[j])

        acc[whose, cols, :] = lax.fori_loop(0, line_n, body, jnp.zeros((width, hidden), F32))

    def send_across(piece):
        cols = slice(piece * cols_p, (piece + 1) * cols_p)
        across.append(launch(remote(acc.at[1, cols, :], acc_in.at[cols, :], "dp", pair)))

    sum_of(1, 0, 2 * cols_p)
    send_across(0)
    send_across(1)
    sum_of(1, 2 * cols_p, 2 * cols_p)
    two_.line_end()
    two_.back_line_start()
    three.back_line_end()
    three.back_start(0)
    two_.back_line_end()
    two_.back_start(0)
    for copy in rest_pair:
        copy.wait_recv()
    rest[side] += rest_in[...]
    bias[1] = bias[0] + bias_in[0]
    rest_flight = []
    for k in range(1, line_n):
        peer = flip(dp, 2 * k)
        rest_flight.append(launch(remote(rest.at[side, flip(line_at, k)], rest_line.at[k - 1], "dp", peer)))
        rest_flight.append(launch(remote(bias.at[1], bias_in.at[k], "dp", peer)))
    send_across(2)
    three.back_end(0)
    three.back_start(1)
    two_.back_end(0)
    two_.back_start(1)
    send_across(3)
    sum_of(0, 0, cols_dp)
    three.back_end(1)
    three.back_start(2)
    final = small_line_end()
    gv_one_o[...] = final[0:2]
    gc_one_o[...] = final[2:3]
    gc_two_o[...] = final[3:4]
    gc_three_o[...] = final[4:5]
    gb_two_o[...] = final[5:6]
    loss_o[...] = jnp.broadcast_to(jnp.sum(final[6:7], axis=1, keepdims=True) * (1.0 / count_all), loss_o.shape)
    for copy in rest_flight:
        copy.wait_recv()
    final_rest = rest[side, line_at]
    final_bias = bias[1]
    for k in range(1, line_n):
        final_rest = final_rest + rest_line[k - 1]
        final_bias = final_bias + bias_in[k]
    gw_two_o[...] = final_rest
    gb_one_o[...] = final_bias[0:1, :]
    three.back_end(2)
    outs = [pltpu.make_async_copy(trunk_out.at[:units, :], gv_three_o, load_sem.at[0])]
    outs[-1].start()
    two_.back_end(1)
    two_.back_start(2)
    for copy in across:
        copy.wait_recv()
    acc[0] += acc_in[...]
    outs.append(pltpu.make_async_copy(acc.at[0], gw_one_o, load_sem.at[1]))
    outs[-1].start()
    two_.back_end(2)
    outs.append(pltpu.make_async_copy(trunk_out.at[units:, :], gv_two_o, load_sem.at[2]))
    outs[-1].start()
    for copy in sent:
        copy.wait_send()
    for s in range(steps):
        for c in range(chunks):
            pl.when(sends_right(s))(rights[s][c].wait_send)
            pl.when(sends_left(s))(lefts[s][c].wait_send)
    for copy in outs:
        copy.wait()


def hand_over(*refs):
    count = (len(refs) - 2) // 3
    near, sems_in, sems_out = refs[2 * count : 3 * count], refs[-2], refs[-1]
    ins = [pltpu.make_async_copy(refs[k], near[k], sems_in.at[k]) for k in range(count)]
    outs = [pltpu.make_async_copy(near[k], refs[count + k], sems_out.at[k]) for k in range(count)]
    for copy in ins:
        copy.start()
    for came, goes in zip(ins, outs):
        came.wait()
        goes.start()
    for copy in outs:
        copy.wait()


def local_dense(
    sensors, query_index, targets, w_one, b_one, w_two, b_two, v_one, c_one, v_two, c_two, v_three, c_three
):
    n_dp, n_q = lax.axis_size("dp"), lax.axis_size("query")
    func_rows, sensor_all = sensors.shape
    queries = query_index.shape[1]
    hidden, basis_n = w_two.shape
    units = v_two.shape[0]
    cols_dp = sensor_all // n_dp
    count_all = func_rows * n_dp * queries * n_q
    line_n, q_n = n_dp // 2, len(bits_of(n_q))
    half = func_rows // 2
    rows_dp = basis_n // n_dp
    hbm, vmem = pl.BlockSpec(memory_space=pl.ANY), pl.BlockSpec(memory_space=pltpu.VMEM)
    sem_n = 160

    def row(value):
        return value.reshape(1, -1)

    def result(*shape):
        return jax.ShapeDtypeStruct(shape, F32)

    results = (
        result(1, 128),
        result(cols_dp, hidden),
        result(1, hidden),
        result(rows_dp, hidden),
        result(1, basis_n),
        result(2, units),
        result(1, units),
        result(units, units),
        result(1, units),
        result(units, basis_n),
        result(1, basis_n),
    )
    outs = pl.pallas_call(
        functools.partial(step_kernel, n_dp, n_q, count_all),
        out_shape=results,
        in_specs=[hbm, vmem, hbm, hbm, vmem, hbm, vmem, vmem, vmem, hbm, vmem, hbm, vmem],
        out_specs=(vmem, hbm, vmem, vmem, vmem, vmem, vmem, hbm, vmem, hbm, vmem),
        scratch_shapes=[
            pltpu.VMEM((func_rows, sensor_all), BF16),
            pltpu.VMEM((func_rows, queries), BF16),
            pltpu.VMEM((sensor_all, hidden), BF16),
            pltpu.VMEM((n_q, hidden, basis_n), BF16),
            pltpu.VMEM((units, units), BF16),
            pltpu.VMEM((units, basis_n), BF16),
            pltpu.VMEM((units, units), BF16),
            pltpu.VMEM((basis_n, units), BF16),
            pltpu.VMEM((func_rows, hidden), F32),
            pltpu.VMEM((n_q, func_rows, hidden), BF16),
            pltpu.VMEM((units, queries), F32),
            pltpu.VMEM((units, queries), F32),
            pltpu.VMEM((units, queries), BF16),
            pltpu.VMEM((units, queries), BF16),
            pltpu.VMEM((basis_n, queries), BF16),
            pltpu.VMEM((func_rows, basis_n), BF16),
            pltpu.VMEM((basis_n, func_rows), BF16),
            pltpu.VMEM((func_rows, queries), BF16),
            pltpu.VMEM((func_rows, basis_n), F32),
            pltpu.VMEM((half, basis_n), F32),
            pltpu.VMEM((q_n, half, basis_n), F32),
            pltpu.VMEM((q_n, half, basis_n), F32),
            pltpu.VMEM((func_rows, basis_n), BF16),
            pltpu.VMEM((line_n, func_rows, hidden), BF16),
            pltpu.VMEM((n_dp, func_rows, cols_dp), BF16),
            pltpu.VMEM((2, line_n, rows_dp, hidden), F32),
            pltpu.VMEM((line_n, rows_dp, hidden), F32),
            pltpu.VMEM((line_n, rows_dp, hidden), F32),
            pltpu.VMEM((2, 8, hidden), F32),
            pltpu.VMEM((line_n, 8, hidden), F32),
            pltpu.VMEM((2 * units, basis_n), F32),
            pltpu.VMEM((2 * units, basis_n), F32),
            pltpu.VMEM((2 * units, basis_n), F32),
            pltpu.VMEM((q_n + 2, 8, units), F32),
            pltpu.VMEM((q_n + line_n, 8, units), F32),
            pltpu.VMEM((5, units, 128), F32),
            pltpu.VMEM((8, min(512, queries)), F32),
            pltpu.VMEM((units, queries), BF16),
            pltpu.VMEM((2, cols_dp, hidden), F32),
            pltpu.VMEM((cols_dp, hidden), F32),
            pltpu.SemaphoreType.DMA((8,)),
            pltpu.SemaphoreType.DMA((sem_n,)),
            pltpu.SemaphoreType.DMA((sem_n,)),
        ],
        compiler_params=pltpu.CompilerParams(
            collective_id=0, has_side_effects=True, vmem_limit_bytes=67043328
        ),
        name="step",
    )(
        sensors,
        query_index,
        targets,
        w_one,
        row(b_one),
        w_two,
        row(b_two),
        v_one,
        row(c_one),
        v_two,
        row(c_two),
        v_three,
        row(c_three),
    )
    outs = pl.pallas_call(
        hand_over,
        out_shape=results,
        in_specs=[hbm] * len(results),
        out_specs=(hbm,) * len(results),
        scratch_shapes=[pltpu.VMEM(value.shape, F32) for value in results]
        + [pltpu.SemaphoreType.DMA((len(results),))] * 2,
        name="hand_over",
    )(*outs)
    loss, gw_one, gb_one, gw_two, gb_two, gv_one, gc_one, gv_two, gc_two, gv_three, gc_three = outs
    return (
        loss[0, 0],
        gw_one,
        gb_one.reshape(-1),
        gw_two.T,
        gb_two.reshape(-1),
        gv_one,
        gc_one.reshape(-1),
        gv_two,
        gc_two.reshape(-1),
        gv_three,
        gc_three.reshape(-1),
    )


def local(sensors, query_index, targets, w_one, b_one, w_two, b_two, v_one, c_one, v_two, *others):
    n_dp, n_q = lax.axis_size("dp"), lax.axis_size("query")
    units, basis_n = v_two.shape[0], w_two.shape[1]
    dense = (
        (sensors.shape[1] // n_dp) % 128 == 0
        and units == basis_n == min(512, query_index.shape[1])
        and (units // 2) % (8 * n_dp * n_q) == 0
        and sensors.shape[0] % (16 * n_q) == 0
        and len(bits_of(n_q)) == 2
        and len(bits_of(n_dp)) == 3
    )
    chosen = local_dense if dense else local_wide
    return chosen(sensors, query_index, targets, w_one, b_one, w_two, b_two, v_one, c_one, v_two, *others)


def solution(mesh):
    placed = (
        P("dp", None),
        P(None, "query"),
        P("dp", "query"),
        P(None, "query"),
        P("query"),
        P("query", None),
        P(),
        P(),
        P(),
        P(),
        P(),
        P(),
        P(),
    )
    return jax.shard_map(
        local,
        mesh=mesh,
        in_specs=placed,
        out_specs=(
            P(),
            P("dp", "query"),
            P("query"),
            P("query", "dp"),
            P(),
            P(),
            P(),
            P(),
            P(),
            P(),
            P(),
        ),
        check_vma=False,
    )
```

```python
import functools
import math

import jax
import jax.numpy as jnp
from jax import lax
from jax.experimental import pallas as pl
from jax.experimental.pallas import tpu as pltpu
from jax.sharding import PartitionSpec as P

GRID = 128


def contract_rows(left, right, precision=None):
    return lax.dot_general(
        left,
        right,
        (((0,), (0,)), ((), ())),
        precision=precision,
        preferred_element_type=jnp.float32,
    )


def contract_cols(left, right, precision=None):
    return lax.dot_general(
        left,
        right,
        (((1,), (1,)), ((), ())),
        precision=precision,
        preferred_element_type=jnp.float32,
    )


def trunk_forward(coords, v_one, c_one, v_two, c_two, v_three, c_three):
    first_act = jnp.tanh(
        coords[0][:, None] * v_one[0][None, :] + coords[1][:, None] * v_one[1][None, :] + c_one
    )
    first_b = first_act.astype(jnp.bfloat16)
    second_act = jnp.tanh(jnp.dot(first_b, v_two, preferred_element_type=jnp.float32) + c_two)
    second_b = second_act.astype(jnp.bfloat16)
    basis_full = jnp.dot(second_b, v_three, preferred_element_type=jnp.float32) + c_three
    return (first_act, first_b, second_act, second_b, basis_full.astype(jnp.bfloat16))


def swap(value, axis, mask):
    count = lax.axis_size(axis)
    return lax.ppermute(value, axis, [(i, i ^ mask) for i in range(count)])


def bits_of(count):
    return [1 << b for b in range(count.bit_length() - 1)]


def gather_xor(value, axis, masks):
    blocks, offsets = value, [0]
    for mask in masks:
        blocks = jnp.concatenate([blocks, swap(blocks, axis, mask)], axis=0)
        offsets = offsets + [o ^ mask for o in offsets]
    return blocks, offsets


def split_pair(value):
    high = lax.reduce_precision(value, 8, 7)
    return high.astype(jnp.bfloat16), (value - high).astype(jnp.bfloat16)


def trunk_backward(coords, first_act, first_b, second_act, second_b, grad_basis, v_two, v_three):
    basis_hi, basis_lo = split_pair(grad_basis)
    grad_v_three = contract_rows(second_b, basis_hi) + contract_rows(second_b, basis_lo)
    grad_c_three = jnp.sum(grad_basis, axis=0)
    grad_second = (contract_cols(basis_hi, v_three) + contract_cols(basis_lo, v_three)) * (
        1.0 - second_act * second_act
    )
    second_hi, second_lo = split_pair(grad_second)
    grad_v_two = contract_rows(first_b, second_hi) + contract_rows(first_b, second_lo)
    grad_c_two = jnp.sum(grad_second, axis=0)
    grad_first = (contract_cols(second_hi, v_two) + contract_cols(second_lo, v_two)) * (
        1.0 - first_act * first_act
    )
    grad_v_one = jnp.stack(
        [jnp.sum(coords[0][:, None] * grad_first, axis=0), jnp.sum(coords[1][:, None] * grad_first, axis=0)]
    )
    grad_c_one = jnp.sum(grad_first, axis=0)
    return (grad_v_one, grad_c_one, grad_v_two, grad_c_two, grad_v_three, grad_c_three)


def local_wide(
    sensors,
    query_index,
    targets,
    w_one,
    b_one,
    w_two,
    b_two,
    v_one,
    c_one,
    v_two,
    c_two,
    v_three,
    c_three,
):
    dp_count, q_count = lax.axis_size("dp"), lax.axis_size("query")
    func_rows = sensors.shape[0]
    query_rows = query_index.shape[1]
    count_all = func_rows * dp_count * query_rows * q_count
    grad_scale = 64.0 / math.sqrt(count_all)
    inv_scale = 1.0 / math.sqrt(w_two.shape[1])
    dp_me, q_me = lax.axis_index("dp"), lax.axis_index("query")
    dp_bits, q_bits = bits_of(dp_count), bits_of(q_count)
    half = func_rows // 2
    parity = lax.rem(q_me, 2)
    mine = parity * half
    other = half - mine

    w_two_all, _ = gather_xor(w_two, "query", q_bits[::-1])
    sensor_cols = sensors.shape[1] // dp_count
    sensors_half = lax.dynamic_slice_in_dim(sensors, mine, half, 0)
    held = []
    for offset in range(dp_count):
        start = jnp.bitwise_xor(dp_me, offset) * sensor_cols
        block = lax.dynamic_slice_in_dim(sensors_half, start, sensor_cols, 1)
        held.append(block if offset == 0 else swap(block, "dp", offset))
    sensors_mine = jnp.concatenate(held, axis=0)
    sensors_other = swap(sensors_mine, "query", 1)

    hidden = jnp.tanh(jnp.dot(sensors, w_one, preferred_element_type=jnp.float32) + b_one)
    hidden_b = hidden.astype(jnp.bfloat16)
    hidden_all, _ = gather_xor(hidden_b, "query", q_bits[::-1])
    hidden_wide = jnp.concatenate(
        [hidden_all[i * func_rows : (i + 1) * func_rows] for i in range(q_count)], axis=1
    )

    coords = query_index.astype(jnp.float32) / (GRID - 1)
    first_act, first_b, second_act, second_b, basis_b = trunk_forward(
        coords, v_one, c_one, v_two, c_two, v_three, c_three
    )

    coeffs = jnp.dot(hidden_wide, w_two_all, preferred_element_type=jnp.float32) + b_two
    coeffs_b = coeffs.astype(jnp.bfloat16)
    prediction = contract_cols(coeffs_b, basis_b) * inv_scale
    misfit = prediction - targets.astype(jnp.float32)
    loss_part = jnp.sum(misfit * misfit)
    misfit_b = (misfit * grad_scale).astype(jnp.bfloat16)

    partial = jnp.dot(misfit_b, basis_b, preferred_element_type=jnp.float32) * inv_scale
    running = lax.dynamic_slice_in_dim(partial, mine, half, 0) + swap(
        lax.dynamic_slice_in_dim(partial, other, half, 0), "query", 1
    )
    for mask in q_bits[1:]:
        running = running + swap(running, "query", mask)
    running_b = running.astype(jnp.bfloat16)
    grad_coeffs_b = jnp.concatenate([running_b, swap(running_b, "query", 1)], axis=0)

    def in_order(value):
        return jnp.concatenate(
            [
                lax.dynamic_slice_in_dim(value, mine, half, 0),
                lax.dynamic_slice_in_dim(value, other, half, 0),
            ],
            axis=0,
        )

    hidden_o = in_order(hidden)
    hidden_bo = in_order(hidden_b)
    grad_pre = contract_cols(grad_coeffs_b, w_two) * (1.0 - hidden_o * hidden_o)
    grad_pre_b = grad_pre.astype(jnp.bfloat16)
    wide_first = dp_bits[1:][::-1] + dp_bits[:1]
    wide_last = dp_bits[:1] + dp_bits[1:][::-1]
    sides = []
    for rows, masks in ((grad_pre_b[:half], wide_first), (grad_pre_b[half:], wide_last)):
        blocks, offsets = gather_xor(rows, "dp", masks)
        sides.append(
            jnp.concatenate(
                [blocks[offsets.index(o) * half : (offsets.index(o) + 1) * half] for o in range(dp_count)],
                axis=0,
            )
        )
    grad_w_one = contract_rows(
        jnp.concatenate([sensors_mine, sensors_other], axis=0), jnp.concatenate(sides, axis=0)
    )

    rest = contract_rows(grad_coeffs_b, hidden_bo)
    bias_sum = jnp.broadcast_to(jnp.sum(grad_pre, axis=0)[None, :], (8, grad_pre.shape[1]))
    for mask in dp_bits[::-1]:
        rows = rest.shape[0] // 2
        upper = jnp.bitwise_and(dp_me, mask) // mask
        keep = lax.dynamic_slice_in_dim(rest, upper * rows, rows, 0)
        give = lax.dynamic_slice_in_dim(rest, (1 - upper) * rows, rows, 0)
        both = jnp.concatenate([keep, bias_sum], axis=0) + swap(
            jnp.concatenate([give, bias_sum], axis=0), "dp", mask
        )
        rest, bias_sum = both[:rows], both[rows:]
    grad_w_two = rest.T
    grad_b_one = bias_sum[0]

    trunk_parts = trunk_backward(
        coords, first_act, first_b, second_act, second_b, inv_scale * contract_rows(misfit_b, coeffs_b), v_two, v_three
    )
    loss_sum, grad_b_two, *sums = lax.psum(
        (loss_part, jnp.sum(partial, axis=0)) + trunk_parts, ("dp", "query")
    )
    return (loss_sum / count_all, grad_w_one, grad_b_one, grad_w_two, grad_b_two, *sums)


MESH = pl.DeviceIdType.MESH
F32, BF16 = jnp.float32, jnp.bfloat16
def natural(left, right):
    return jnp.dot(left, right, preferred_element_type=F32)


def lanes_summed(value):
    total = value[:, :128]
    for start in range(128, value.shape[1], 128):
        total = total + value[:, start : start + 128]
    return total


class Trunk:
    def __init__(self, partial, landing, total, base, rows, order, back, me, flip, bit, line, launch, remote):
        self.partial, self.landing, self.total = partial, landing, total
        self.me, self.flip, self.bit, self.line = me, flip, bit, line
        self.launch, self.remote = launch, remote
        self.order, self.back = order, back
        self.size, self.off, self.land = rows, base, base
        self.stride = {step: rows >> (k + 1) for k, step in enumerate(order)}
        self.flight = []

    def span(self, start, size):
        return pl.ds(pl.multiple_of(start, 8), size)

    def send(self, src, dst, axis, offset):
        self.flight.append(self.launch(self.remote(src, dst, axis, self.flip(self.me[axis], offset))))

    def wait(self):
        for copy in self.flight:
            copy.wait_recv()
        self.flight = []

    def start(self, k):
        axis, mask = self.order[k]
        size = self.size // 2
        up = self.bit(self.me[axis], mask)
        give = self.span(self.off + (1 - up) * size, size)
        self.send(self.partial.at[give, :], self.landing.at[self.land : self.land + size, :], axis, mask)
        self.off = self.off + up * size

    def end(self, k):
        self.wait()
        self.size //= 2
        self.partial[self.span(self.off, self.size), :] += self.landing[self.land : self.land + self.size, :]
        self.land += self.size

    def line_start(self):
        at, count = self.line
        size = self.size // count
        for k in range(1, count):
            give = self.span(self.off + self.flip(at, k) * size, size)
            first = self.land + (k - 1) * size
            self.send(self.partial.at[give, :], self.landing.at[first : first + size, :], "dp", 2 * k)

    def line_end(self):
        at, count = self.line
        size = self.size // count
        self.wait()
        mine = self.span(self.off + at * size, size)
        value = self.partial[mine, :]
        for k in range(1, count):
            first = self.land + (k - 1) * size
            value = value + self.landing[first : first + size, :]
        self.total[mine, :] = value

    def back_line_start(self):
        at, count = self.line
        size = self.size // count
        mine = self.total.at[self.span(self.off + at * size, size), :]
        for k in range(1, count):
            self.send(mine, mine, "dp", 2 * k)
        self.held = [(self.off, self.size)]

    def back_start(self, k):
        axis, mask = step = self.back[k]
        if k == len(self.back) - 1:
            rows = self.stride[step]
            self.held = [(self.held[0][0] // rows * rows, rows)]
        for off, size in self.held:
            block = self.total.at[self.span(off, size), :]
            self.send(block, block, axis, mask)
        turn = self.stride[step] * (1 - 2 * self.bit(self.me[axis], mask))
        self.held = self.held + [(off + turn, size) for off, size in self.held]

    def back_end(self, k):
        self.wait()

    def back_line_end(self):
        self.wait()


def step_kernel(
    n_dp,
    n_q,
    count_all,
    sensors_h,
    qidx_h,
    targets_h,
    w_one_h,
    b_one_h,
    w_two_h,
    b_two_h,
    v_one_h,
    c_one_h,
    v_two_h,
    c_two_h,
    v_three_h,
    c_three_h,
    loss_h,
    gw_one_o,
    gb_one_h,
    gw_two_h,
    gb_two_h,
    gv_one_h,
    gc_one_h,
    gv_two_o,
    gc_two_h,
    gv_three_o,
    gc_three_h,
    qidx,
    b_one,
    b_two,
    v_one,
    c_one,
    c_two,
    c_three,
    loss_o,
    gb_one_o,
    gw_two_o,
    gb_two_o,
    gv_one_o,
    gc_one_o,
    gc_two_o,
    gc_three_o,
    sens,
    tgt,
    w_one,
    w_two,
    v_two,
    v_three,
    v_two_t,
    v_three_t,
    hid,
    hid_b,
    first,
    second,
    first_b,
    second_b,
    basis,
    coef_b,
    coef_bt,
    mis_b,
    gco,
    gco_in,
    gco_run,
    gco_rx,
    gco_b,
    pre_all,
    sens_all,
    rest,
    rest_in,
    rest_line,
    bias,
    bias_in,
    trunk,
    trunk_in,
    trunk_out,
    small,
    small_in,
    sums,
    loss_row,
    g_two_b,
    acc,
    acc_in,
    load_sem,
    send_sem,
    recv_sem,
):
    func_rows, sensor_all = sens.shape
    hidden = w_one.shape[1]
    units, queries = first.shape
    basis_n = coef_b.shape[1]
    cols_dp = sensor_all // n_dp
    block = min(512, queries)
    blocks = queries // block
    inv_scale = 1.0 / math.sqrt(basis_n)
    grad_scale = 64.0 / math.sqrt(count_all)
    dp, q = lax.axis_index("dp"), lax.axis_index("query")
    me = {"dp": dp, "query": q}
    q_bits = bits_of(n_q)
    half = func_rows // 2
    part = lax.rem(q, 2)
    mine = pl.multiple_of(part * half, 8)
    other = pl.multiple_of((1 - part) * half, 8)
    side, line_at, line_n = lax.rem(dp, 2), dp // 2, n_dp // 2

    def bit(index, mask):
        return lax.rem(index // mask, 2)

    def flip(index, offset):
        result = index
        for mask in bits_of(n_dp * n_q):
            if offset & mask:
                result = result + mask * (1 - 2 * bit(index, mask))
        return result

    used = [0]

    def remote(src, dst, axis, peer):
        k = used[0]
        used[0] = k + 1
        return pltpu.make_async_remote_copy(
            src_ref=src,
            dst_ref=dst,
            send_sem=send_sem.at[k],
            recv_sem=recv_sem.at[k],
            device_id={axis: peer},
            device_id_type=MESH,
        )

    sent = []

    def launch(copy):
        copy.start()
        sent.append(copy)
        return copy

    pair = flip(dp, 1)
    barrier = pltpu.get_barrier_semaphore()
    dp_peers = [pair] + [flip(dp, 2 * k) for k in range(1, line_n)]
    for peer in dp_peers:
        pl.semaphore_signal(barrier, inc=1, device_id={"dp": peer}, device_id_type=MESH)
    for mask in q_bits:
        pl.semaphore_signal(barrier, inc=1, device_id={"query": flip(q, mask)}, device_id_type=MESH)

    def sensor_block(index, rows):
        return sensors_h.at[rows, pl.ds(pl.multiple_of(index * cols_dp, 128), cols_dp)]

    every = pl.ds(0, func_rows)
    loads = {}
    for k, (name, src, dst) in enumerate(
        (
            ("w_one", w_one_h, w_one),
            ("sens", sensors_h, sens),
            ("b_one", b_one_h, b_one),
            ("qidx", qidx_h, qidx),
            ("b_two", b_two_h, b_two),
            ("v_one", v_one_h, v_one),
            ("c_one", c_one_h, c_one),
            ("c_two", c_two_h, c_two),
            ("c_three", c_three_h, c_three),
            ("v_two", v_two_h, v_two),
            ("v_three", v_three_h, v_three),
            ("w_two", w_two_h, w_two.at[q]),
            ("targets", targets_h, tgt),
            ("own0", sensor_block(line_at * 2, every), sens_all.at[line_at * 2]),
            ("own1", sensor_block(line_at * 2 + 1, every), sens_all.at[line_at * 2 + 1]),
        )
    ):
        loads[name] = pltpu.make_async_copy(src, dst, load_sem.at[k])
        loads[name].start()
    pl.semaphore_wait(barrier, len(dp_peers) + len(q_bits))

    q_order = q_bits[::-1]
    w_half = hidden // 2
    w_rows = [pl.ds(pl.multiple_of(side * w_half + c * (w_half // 2), 16), w_half // 2) for c in range(2)]
    q_far = flip(q, q_order[0])
    w_far = [launch(remote(w_two_h.at[rows, :], w_two.at[q, rows, :], "query", q_far)) for rows in w_rows]
    bulk = []
    rows_mine = pl.ds(mine, half)
    share_n = func_rows // n_q

    def rows_of(member):
        return pl.ds(pl.multiple_of(member * share_n, 16), share_n)

    for k in [1] + list(range(line_n - 1, 1, -1)):
        to = flip(line_at, k)
        for s in range(2):
            copy = remote(
                sensor_block(to * 2 + s, rows_of(q)), sens_all.at[line_at * 2 + s, rows_of(q), :], "dp", flip(dp, 2 * k)
            )
            bulk.append((to * 2 + s, launch(copy)))

    def pass_on(index, member, mask):
        ref = sens_all.at[index, rows_of(member), :]
        return launch(remote(ref, ref, "query", flip(q, mask)))

    far, passed = [], []

    def pass_far(k):
        for index, copy in bulk[2 * k : 2 * k + 2]:
            copy.wait_recv()
            far.append((index, pass_on(index, q, q_order[0])))
            passed.append(pass_on(index, q, 1))


    loads["w_one"].wait()
    loads["sens"].wait()
    loads["b_one"].wait()
    act = jnp.tanh(natural(sens[...], w_one[...]) + b_one[...])
    hid[...] = act
    hid_b[q] = act.astype(BF16)
    h_far = launch(remote(hid_b.at[q], hid_b.at[q], "query", q_far))

    for name in ("qidx", "b_two", "v_one", "c_one", "c_two", "c_three", "v_two"):
        loads[name].wait()
    loads["v_three"].wait()
    v_two_t[...] = v_two[...].astype(F32).T.astype(BF16)
    v_three_t[...] = v_three[...].astype(F32).T.astype(BF16)
    columns = jnp.concatenate(
        [v_one[...], c_one[...], c_two[...], c_three[...], jnp.zeros((3, units), F32)], axis=0
    ).T

    def coords_of(span):
        x = qidx[0:1, span].astype(F32) / (GRID - 1)
        y = qidx[1:2, span].astype(F32) / (GRID - 1)
        return x, y

    def forward(i, carry):
        span = pl.ds(pl.multiple_of(i * block, 128), block)
        x, y = coords_of(span)
        one = jnp.tanh(columns[:, 0:1] * x + columns[:, 1:2] * y + columns[:, 2:3])
        first[:, span] = one
        one_b = one.astype(BF16)
        first_b[:, span] = one_b
        two = jnp.tanh(natural(v_two_t[...], one_b) + columns[:, 3:4])
        second[:, span] = two
        two_b = two.astype(BF16)
        second_b[:, span] = two_b
        basis[:, span] = (natural(v_three_t[...], two_b) + columns[:, 4:5]).astype(BF16)
        return carry

    def spread(buffer, held, masks):
        group = []
        for mask in masks:
            for copy in group:
                copy.wait_recv()
            group = [
                launch(remote(buffer.at[flip(q, o)], buffer.at[flip(q, o)], "query", flip(q, mask))) for o in held
            ]
            held = held + [o ^ mask for o in held]
        return group

    lax.fori_loop(0, blocks // 2, forward, 0)
    w_pair = []
    for rows, copy in zip(w_rows, w_far):
        copy.wait_recv()
        w_pair.append(launch(remote(w_two.at[q_far, rows, :], w_two.at[q_far, rows, :], "dp", pair)))
    lax.fori_loop(blocks // 2, blocks, forward, 0)
    loads["w_two"].wait()
    h_far.wait_recv()
    h_last = spread(hid_b, [0, q_order[0]], q_order[1:])
    for copy in w_pair:
        copy.wait_recv()
    w_last = spread(w_two, [0, q_order[0]], q_order[1:])
    for copy in h_last + w_last:
        copy.wait_recv()

    pass_far(0)
    coef = natural(hid_b[0], w_two[0])
    for i in range(1, n_q):
        coef = coef + natural(hid_b[i], w_two[i])
    coef = coef + b_two[...]
    coef_b[...] = coef.astype(BF16)
    coef_bt[...] = coef.T.astype(BF16)

    loads["targets"].wait()
    loss_row[...] = jnp.zeros_like(loss_row)

    def fit(i, carry):
        span = pl.ds(pl.multiple_of(i * block, 128), block)
        base = basis[:, span]
        miss = natural(coef_b[...], base) * inv_scale - tgt[:, span].astype(F32)
        loss_row[0:1, :] += jnp.sum(miss * miss, axis=0, keepdims=True)
        miss_b = (miss * grad_scale).astype(BF16)
        mis_b[:, span] = miss_b
        return carry

    lax.fori_loop(0, blocks, fit, 0, unroll=True)
    gco[pl.ds(other, half), :] = contract_cols(mis_b[pl.ds(other, half), :], basis[...]) * inv_scale
    core_step = launch(remote(gco.at[pl.ds(other, half), :], gco_in, "query", flip(q, 1)))
    gco[rows_mine, :] = contract_cols(mis_b[rows_mine, :], basis[...]) * inv_scale
    gb_two_row = jnp.sum(gco[...], axis=0, keepdims=True)
    trunk[...] = jnp.zeros_like(trunk)
    sums[...] = jnp.zeros_like(sums)
    core_step.wait_recv()
    gco_run[0] = gco[rows_mine, :] + gco_in[...]
    quarter, piece_n = half // 2, half // 4
    at_mine = bit(q, q_bits[1]) * quarter
    at_other = quarter - at_mine

    def gco_piece(start, c):
        return pl.ds(pl.multiple_of(start + c * piece_n, 16), piece_n)

    reduce_steps = [
        launch(remote(gco_run.at[0, gco_piece(at_other, c), :], gco_rx.at[0, gco_piece(0, c), :], "query", q_far))
        for c in range(2)
    ]
    shares, comes = [], []

    def reduce_piece(c):
        reduce_steps[c].wait_recv()
        total = gco_run[0, gco_piece(at_mine, c), :] + gco_rx[0, gco_piece(0, c), :]
        rows = gco_piece(mine + at_mine, c)
        gco_b[rows, :] = total.astype(BF16)
        ref = gco_b.at[rows, :]
        comes.append(launch(remote(ref, ref, "query", q_far)))
        shares.append(launch(remote(ref, ref, "query", flip(q, 1))))


    bits = [("query", m) for m in q_bits] + [("dp", 1)]
    across_q = [("query", m) for m in q_bits[1:]]
    order, back = [bits[0], ("dp", 1)] + across_q, [("dp", 1)] + across_q + [bits[0]]
    place = (me, flip, bit, (line_at, line_n), launch, remote)
    three = Trunk(trunk, trunk_in, trunk_out, 0, units, order, back, *place)
    two_ = Trunk(trunk, trunk_in, trunk_out, units, units, order, across_q + [("dp", 1), bits[0]], *place)

    def backward_top(i, carry):
        span = pl.ds(pl.multiple_of(i * block, 128), block)
        g_base = natural(coef_bt[...], mis_b[:, span]) * inv_scale
        sums[0] += lanes_summed(g_base)
        g_base = g_base.astype(BF16)
        trunk[:units, :] += contract_cols(second_b[:, span], g_base)
        two = second[:, span]
        g_two = natural(v_three[...], g_base) * (1.0 - two * two)
        sums[1] += lanes_summed(g_two)
        g_two_b[:, span] = g_two.astype(BF16)
        return carry

    def backward_low(i, carry):
        span = pl.ds(pl.multiple_of(i * block, 128), block)
        x, y = coords_of(span)
        g_two = g_two_b[:, span]
        trunk[units:, :] += contract_cols(first_b[:, span], g_two)
        one = first[:, span]
        g_one = natural(v_two[...], g_two) * (1.0 - one * one)
        sums[2] += lanes_summed(g_one)
        sums[3] += lanes_summed(g_one * x)
        sums[4] += lanes_summed(g_one * y)
        return carry

    lax.fori_loop(0, blocks, backward_top, 0, unroll=2)
    three.start(0)
    reduce_piece(0)
    lax.fori_loop(0, blocks // 2, backward_low, 0, unroll=True)
    three.end(0)
    three.start(1)
    reduce_piece(1)
    lax.fori_loop(blocks // 2, blocks, backward_low, 0, unroll=True)

    pass_far(1)
    for c in range(2):
        comes[c].wait_recv()
        ref = gco_b.at[gco_piece(mine + at_other, c), :]
        shares.append(launch(remote(ref, ref, "query", flip(q, 1))))

    two_.start(0)
    lane = lax.broadcasted_iota(jnp.int32, (units, 128), 1)
    table = jnp.zeros((units, 128), F32)
    for row, which in enumerate((3, 4, 2, 1, 0)):
        table = jnp.where(lane == row, jnp.sum(sums[which], axis=1, keepdims=True), table)
    rows = table.T[0:8]
    line = lax.broadcasted_iota(jnp.int32, rows.shape, 0)
    rows = jnp.where(line == 5, gb_two_row, rows)
    rows = jnp.where(line == 6, loss_row[0:1, :], rows)
    small[0] = rows
    s_flight = []

    def small_start(k):
        axis, mask = bits[k]
        s_flight.append(launch(remote(small.at[k], small_in.at[k], axis, flip(me[axis], mask))))

    def small_end(k):
        s_flight.pop().wait_recv()
        small[k + 1] = small[k] + small_in[k]

    def small_line_start():
        k = len(bits)
        for o in range(1, line_n):
            s_flight.append(launch(remote(small.at[k], small_in.at[k + o - 1], "dp", flip(dp, 2 * o))))

    def small_line_end():
        k = len(bits)
        total = small[k]
        for o in range(1, line_n):
            s_flight[o - 1].wait_recv()
            total = total + small_in[k + o - 1]
        return total

    small_start(0)

    for copy in shares:
        copy.wait_recv()
    act = hid[...]
    g_pre = contract_cols(gco_b[...], w_two[q]) * (1.0 - act * act)
    pre_all[line_at] = g_pre.astype(BF16)

    chunks = 4
    rows_c = func_rows // chunks

    def hop(at, c, peer):
        ref = pre_all.at[jnp.clip(at, 0, line_n - 1), c * rows_c : (c + 1) * rows_c, :]
        return remote(ref, ref, "dp", peer)

    to_right = jnp.minimum(dp + 2, n_dp - 2 + side)
    to_left = jnp.maximum(dp - 2, side)
    steps = line_n - 1
    rights = [[hop(line_at - s, c, to_right) for c in range(chunks)] for s in range(steps)]
    lefts = [[hop(line_at + s, c, to_left) for c in range(chunks)] for s in range(steps)]

    def sends_right(s):
        return jnp.logical_and(line_at - s >= 0, line_at < line_n - 1)

    def sends_left(s):
        return jnp.logical_and(line_at + s < line_n, line_at > 0)

    for c in range(chunks):
        pl.when(sends_right(0))(rights[0][c].start)
        pl.when(sends_left(0))(lefts[0][c].start)

    def gather_step(s, some=range(chunks)):
        for c in some:

            @pl.when(line_at - 1 - s >= 0)
            def _():
                rights[s][c].wait_recv()
                if s + 1 < steps:
                    pl.when(sends_right(s + 1))(rights[s + 1][c].start)

            @pl.when(line_at + 1 + s < line_n)
            def _():
                lefts[s][c].wait_recv()
                if s + 1 < steps:
                    pl.when(sends_left(s + 1))(lefts[s + 1][c].start)

    bias[0] = jnp.broadcast_to(jnp.sum(g_pre, axis=0, keepdims=True), bias.shape[1:])
    gco_bt = gco_b[...].astype(F32).T.astype(BF16)
    rest_all = natural(gco_bt, hid_b[q])
    rows_dp = basis_n // n_dp
    for j in range(n_dp):
        rest[j % 2, j // 2] = rest_all[j * rows_dp : (j + 1) * rows_dp, :]
    two_.end(0)
    two_.start(1)
    small_end(0)
    small_start(1)
    three.end(1)
    three.start(2)
    for k in range(2, line_n - 1):
        pass_far(k)
    for s in range(steps - 2):
        gather_step(s)
    gather_step(steps - 2, range(chunks // 2))
    two_.end(1)
    two_.start(2)
    gather_step(steps - 2, range(chunks // 2, chunks))
    small_end(1)
    small_start(2)
    three.end(2)
    three.line_start()
    rest_pair = [
        launch(remote(rest.at[1 - side], rest_in, "dp", pair)),
        launch(remote(bias.at[0], bias_in.at[0], "dp", pair)),
    ]
    loads["own0"].wait()
    loads["own1"].wait()
    for index, copy in far:
        copy.wait_recv()
        passed.append(pass_on(index, q_far, 1))
    two_.end(2)
    two_.line_start()
    small_end(2)
    small_line_start()
    gather_step(steps - 1)
    for copy in passed:
        copy.wait_recv()

    pieces = 4
    cols_p = cols_dp // pieces
    across = []

    def sum_of(whose, first_col, width):
        cols = slice(first_col, first_col + width)

        def body(j, carry):
            index = j * 2 + (1 - side if whose else side)
            return carry + contract_rows(sens_all[index, :, cols], pre_all[j])

        acc[whose, cols, :] = lax.fori_loop(0, line_n, body, jnp.zeros((width, hidden), F32))

    def send_across(piece):
        cols = slice(piece * cols_p, (piece + 1) * cols_p)
        across.append(launch(remote(acc.at[1, cols, :], acc_in.at[cols, :], "dp", pair)))

    sum_of(1, 0, 2 * cols_p)
    send_across(0)
    three.line_end()
    three.back_line_start()
    send_across(1)
    sum_of(1, 2 * cols_p, 2 * cols_p)
    two_.line_end()
    two_.back_line_start()
    three.back_line_end()
    three.back_start(0)
    two_.back_line_end()
    two_.back_start(0)
    for copy in rest_pair:
        copy.wait_recv()
    rest[side] += rest_in[...]
    bias[1] = bias[0] + bias_in[0]
    rest_flight = []
    for k in range(1, line_n):
        peer = flip(dp, 2 * k)
        rest_flight.append(launch(remote(rest.at[side, flip(line_at, k)], rest_line.at[k - 1], "dp", peer)))
        rest_flight.append(launch(remote(bias.at[1], bias_in.at[k], "dp", peer)))
    send_across(2)
    three.back_end(0)
    three.back_start(1)
    two_.back_end(0)
    two_.back_start(1)
    send_across(3)
    sum_of(0, 0, cols_dp)
    three.back_end(1)
    three.back_start(2)
    outs = []

    def put(src, dst):
        outs.append(pltpu.make_async_copy(src, dst, load_sem.at[len(outs)]))
        outs[-1].start()

    final = small_line_end()
    gv_one_o[...] = final[0:2]
    gc_one_o[...] = final[2:3]
    gc_two_o[...] = final[3:4]
    gc_three_o[...] = final[4:5]
    gb_two_o[...] = final[5:6]
    loss_o[...] = jnp.broadcast_to(jnp.sum(final[6:7], axis=1, keepdims=True) * (1.0 / count_all), loss_o.shape)
    for copy in rest_flight:
        copy.wait_recv()
    final_rest = rest[side, line_at]
    final_bias = bias[1]
    for k in range(1, line_n):
        final_rest = final_rest + rest_line[k - 1]
        final_bias = final_bias + bias_in[k]
    gw_two_o[...] = final_rest
    gb_one_o[...] = final_bias[0:1, :]
    for src, dst in (
        (gv_one_o, gv_one_h),
        (gc_one_o, gc_one_h),
        (gc_two_o, gc_two_h),
        (gc_three_o, gc_three_h),
        (gb_two_o, gb_two_h),
        (loss_o, loss_h),
        (gw_two_o, gw_two_h),
        (gb_one_o, gb_one_h),
    ):
        put(src, dst)
    three.back_end(2)
    put(trunk_out.at[:units, :], gv_three_o)
    two_.back_end(1)
    two_.back_start(2)
    for copy in across:
        copy.wait_recv()
    acc[0] += acc_in[...]
    put(acc.at[0], gw_one_o)
    two_.back_end(2)
    put(trunk_out.at[units:, :], gv_two_o)
    for copy in sent:
        copy.wait_send()
    for s in range(steps):
        for c in range(chunks):
            pl.when(sends_right(s))(rights[s][c].wait_send)
            pl.when(sends_left(s))(lefts[s][c].wait_send)
    for copy in outs:
        copy.wait()


def hand_over(*refs):
    count = (len(refs) - 2) // 3
    near, sems_in, sems_out = refs[2 * count : 3 * count], refs[-2], refs[-1]
    ins = [pltpu.make_async_copy(refs[k], near[k], sems_in.at[k]) for k in range(count)]
    outs = [pltpu.make_async_copy(near[k], refs[count + k], sems_out.at[k]) for k in range(count)]
    for copy in ins:
        copy.start()
    for came, goes in zip(ins, outs):
        came.wait()
        goes.start()
    for copy in outs:
        copy.wait()


def local_dense(
    sensors, query_index, targets, w_one, b_one, w_two, b_two, v_one, c_one, v_two, c_two, v_three, c_three
):
    n_dp, n_q = lax.axis_size("dp"), lax.axis_size("query")
    func_rows, sensor_all = sensors.shape
    queries = query_index.shape[1]
    hidden, basis_n = w_two.shape
    units = v_two.shape[0]
    cols_dp = sensor_all // n_dp
    count_all = func_rows * n_dp * queries * n_q
    line_n, q_n = n_dp // 2, len(bits_of(n_q))
    half = func_rows // 2
    rows_dp = basis_n // n_dp
    hbm = pl.BlockSpec(memory_space=pl.ANY)
    sem_n = 160

    def row(value):
        return value.reshape(1, -1)

    def result(*shape):
        return jax.ShapeDtypeStruct(shape, F32)

    results = (
        result(1, 128),
        result(cols_dp, hidden),
        result(1, hidden),
        result(rows_dp, hidden),
        result(1, basis_n),
        result(2, units),
        result(1, units),
        result(units, units),
        result(1, units),
        result(units, basis_n),
        result(1, basis_n),
    )
    outs = pl.pallas_call(
        functools.partial(step_kernel, n_dp, n_q, count_all),
        out_shape=results,
        in_specs=[hbm] * 13,
        out_specs=(hbm,) * len(results),
        scratch_shapes=[
            pltpu.VMEM((2, queries), jnp.int32),
            pltpu.VMEM((1, hidden), F32),
            pltpu.VMEM((1, basis_n), F32),
            pltpu.VMEM((2, units), F32),
            pltpu.VMEM((1, units), F32),
            pltpu.VMEM((1, units), F32),
            pltpu.VMEM((1, basis_n), F32),
            pltpu.VMEM((1, 128), F32),
            pltpu.VMEM((1, hidden), F32),
            pltpu.VMEM((rows_dp, hidden), F32),
            pltpu.VMEM((1, basis_n), F32),
            pltpu.VMEM((2, units), F32),
            pltpu.VMEM((1, units), F32),
            pltpu.VMEM((1, units), F32),
            pltpu.VMEM((1, basis_n), F32),
            pltpu.VMEM((func_rows, sensor_all), BF16),
            pltpu.VMEM((func_rows, queries), BF16),
            pltpu.VMEM((sensor_all, hidden), BF16),
            pltpu.VMEM((n_q, hidden, basis_n), BF16),
            pltpu.VMEM((units, units), BF16),
            pltpu.VMEM((units, basis_n), BF16),
            pltpu.VMEM((units, units), BF16),
            pltpu.VMEM((basis_n, units), BF16),
            pltpu.VMEM((func_rows, hidden), F32),
            pltpu.VMEM((n_q, func_rows, hidden), BF16),
            pltpu.VMEM((units, queries), F32),
            pltpu.VMEM((units, queries), F32),
            pltpu.VMEM((units, queries), BF16),
            pltpu.VMEM((units, queries), BF16),
            pltpu.VMEM((basis_n, queries), BF16),
            pltpu.VMEM((func_rows, basis_n), BF16),
            pltpu.VMEM((basis_n, func_rows), BF16),
            pltpu.VMEM((func_rows, queries), BF16),
            pltpu.VMEM((func_rows, basis_n), F32),
            pltpu.VMEM((half, basis_n), F32),
            pltpu.VMEM((q_n, half, basis_n), F32),
            pltpu.VMEM((q_n, half, basis_n), F32),
            pltpu.VMEM((func_rows, basis_n), BF16),
            pltpu.VMEM((line_n, func_rows, hidden), BF16),
            pltpu.VMEM((n_dp, func_rows, cols_dp), BF16),
            pltpu.VMEM((2, line_n, rows_dp, hidden), F32),
            pltpu.VMEM((line_n, rows_dp, hidden), F32),
            pltpu.VMEM((line_n, rows_dp, hidden), F32),
            pltpu.VMEM((2, 8, hidden), F32),
            pltpu.VMEM((line_n, 8, hidden), F32),
            pltpu.VMEM((2 * units, basis_n), F32),
            pltpu.VMEM((2 * units, basis_n), F32),
            pltpu.VMEM((2 * units, basis_n), F32),
            pltpu.VMEM((q_n + 2, 8, units), F32),
            pltpu.VMEM((q_n + line_n, 8, units), F32),
            pltpu.VMEM((5, units, 128), F32),
            pltpu.VMEM((8, min(512, queries)), F32),
            pltpu.VMEM((units, queries), BF16),
            pltpu.VMEM((2, cols_dp, hidden), F32),
            pltpu.VMEM((cols_dp, hidden), F32),
            pltpu.SemaphoreType.DMA((32,)),
            pltpu.SemaphoreType.DMA((sem_n,)),
            pltpu.SemaphoreType.DMA((sem_n,)),
        ],
        compiler_params=pltpu.CompilerParams(
            collective_id=0, has_side_effects=True, vmem_limit_bytes=67043328
        ),
        name="step",
    )(
        sensors,
        query_index,
        targets,
        w_one,
        row(b_one),
        w_two,
        row(b_two),
        v_one,
        row(c_one),
        v_two,
        row(c_two),
        v_three,
        row(c_three),
    )
    outs = pl.pallas_call(
        hand_over,
        out_shape=results,
        in_specs=[hbm] * len(results),
        out_specs=(hbm,) * len(results),
        scratch_shapes=[pltpu.VMEM(value.shape, F32) for value in results]
        + [pltpu.SemaphoreType.DMA((len(results),))] * 2,
        name="hand_over",
    )(*outs)
    loss, gw_one, gb_one, gw_two, gb_two, gv_one, gc_one, gv_two, gc_two, gv_three, gc_three = outs
    return (
        loss[0, 0],
        gw_one,
        gb_one.reshape(-1),
        gw_two.T,
        gb_two.reshape(-1),
        gv_one,
        gc_one.reshape(-1),
        gv_two,
        gc_two.reshape(-1),
        gv_three,
        gc_three.reshape(-1),
    )


def local(sensors, query_index, targets, w_one, b_one, w_two, b_two, v_one, c_one, v_two, *others):
    n_dp, n_q = lax.axis_size("dp"), lax.axis_size("query")
    units, basis_n = v_two.shape[0], w_two.shape[1]
    dense = (
        (sensors.shape[1] // n_dp) % 128 == 0
        and units == basis_n == min(512, query_index.shape[1])
        and (units // 2) % (8 * n_dp * n_q) == 0
        and sensors.shape[0] % (16 * n_q) == 0
        and len(bits_of(n_q)) == 2
        and len(bits_of(n_dp)) == 3
    )
    chosen = local_dense if dense else local_wide
    return chosen(sensors, query_index, targets, w_one, b_one, w_two, b_two, v_one, c_one, v_two, *others)


def solution(mesh):
    placed = (
        P("dp", None),
        P(None, "query"),
        P("dp", "query"),
        P(None, "query"),
        P("query"),
        P("query", None),
        P(),
        P(),
        P(),
        P(),
        P(),
        P(),
        P(),
    )
    return jax.shard_map(
        local,
        mesh=mesh,
        in_specs=placed,
        out_specs=(
            P(),
            P("dp", "query"),
            P("query"),
            P("query", "dp"),
            P(),
            P(),
            P(),
            P(),
            P(),
            P(),
            P(),
        ),
        check_vma=False,
    )
```

```python
import functools
import math

import jax
import jax.numpy as jnp
from jax import lax
from jax.experimental import pallas as pl
from jax.experimental.pallas import tpu as pltpu
from jax.sharding import PartitionSpec as P

GRID = 128


def contract_rows(left, right, precision=None):
    return lax.dot_general(
        left,
        right,
        (((0,), (0,)), ((), ())),
        precision=precision,
        preferred_element_type=jnp.float32,
    )


def contract_cols(left, right, precision=None):
    return lax.dot_general(
        left,
        right,
        (((1,), (1,)), ((), ())),
        precision=precision,
        preferred_element_type=jnp.float32,
    )


def trunk_forward(coords, v_one, c_one, v_two, c_two, v_three, c_three):
    first_act = jnp.tanh(
        coords[0][:, None] * v_one[0][None, :] + coords[1][:, None] * v_one[1][None, :] + c_one
    )
    first_b = first_act.astype(jnp.bfloat16)
    second_act = jnp.tanh(jnp.dot(first_b, v_two, preferred_element_type=jnp.float32) + c_two)
    second_b = second_act.astype(jnp.bfloat16)
    basis_full = jnp.dot(second_b, v_three, preferred_element_type=jnp.float32) + c_three
    return (first_act, first_b, second_act, second_b, basis_full.astype(jnp.bfloat16))


def swap(value, axis, mask):
    count = lax.axis_size(axis)
    return lax.ppermute(value, axis, [(i, i ^ mask) for i in range(count)])


def bits_of(count):
    return [1 << b for b in range(count.bit_length() - 1)]


def gather_xor(value, axis, masks):
    blocks, offsets = value, [0]
    for mask in masks:
        blocks = jnp.concatenate([blocks, swap(blocks, axis, mask)], axis=0)
        offsets = offsets + [o ^ mask for o in offsets]
    return blocks, offsets


def split_pair(value):
    high = lax.reduce_precision(value, 8, 7)
    return high.astype(jnp.bfloat16), (value - high).astype(jnp.bfloat16)


def trunk_backward(coords, first_act, first_b, second_act, second_b, grad_basis, v_two, v_three):
    basis_hi, basis_lo = split_pair(grad_basis)
    grad_v_three = contract_rows(second_b, basis_hi) + contract_rows(second_b, basis_lo)
    grad_c_three = jnp.sum(grad_basis, axis=0)
    grad_second = (contract_cols(basis_hi, v_three) + contract_cols(basis_lo, v_three)) * (
        1.0 - second_act * second_act
    )
    second_hi, second_lo = split_pair(grad_second)
    grad_v_two = contract_rows(first_b, second_hi) + contract_rows(first_b, second_lo)
    grad_c_two = jnp.sum(grad_second, axis=0)
    grad_first = (contract_cols(second_hi, v_two) + contract_cols(second_lo, v_two)) * (
        1.0 - first_act * first_act
    )
    grad_v_one = jnp.stack(
        [jnp.sum(coords[0][:, None] * grad_first, axis=0), jnp.sum(coords[1][:, None] * grad_first, axis=0)]
    )
    grad_c_one = jnp.sum(grad_first, axis=0)
    return (grad_v_one, grad_c_one, grad_v_two, grad_c_two, grad_v_three, grad_c_three)


def local_wide(
    sensors,
    query_index,
    targets,
    w_one,
    b_one,
    w_two,
    b_two,
    v_one,
    c_one,
    v_two,
    c_two,
    v_three,
    c_three,
):
    dp_count, q_count = lax.axis_size("dp"), lax.axis_size("query")
    func_rows = sensors.shape[0]
    query_rows = query_index.shape[1]
    count_all = func_rows * dp_count * query_rows * q_count
    grad_scale = 64.0 / math.sqrt(count_all)
    inv_scale = 1.0 / math.sqrt(w_two.shape[1])
    dp_me, q_me = lax.axis_index("dp"), lax.axis_index("query")
    dp_bits, q_bits = bits_of(dp_count), bits_of(q_count)
    half = func_rows // 2
    parity = lax.rem(q_me, 2)
    mine = parity * half
    other = half - mine

    w_two_all, _ = gather_xor(w_two, "query", q_bits[::-1])
    sensor_cols = sensors.shape[1] // dp_count
    sensors_half = lax.dynamic_slice_in_dim(sensors, mine, half, 0)
    held = []
    for offset in range(dp_count):
        start = jnp.bitwise_xor(dp_me, offset) * sensor_cols
        block = lax.dynamic_slice_in_dim(sensors_half, start, sensor_cols, 1)
        held.append(block if offset == 0 else swap(block, "dp", offset))
    sensors_mine = jnp.concatenate(held, axis=0)
    sensors_other = swap(sensors_mine, "query", 1)

    hidden = jnp.tanh(jnp.dot(sensors, w_one, preferred_element_type=jnp.float32) + b_one)
    hidden_b = hidden.astype(jnp.bfloat16)
    hidden_all, _ = gather_xor(hidden_b, "query", q_bits[::-1])
    hidden_wide = jnp.concatenate(
        [hidden_all[i * func_rows : (i + 1) * func_rows] for i in range(q_count)], axis=1
    )

    coords = query_index.astype(jnp.float32) / (GRID - 1)
    first_act, first_b, second_act, second_b, basis_b = trunk_forward(
        coords, v_one, c_one, v_two, c_two, v_three, c_three
    )

    coeffs = jnp.dot(hidden_wide, w_two_all, preferred_element_type=jnp.float32) + b_two
    coeffs_b = coeffs.astype(jnp.bfloat16)
    prediction = contract_cols(coeffs_b, basis_b) * inv_scale
    misfit = prediction - targets.astype(jnp.float32)
    loss_part = jnp.sum(misfit * misfit)
    misfit_b = (misfit * grad_scale).astype(jnp.bfloat16)

    partial = jnp.dot(misfit_b, basis_b, preferred_element_type=jnp.float32) * inv_scale
    running = lax.dynamic_slice_in_dim(partial, mine, half, 0) + swap(
        lax.dynamic_slice_in_dim(partial, other, half, 0), "query", 1
    )
    for mask in q_bits[1:]:
        running = running + swap(running, "query", mask)
    running_b = running.astype(jnp.bfloat16)
    grad_coeffs_b = jnp.concatenate([running_b, swap(running_b, "query", 1)], axis=0)

    def in_order(value):
        return jnp.concatenate(
            [
                lax.dynamic_slice_in_dim(value, mine, half, 0),
                lax.dynamic_slice_in_dim(value, other, half, 0),
            ],
            axis=0,
        )

    hidden_o = in_order(hidden)
    hidden_bo = in_order(hidden_b)
    grad_pre = contract_cols(grad_coeffs_b, w_two) * (1.0 - hidden_o * hidden_o)
    grad_pre_b = grad_pre.astype(jnp.bfloat16)
    wide_first = dp_bits[1:][::-1] + dp_bits[:1]
    wide_last = dp_bits[:1] + dp_bits[1:][::-1]
    sides = []
    for rows, masks in ((grad_pre_b[:half], wide_first), (grad_pre_b[half:], wide_last)):
        blocks, offsets = gather_xor(rows, "dp", masks)
        sides.append(
            jnp.concatenate(
                [blocks[offsets.index(o) * half : (offsets.index(o) + 1) * half] for o in range(dp_count)],
                axis=0,
            )
        )
    grad_w_one = contract_rows(
        jnp.concatenate([sensors_mine, sensors_other], axis=0), jnp.concatenate(sides, axis=0)
    )

    rest = contract_rows(grad_coeffs_b, hidden_bo)
    bias_sum = jnp.broadcast_to(jnp.sum(grad_pre, axis=0)[None, :], (8, grad_pre.shape[1]))
    for mask in dp_bits[::-1]:
        rows = rest.shape[0] // 2
        upper = jnp.bitwise_and(dp_me, mask) // mask
        keep = lax.dynamic_slice_in_dim(rest, upper * rows, rows, 0)
        give = lax.dynamic_slice_in_dim(rest, (1 - upper) * rows, rows, 0)
        both = jnp.concatenate([keep, bias_sum], axis=0) + swap(
            jnp.concatenate([give, bias_sum], axis=0), "dp", mask
        )
        rest, bias_sum = both[:rows], both[rows:]
    grad_w_two = rest.T
    grad_b_one = bias_sum[0]

    trunk_parts = trunk_backward(
        coords, first_act, first_b, second_act, second_b, inv_scale * contract_rows(misfit_b, coeffs_b), v_two, v_three
    )
    loss_sum, grad_b_two, *sums = lax.psum(
        (loss_part, jnp.sum(partial, axis=0)) + trunk_parts, ("dp", "query")
    )
    return (loss_sum / count_all, grad_w_one, grad_b_one, grad_w_two, grad_b_two, *sums)


MESH = pl.DeviceIdType.MESH
F32, BF16 = jnp.float32, jnp.bfloat16
def natural(left, right):
    return jnp.dot(left, right, preferred_element_type=F32)


def lanes_summed(value):
    total = value[:, :128]
    for start in range(128, value.shape[1], 128):
        total = total + value[:, start : start + 128]
    return total


class Trunk:
    def __init__(self, partial, landing, total, base, rows, order, back, me, flip, bit, line, launch, remote):
        self.partial, self.landing, self.total = partial, landing, total
        self.me, self.flip, self.bit, self.line = me, flip, bit, line
        self.launch, self.remote = launch, remote
        self.order, self.back = order, back
        self.size, self.off, self.land = rows, base, base
        self.stride = {step: rows >> (k + 1) for k, step in enumerate(order)}
        self.flight = []

    def span(self, start, size):
        return pl.ds(pl.multiple_of(start, 8), size)

    def send(self, src, dst, axis, offset):
        self.flight.append(self.launch(self.remote(src, dst, axis, self.flip(self.me[axis], offset))))

    def wait(self):
        for copy in self.flight:
            copy.wait_recv()
        self.flight = []

    def start(self, k):
        axis, mask = self.order[k]
        size = self.size // 2
        up = self.bit(self.me[axis], mask)
        give = self.span(self.off + (1 - up) * size, size)
        self.send(self.partial.at[give, :], self.landing.at[self.land : self.land + size, :], axis, mask)
        self.off = self.off + up * size

    def end(self, k):
        self.wait()
        self.size //= 2
        self.partial[self.span(self.off, self.size), :] += self.landing[self.land : self.land + self.size, :]
        self.land += self.size

    def line_start(self):
        at, count = self.line
        size = self.size // count
        for k in range(1, count):
            give = self.span(self.off + self.flip(at, k) * size, size)
            first = self.land + (k - 1) * size
            self.send(self.partial.at[give, :], self.landing.at[first : first + size, :], "dp", 2 * k)

    def line_end(self):
        at, count = self.line
        size = self.size // count
        self.wait()
        mine = self.span(self.off + at * size, size)
        value = self.partial[mine, :]
        for k in range(1, count):
            first = self.land + (k - 1) * size
            value = value + self.landing[first : first + size, :]
        self.total[mine, :] = value

    def back_line_start(self):
        at, count = self.line
        size = self.size // count
        mine = self.total.at[self.span(self.off + at * size, size), :]
        for k in range(1, count):
            self.send(mine, mine, "dp", 2 * k)
        self.held = [[(self.off, self.size)] for _ in self.back]

    def back_start(self, k):
        width = self.total.shape[1] // len(self.back)
        for j, back in enumerate(self.back):
            axis, mask = step = back[k]
            held = self.held[j]
            if k == len(back) - 1:
                rows = self.stride[step]
                held = [(held[0][0] // rows * rows, rows)]
            cols = slice(j * width, (j + 1) * width)
            for off, size in held:
                block = self.total.at[self.span(off, size), cols]
                self.send(block, block, axis, mask)
            turn = self.stride[step] * (1 - 2 * self.bit(self.me[axis], mask))
            self.held[j] = held + [(off + turn, size) for off, size in held]

    def back_end(self, k):
        self.wait()

    def back_line_end(self):
        self.wait()


def step_kernel(
    n_dp,
    n_q,
    count_all,
    sensors_h,
    qidx_h,
    targets_h,
    w_one_h,
    b_one_h,
    w_two_h,
    b_two_h,
    v_one_h,
    c_one_h,
    v_two_h,
    c_two_h,
    v_three_h,
    c_three_h,
    loss_h,
    gw_one_o,
    gb_one_h,
    gw_two_h,
    gb_two_h,
    gv_one_h,
    gc_one_h,
    gv_two_o,
    gc_two_h,
    gv_three_o,
    gc_three_h,
    qidx,
    b_one,
    b_two,
    v_one,
    c_one,
    c_two,
    c_three,
    loss_o,
    gb_one_o,
    gw_two_o,
    gb_two_o,
    gv_one_o,
    gc_one_o,
    gc_two_o,
    gc_three_o,
    sens,
    tgt,
    w_one,
    w_two,
    v_two,
    v_three,
    v_two_t,
    v_three_t,
    hid,
    hid_b,
    first,
    second,
    first_b,
    second_b,
    basis,
    coef_b,
    coef_bt,
    mis_b,
    gco,
    gco_in,
    gco_run,
    gco_rx,
    gco_b,
    pre_all,
    sens_all,
    rest,
    rest_in,
    rest_line,
    bias,
    bias_in,
    trunk,
    trunk_in,
    trunk_out,
    small,
    small_in,
    sums,
    loss_row,
    g_two_b,
    acc,
    acc_in,
    load_sem,
    send_sem,
    recv_sem,
):
    func_rows, sensor_all = sens.shape
    hidden = w_one.shape[1]
    units, queries = first.shape
    basis_n = coef_b.shape[1]
    cols_dp = sensor_all // n_dp
    block = min(512, queries)
    blocks = queries // block
    inv_scale = 1.0 / math.sqrt(basis_n)
    grad_scale = 64.0 / math.sqrt(count_all)
    dp, q = lax.axis_index("dp"), lax.axis_index("query")
    me = {"dp": dp, "query": q}
    q_bits = bits_of(n_q)
    half = func_rows // 2
    part = lax.rem(q, 2)
    mine = pl.multiple_of(part * half, 8)
    other = pl.multiple_of((1 - part) * half, 8)
    side, line_at, line_n = lax.rem(dp, 2), dp // 2, n_dp // 2

    def bit(index, mask):
        return lax.rem(index // mask, 2)

    def flip(index, offset):
        result = index
        for mask in bits_of(n_dp * n_q):
            if offset & mask:
                result = result + mask * (1 - 2 * bit(index, mask))
        return result

    used = [0]

    def remote(src, dst, axis, peer):
        k = used[0]
        used[0] = k + 1
        return pltpu.make_async_remote_copy(
            src_ref=src,
            dst_ref=dst,
            send_sem=send_sem.at[k],
            recv_sem=recv_sem.at[k],
            device_id={axis: peer},
            device_id_type=MESH,
        )

    sent = []

    def launch(copy):
        copy.start()
        sent.append(copy)
        return copy

    pair = flip(dp, 1)
    barrier = pltpu.get_barrier_semaphore()
    dp_peers = [pair] + [flip(dp, 2 * k) for k in range(1, line_n)]
    for peer in dp_peers:
        pl.semaphore_signal(barrier, inc=1, device_id={"dp": peer}, device_id_type=MESH)
    for mask in q_bits:
        pl.semaphore_signal(barrier, inc=1, device_id={"query": flip(q, mask)}, device_id_type=MESH)

    def sensor_block(index, rows):
        return sensors_h.at[rows, pl.ds(pl.multiple_of(index * cols_dp, 128), cols_dp)]

    every = pl.ds(0, func_rows)
    loads = {}
    for k, (name, src, dst) in enumerate(
        (
            ("w_one", w_one_h, w_one),
            ("sens", sensors_h, sens),
            ("b_one", b_one_h, b_one),
            ("qidx", qidx_h, qidx),
            ("b_two", b_two_h, b_two),
            ("v_one", v_one_h, v_one),
            ("c_one", c_one_h, c_one),
            ("c_two", c_two_h, c_two),
            ("c_three", c_three_h, c_three),
            ("v_two", v_two_h, v_two),
            ("v_three", v_three_h, v_three),
            ("w_two", w_two_h, w_two.at[q]),
            ("targets", targets_h, tgt),
            ("own0", sensor_block(line_at * 2, every), sens_all.at[line_at * 2]),
            ("own1", sensor_block(line_at * 2 + 1, every), sens_all.at[line_at * 2 + 1]),
        )
    ):
        loads[name] = pltpu.make_async_copy(src, dst, load_sem.at[k])
        loads[name].start()
    pl.semaphore_wait(barrier, len(dp_peers) + len(q_bits))

    q_order = q_bits[::-1]
    w_half = hidden // 2
    w_rows = [pl.ds(pl.multiple_of(side * w_half + c * (w_half // 2), 16), w_half // 2) for c in range(2)]
    q_far = flip(q, q_order[0])
    w_far = [launch(remote(w_two_h.at[rows, :], w_two.at[q, rows, :], "query", q_far)) for rows in w_rows]
    bulk = []
    rows_mine = pl.ds(mine, half)
    share_n = func_rows // n_q

    def rows_of(member):
        return pl.ds(pl.multiple_of(member * share_n, 16), share_n)

    for k in [1] + list(range(line_n - 1, 1, -1)):
        to = flip(line_at, k)
        for s in range(2):
            copy = remote(
                sensor_block(to * 2 + s, rows_of(q)), sens_all.at[line_at * 2 + s, rows_of(q), :], "dp", flip(dp, 2 * k)
            )
            bulk.append((to * 2 + s, launch(copy)))

    def pass_on(index, member, mask):
        ref = sens_all.at[index, rows_of(member), :]
        return launch(remote(ref, ref, "query", flip(q, mask)))

    far, passed = [], []

    def pass_far(k):
        for index, copy in bulk[2 * k : 2 * k + 2]:
            copy.wait_recv()
            far.append((index, pass_on(index, q, q_order[0])))
            passed.append(pass_on(index, q, 1))


    loads["w_one"].wait()
    loads["sens"].wait()
    loads["b_one"].wait()
    act = jnp.tanh(natural(sens[...], w_one[...]) + b_one[...])
    hid[...] = act
    hid_b[q] = act.astype(BF16)
    h_far = launch(remote(hid_b.at[q], hid_b.at[q], "query", q_far))

    for name in ("qidx", "b_two", "v_one", "c_one", "c_two", "c_three", "v_two"):
        loads[name].wait()
    loads["v_three"].wait()
    v_two_t[...] = v_two[...].astype(F32).T.astype(BF16)
    v_three_t[...] = v_three[...].astype(F32).T.astype(BF16)
    columns = jnp.concatenate(
        [v_one[...], c_one[...], c_two[...], c_three[...], jnp.zeros((3, units), F32)], axis=0
    ).T

    def coords_of(span):
        x = qidx[0:1, span].astype(F32) / (GRID - 1)
        y = qidx[1:2, span].astype(F32) / (GRID - 1)
        return x, y

    def forward(i, carry):
        span = pl.ds(pl.multiple_of(i * block, 128), block)
        x, y = coords_of(span)
        one = jnp.tanh(columns[:, 0:1] * x + columns[:, 1:2] * y + columns[:, 2:3])
        first[:, span] = one
        one_b = one.astype(BF16)
        first_b[:, span] = one_b
        two = jnp.tanh(natural(v_two_t[...], one_b) + columns[:, 3:4])
        second[:, span] = two
        two_b = two.astype(BF16)
        second_b[:, span] = two_b
        basis[:, span] = (natural(v_three_t[...], two_b) + columns[:, 4:5]).astype(BF16)
        return carry

    def spread(buffer, held, masks):
        group = []
        for mask in masks:
            for copy in group:
                copy.wait_recv()
            group = [
                launch(remote(buffer.at[flip(q, o)], buffer.at[flip(q, o)], "query", flip(q, mask))) for o in held
            ]
            held = held + [o ^ mask for o in held]
        return group

    lax.fori_loop(0, blocks // 2, forward, 0)
    w_pair = []
    for rows, copy in zip(w_rows, w_far):
        copy.wait_recv()
        w_pair.append(launch(remote(w_two.at[q_far, rows, :], w_two.at[q_far, rows, :], "dp", pair)))
    lax.fori_loop(blocks // 2, blocks, forward, 0)
    loads["w_two"].wait()
    h_far.wait_recv()
    h_last = spread(hid_b, [0, q_order[0]], q_order[1:])
    for copy in w_pair:
        copy.wait_recv()
    w_last = spread(w_two, [0, q_order[0]], q_order[1:])
    for copy in h_last + w_last:
        copy.wait_recv()

    pass_far(0)
    coef = natural(hid_b[0], w_two[0])
    for i in range(1, n_q):
        coef = coef + natural(hid_b[i], w_two[i])
    coef = coef + b_two[...]
    coef_b[...] = coef.astype(BF16)
    coef_bt[...] = coef.T.astype(BF16)

    loads["targets"].wait()
    loss_row[...] = jnp.zeros_like(loss_row)

    def fit(i, carry):
        span = pl.ds(pl.multiple_of(i * block, 128), block)
        base = basis[:, span]
        miss = natural(coef_b[...], base) * inv_scale - tgt[:, span].astype(F32)
        loss_row[0:1, :] += jnp.sum(miss * miss, axis=0, keepdims=True)
        miss_b = (miss * grad_scale).astype(BF16)
        mis_b[:, span] = miss_b
        return carry

    lax.fori_loop(0, blocks, fit, 0, unroll=True)
    gco[pl.ds(other, half), :] = contract_cols(mis_b[pl.ds(other, half), :], basis[...]) * inv_scale
    core_step = launch(remote(gco.at[pl.ds(other, half), :], gco_in, "query", flip(q, 1)))
    gco[rows_mine, :] = contract_cols(mis_b[rows_mine, :], basis[...]) * inv_scale
    gb_two_row = jnp.sum(gco[...], axis=0, keepdims=True)
    trunk[...] = jnp.zeros_like(trunk)
    sums[...] = jnp.zeros_like(sums)
    core_step.wait_recv()
    gco_run[0] = gco[rows_mine, :] + gco_in[...]
    quarter, piece_n = half // 2, half // 4
    at_mine = bit(q, q_bits[1]) * quarter
    at_other = quarter - at_mine

    def gco_piece(start, c):
        return pl.ds(pl.multiple_of(start + c * piece_n, 16), piece_n)

    reduce_steps = [
        launch(remote(gco_run.at[0, gco_piece(at_other, c), :], gco_rx.at[0, gco_piece(0, c), :], "query", q_far))
        for c in range(2)
    ]
    shares, comes = [], []

    def reduce_piece(c):
        reduce_steps[c].wait_recv()
        total = gco_run[0, gco_piece(at_mine, c), :] + gco_rx[0, gco_piece(0, c), :]
        rows = gco_piece(mine + at_mine, c)
        gco_b[rows, :] = total.astype(BF16)
        ref = gco_b.at[rows, :]
        comes.append(launch(remote(ref, ref, "query", q_far)))
        shares.append(launch(remote(ref, ref, "query", flip(q, 1))))


    bits = [("query", m) for m in q_bits] + [("dp", 1)]
    across_q = [("query", m) for m in q_bits[1:]]
    order, back = [bits[0], ("dp", 1)] + across_q, [("dp", 1)] + across_q + [bits[0]]
    place = (me, flip, bit, (line_at, line_n), launch, remote)
    three = Trunk(trunk, trunk_in, trunk_out, 0, units, order, [back], *place)
    two_ = Trunk(trunk, trunk_in, trunk_out, units, units, order, [across_q + [("dp", 1), bits[0]], back], *place)

    def backward_top(i, carry):
        span = pl.ds(pl.multiple_of(i * block, 128), block)
        g_base = natural(coef_bt[...], mis_b[:, span]) * inv_scale
        sums[0] += lanes_summed(g_base)
        g_base = g_base.astype(BF16)
        trunk[:units, :] += contract_cols(second_b[:, span], g_base)
        two = second[:, span]
        g_two = natural(v_three[...], g_base) * (1.0 - two * two)
        sums[1] += lanes_summed(g_two)
        g_two_b[:, span] = g_two.astype(BF16)
        return carry

    def backward_low(i, carry):
        span = pl.ds(pl.multiple_of(i * block, 128), block)
        x, y = coords_of(span)
        g_two = g_two_b[:, span]
        trunk[units:, :] += contract_cols(first_b[:, span], g_two)
        one = first[:, span]
        g_one = natural(v_two[...], g_two) * (1.0 - one * one)
        sums[2] += lanes_summed(g_one)
        sums[3] += lanes_summed(g_one * x)
        sums[4] += lanes_summed(g_one * y)
        return carry

    lax.fori_loop(0, blocks, backward_top, 0, unroll=2)
    three.start(0)
    reduce_piece(0)
    lax.fori_loop(0, blocks // 2, backward_low, 0, unroll=True)
    three.end(0)
    three.start(1)
    reduce_piece(1)
    lax.fori_loop(blocks // 2, blocks, backward_low, 0, unroll=True)

    pass_far(1)
    for c in range(2):
        comes[c].wait_recv()
        ref = gco_b.at[gco_piece(mine + at_other, c), :]
        shares.append(launch(remote(ref, ref, "query", flip(q, 1))))

    two_.start(0)
    lane = lax.broadcasted_iota(jnp.int32, (units, 128), 1)
    table = jnp.zeros((units, 128), F32)
    for row, which in enumerate((3, 4, 2, 1, 0)):
        table = jnp.where(lane == row, jnp.sum(sums[which], axis=1, keepdims=True), table)
    rows = table.T[0:8]
    line = lax.broadcasted_iota(jnp.int32, rows.shape, 0)
    rows = jnp.where(line == 5, gb_two_row, rows)
    rows = jnp.where(line == 6, loss_row[0:1, :], rows)
    small[0] = rows
    s_flight = []

    def small_start(k):
        axis, mask = bits[k]
        s_flight.append(launch(remote(small.at[k], small_in.at[k], axis, flip(me[axis], mask))))

    def small_end(k):
        s_flight.pop().wait_recv()
        small[k + 1] = small[k] + small_in[k]

    def small_line_start():
        k = len(bits)
        for o in range(1, line_n):
            s_flight.append(launch(remote(small.at[k], small_in.at[k + o - 1], "dp", flip(dp, 2 * o))))

    def small_line_end():
        k = len(bits)
        total = small[k]
        for o in range(1, line_n):
            s_flight[o - 1].wait_recv()
            total = total + small_in[k + o - 1]
        return total

    small_start(0)

    for copy in shares:
        copy.wait_recv()
    act = hid[...]
    g_pre = contract_cols(gco_b[...], w_two[q]) * (1.0 - act * act)
    pre_all[line_at] = g_pre.astype(BF16)

    chunks = 4
    rows_c = func_rows // chunks

    def hop(at, c, peer):
        ref = pre_all.at[jnp.clip(at, 0, line_n - 1), c * rows_c : (c + 1) * rows_c, :]
        return remote(ref, ref, "dp", peer)

    to_right = jnp.minimum(dp + 2, n_dp - 2 + side)
    to_left = jnp.maximum(dp - 2, side)
    steps = line_n - 1
    rights = [[hop(line_at - s, c, to_right) for c in range(chunks)] for s in range(steps)]
    lefts = [[hop(line_at + s, c, to_left) for c in range(chunks)] for s in range(steps)]

    def sends_right(s):
        return jnp.logical_and(line_at - s >= 0, line_at < line_n - 1)

    def sends_left(s):
        return jnp.logical_and(line_at + s < line_n, line_at > 0)

    for c in range(chunks):
        pl.when(sends_right(0))(rights[0][c].start)
        pl.when(sends_left(0))(lefts[0][c].start)

    def gather_step(s, some=range(chunks)):
        for c in some:

            @pl.when(line_at - 1 - s >= 0)
            def _():
                rights[s][c].wait_recv()
                if s + 1 < steps:
                    pl.when(sends_right(s + 1))(rights[s + 1][c].start)

            @pl.when(line_at + 1 + s < line_n)
            def _():
                lefts[s][c].wait_recv()
                if s + 1 < steps:
                    pl.when(sends_left(s + 1))(lefts[s + 1][c].start)

    bias[0] = jnp.broadcast_to(jnp.sum(g_pre, axis=0, keepdims=True), bias.shape[1:])
    gco_bt = gco_b[...].astype(F32).T.astype(BF16)
    rest_all = natural(gco_bt, hid_b[q])
    rows_dp = basis_n // n_dp
    for j in range(n_dp):
        rest[j % 2, j // 2] = rest_all[j * rows_dp : (j + 1) * rows_dp, :]
    two_.end(0)
    two_.start(1)
    small_end(0)
    small_start(1)
    three.end(1)
    three.start(2)
    for k in range(2, line_n - 1):
        pass_far(k)
    for s in range(steps - 2):
        gather_step(s)
    gather_step(steps - 2, range(chunks // 2))
    two_.end(1)
    two_.start(2)
    gather_step(steps - 2, range(chunks // 2, chunks))
    small_end(1)
    small_start(2)
    three.end(2)
    three.line_start()
    rest_pair = [
        launch(remote(rest.at[1 - side], rest_in, "dp", pair)),
        launch(remote(bias.at[0], bias_in.at[0], "dp", pair)),
    ]
    loads["own0"].wait()
    loads["own1"].wait()
    for index, copy in far:
        copy.wait_recv()
        passed.append(pass_on(index, q_far, 1))
    two_.end(2)
    two_.line_start()
    small_end(2)
    small_line_start()
    gather_step(steps - 1)
    for copy in passed:
        copy.wait_recv()

    pieces = 4
    cols_p = cols_dp // pieces
    across = []

    def sum_of(whose, first_col, width):
        cols = slice(first_col, first_col + width)

        def body(j, carry):
            index = j * 2 + (1 - side if whose else side)
            return carry + contract_rows(sens_all[index, :, cols], pre_all[j])

        acc[whose, cols, :] = lax.fori_loop(0, line_n, body, jnp.zeros((width, hidden), F32))

    def send_across(piece):
        cols = slice(piece * cols_p, (piece + 1) * cols_p)
        across.append(launch(remote(acc.at[1, cols, :], acc_in.at[cols, :], "dp", pair)))

    sum_of(1, 0, 2 * cols_p)
    send_across(0)
    three.line_end()
    three.back_line_start()
    send_across(1)
    sum_of(1, 2 * cols_p, 2 * cols_p)
    two_.line_end()
    two_.back_line_start()
    three.back_line_end()
    three.back_start(0)
    two_.back_line_end()
    two_.back_start(0)
    for copy in rest_pair:
        copy.wait_recv()
    rest[side] += rest_in[...]
    bias[1] = bias[0] + bias_in[0]
    rest_flight = []
    for k in range(1, line_n):
        peer = flip(dp, 2 * k)
        rest_flight.append(launch(remote(rest.at[side, flip(line_at, k)], rest_line.at[k - 1], "dp", peer)))
        rest_flight.append(launch(remote(bias.at[1], bias_in.at[k], "dp", peer)))
    send_across(2)
    three.back_end(0)
    three.back_start(1)
    two_.back_end(0)
    two_.back_start(1)
    send_across(3)
    sum_of(0, 0, cols_dp)
    three.back_end(1)
    three.back_start(2)
    outs = []

    def put(src, dst):
        outs.append(pltpu.make_async_copy(src, dst, load_sem.at[len(outs)]))
        outs[-1].start()

    final = small_line_end()
    gv_one_o[...] = final[0:2]
    gc_one_o[...] = final[2:3]
    gc_two_o[...] = final[3:4]
    gc_three_o[...] = final[4:5]
    gb_two_o[...] = final[5:6]
    loss_o[...] = jnp.broadcast_to(jnp.sum(final[6:7], axis=1, keepdims=True) * (1.0 / count_all), loss_o.shape)
    for copy in rest_flight:
        copy.wait_recv()
    final_rest = rest[side, line_at]
    final_bias = bias[1]
    for k in range(1, line_n):
        final_rest = final_rest + rest_line[k - 1]
        final_bias = final_bias + bias_in[k]
    gw_two_o[...] = final_rest
    gb_one_o[...] = final_bias[0:1, :]
    for src, dst in (
        (gv_one_o, gv_one_h),
        (gc_one_o, gc_one_h),
        (gc_two_o, gc_two_h),
        (gc_three_o, gc_three_h),
        (gb_two_o, gb_two_h),
        (loss_o, loss_h),
        (gw_two_o, gw_two_h),
        (gb_one_o, gb_one_h),
    ):
        put(src, dst)
    three.back_end(2)
    put(trunk_out.at[:units, :], gv_three_o)
    two_.back_end(1)
    two_.back_start(2)
    for copy in across:
        copy.wait_recv()
    acc[0] += acc_in[...]
    put(acc.at[0], gw_one_o)
    two_.back_end(2)
    put(trunk_out.at[units:, :], gv_two_o)
    for copy in sent:
        copy.wait_send()
    for s in range(steps):
        for c in range(chunks):
            pl.when(sends_right(s))(rights[s][c].wait_send)
            pl.when(sends_left(s))(lefts[s][c].wait_send)
    for copy in outs:
        copy.wait()


def hand_over(*refs):
    count = (len(refs) - 2) // 3
    near, sems_in, sems_out = refs[2 * count : 3 * count], refs[-2], refs[-1]
    ins = [pltpu.make_async_copy(refs[k], near[k], sems_in.at[k]) for k in range(count)]
    outs = [pltpu.make_async_copy(near[k], refs[count + k], sems_out.at[k]) for k in range(count)]
    for copy in ins:
        copy.start()
    for came, goes in zip(ins, outs):
        came.wait()
        goes.start()
    for copy in outs:
        copy.wait()


def local_dense(
    sensors, query_index, targets, w_one, b_one, w_two, b_two, v_one, c_one, v_two, c_two, v_three, c_three
):
    n_dp, n_q = lax.axis_size("dp"), lax.axis_size("query")
    func_rows, sensor_all = sensors.shape
    queries = query_index.shape[1]
    hidden, basis_n = w_two.shape
    units = v_two.shape[0]
    cols_dp = sensor_all // n_dp
    count_all = func_rows * n_dp * queries * n_q
    line_n, q_n = n_dp // 2, len(bits_of(n_q))
    half = func_rows // 2
    rows_dp = basis_n // n_dp
    hbm = pl.BlockSpec(memory_space=pl.ANY)
    sem_n = 160

    def row(value):
        return value.reshape(1, -1)

    def result(*shape):
        return jax.ShapeDtypeStruct(shape, F32)

    results = (
        result(1, 128),
        result(cols_dp, hidden),
        result(1, hidden),
        result(rows_dp, hidden),
        result(1, basis_n),
        result(2, units),
        result(1, units),
        result(units, units),
        result(1, units),
        result(units, basis_n),
        result(1, basis_n),
    )
    outs = pl.pallas_call(
        functools.partial(step_kernel, n_dp, n_q, count_all),
        out_shape=results,
        in_specs=[hbm] * 13,
        out_specs=(hbm,) * len(results),
        scratch_shapes=[
            pltpu.VMEM((2, queries), jnp.int32),
            pltpu.VMEM((1, hidden), F32),
            pltpu.VMEM((1, basis_n), F32),
            pltpu.VMEM((2, units), F32),
            pltpu.VMEM((1, units), F32),
            pltpu.VMEM((1, units), F32),
            pltpu.VMEM((1, basis_n), F32),
            pltpu.VMEM((1, 128), F32),
            pltpu.VMEM((1, hidden), F32),
            pltpu.VMEM((rows_dp, hidden), F32),
            pltpu.VMEM((1, basis_n), F32),
            pltpu.VMEM((2, units), F32),
            pltpu.VMEM((1, units), F32),
            pltpu.VMEM((1, units), F32),
            pltpu.VMEM((1, basis_n), F32),
            pltpu.VMEM((func_rows, sensor_all), BF16),
            pltpu.VMEM((func_rows, queries), BF16),
            pltpu.VMEM((sensor_all, hidden), BF16),
            pltpu.VMEM((n_q, hidden, basis_n), BF16),
            pltpu.VMEM((units, units), BF16),
            pltpu.VMEM((units, basis_n), BF16),
            pltpu.VMEM((units, units), BF16),
            pltpu.VMEM((basis_n, units), BF16),
            pltpu.VMEM((func_rows, hidden), F32),
            pltpu.VMEM((n_q, func_rows, hidden), BF16),
            pltpu.VMEM((units, queries), F32),
            pltpu.VMEM((units, queries), F32),
            pltpu.VMEM((units, queries), BF16),
            pltpu.VMEM((units, queries), BF16),
            pltpu.VMEM((basis_n, queries), BF16),
            pltpu.VMEM((func_rows, basis_n), BF16),
            pltpu.VMEM((basis_n, func_rows), BF16),
            pltpu.VMEM((func_rows, queries), BF16),
            pltpu.VMEM((func_rows, basis_n), F32),
            pltpu.VMEM((half, basis_n), F32),
            pltpu.VMEM((q_n, half, basis_n), F32),
            pltpu.VMEM((q_n, half, basis_n), F32),
            pltpu.VMEM((func_rows, basis_n), BF16),
            pltpu.VMEM((line_n, func_rows, hidden), BF16),
            pltpu.VMEM((n_dp, func_rows, cols_dp), BF16),
            pltpu.VMEM((2, line_n, rows_dp, hidden), F32),
            pltpu.VMEM((line_n, rows_dp, hidden), F32),
            pltpu.VMEM((line_n, rows_dp, hidden), F32),
            pltpu.VMEM((2, 8, hidden), F32),
            pltpu.VMEM((line_n, 8, hidden), F32),
            pltpu.VMEM((2 * units, basis_n), F32),
            pltpu.VMEM((2 * units, basis_n), F32),
            pltpu.VMEM((2 * units, basis_n), F32),
            pltpu.VMEM((q_n + 2, 8, units), F32),
            pltpu.VMEM((q_n + line_n, 8, units), F32),
            pltpu.VMEM((5, units, 128), F32),
            pltpu.VMEM((8, min(512, queries)), F32),
            pltpu.VMEM((units, queries), BF16),
            pltpu.VMEM((2, cols_dp, hidden), F32),
            pltpu.VMEM((cols_dp, hidden), F32),
            pltpu.SemaphoreType.DMA((32,)),
            pltpu.SemaphoreType.DMA((sem_n,)),
            pltpu.SemaphoreType.DMA((sem_n,)),
        ],
        compiler_params=pltpu.CompilerParams(
            collective_id=0, has_side_effects=True, vmem_limit_bytes=67043328
        ),
        name="step",
    )(
        sensors,
        query_index,
        targets,
        w_one,
        row(b_one),
        w_two,
        row(b_two),
        v_one,
        row(c_one),
        v_two,
        row(c_two),
        v_three,
        row(c_three),
    )
    outs = pl.pallas_call(
        hand_over,
        out_shape=results,
        in_specs=[hbm] * len(results),
        out_specs=(hbm,) * len(results),
        scratch_shapes=[pltpu.VMEM(value.shape, F32) for value in results]
        + [pltpu.SemaphoreType.DMA((len(results),))] * 2,
        name="hand_over",
    )(*outs)
    loss, gw_one, gb_one, gw_two, gb_two, gv_one, gc_one, gv_two, gc_two, gv_three, gc_three = outs
    return (
        loss[0, 0],
        gw_one,
        gb_one.reshape(-1),
        gw_two.T,
        gb_two.reshape(-1),
        gv_one,
        gc_one.reshape(-1),
        gv_two,
        gc_two.reshape(-1),
        gv_three,
        gc_three.reshape(-1),
    )


def local(sensors, query_index, targets, w_one, b_one, w_two, b_two, v_one, c_one, v_two, *others):
    n_dp, n_q = lax.axis_size("dp"), lax.axis_size("query")
    units, basis_n = v_two.shape[0], w_two.shape[1]
    dense = (
        (sensors.shape[1] // n_dp) % 128 == 0
        and units == basis_n == min(512, query_index.shape[1])
        and (units // 2) % (8 * n_dp * n_q) == 0
        and sensors.shape[0] % (16 * n_q) == 0
        and len(bits_of(n_q)) == 2
        and len(bits_of(n_dp)) == 3
    )
    chosen = local_dense if dense else local_wide
    return chosen(sensors, query_index, targets, w_one, b_one, w_two, b_two, v_one, c_one, v_two, *others)


def solution(mesh):
    placed = (
        P("dp", None),
        P(None, "query"),
        P("dp", "query"),
        P(None, "query"),
        P("query"),
        P("query", None),
        P(),
        P(),
        P(),
        P(),
        P(),
        P(),
        P(),
    )
    return jax.shard_map(
        local,
        mesh=mesh,
        in_specs=placed,
        out_specs=(
            P(),
            P("dp", "query"),
            P("query"),
            P("query", "dp"),
            P(),
            P(),
            P(),
            P(),
            P(),
            P(),
            P(),
        ),
        check_vma=False,
    )
```
